128 devices in a mesh: tp: 2 (over core), cp: 64 (over z, y, x).
Axes of the slice: x: 4, y: 4, z: 4, core: 2. Of those that a mesh axis runs over, the one named last changes fastest.
Arguments:
- hidden: bfloat16 [2, 8192, 2048], P(None, 'cp')
- grad_out: bfloat16 [2, 8192, 2048], P(None, 'cp')
- w_query: bfloat16 [2048, 16, 128], P(None, 'tp')
- w_key: bfloat16 [2048, 128], replicated
- w_value: bfloat16 [2048, 128], replicated
- w_out: bfloat16 [16, 128, 2048], P('tp')
Outputs:
- output 1: bfloat16 [2, 8192, 2048], P(None, 'cp')
- output 2: bfloat16 [2, 8192, 2048], P(None, 'cp')
- output 3: float32 [2048, 16, 128], P(None, 'tp')
- output 4: float32 [2048, 128], replicated
- output 5: float32 [2048, 128], replicated
- output 6: float32 [16, 128, 2048], P('tp')
All inputs are finite; a program needn't handle non-finite values.
Results may differ from the reference program's by a relative error of at most 0.0101215.
Values are sent between devices in bfloat16 or wider.
A program may use at most 1 GiB of HBM per device.

```python
import jax
import jax.numpy as jnp
from jax import lax

BATCH = 2
SEQ = 8192
D_MODEL = 2048
HEADS = 16
HEAD_DIM = 128
Q_ROWS = 128


def rope_tables(positions):
    half_dim = HEAD_DIM // 2
    inv_freq = 1.0 / jnp.power(10000.0, jnp.arange(half_dim, dtype=jnp.float32) * (2.0 / HEAD_DIM))
    angles = positions.astype(jnp.float32)[:, None] * inv_freq[None, :]
    return jnp.cos(angles), jnp.sin(angles)


def rotate(rot_in, cos_tab, sin_tab):
    half_dim = rot_in.shape[-1] // 2
    low_half = rot_in[..., :half_dim]
    high_half = rot_in[..., half_dim:]
    return jnp.concatenate([low_half * cos_tab - high_half * sin_tab, high_half * cos_tab + low_half * sin_tab], axis=-1)


def unrotate(rot_in, cos_tab, sin_tab):
    half_dim = rot_in.shape[-1] // 2
    low_half = rot_in[..., :half_dim]
    high_half = rot_in[..., half_dim:]
    return jnp.concatenate([low_half * cos_tab + high_half * sin_tab, high_half * cos_tab - low_half * sin_tab], axis=-1)


def setup_inputs(seed: int = 0) -> dict:
    sub_keys = jax.random.split(jax.random.key(seed), 6)
    hidden = jax.random.normal(sub_keys[0], (BATCH, SEQ, D_MODEL), jnp.float32)
    grad_out = jax.random.normal(sub_keys[1], (BATCH, SEQ, D_MODEL), jnp.float32)
    in_scale = D_MODEL ** -0.5
    w_query = jax.random.normal(sub_keys[2], (D_MODEL, HEADS, HEAD_DIM), jnp.float32) * in_scale
    w_key = jax.random.normal(sub_keys[3], (D_MODEL, HEAD_DIM), jnp.float32) * in_scale
    w_value = jax.random.normal(sub_keys[4], (D_MODEL, HEAD_DIM), jnp.float32) * in_scale
    w_out = jax.random.normal(sub_keys[5], (HEADS, HEAD_DIM, D_MODEL), jnp.float32) * (HEADS * HEAD_DIM) ** -0.5
    return {"hidden": hidden.astype(jnp.bfloat16), "grad_out": grad_out.astype(jnp.bfloat16), "w_query": w_query.astype(jnp.bfloat16), "w_key": w_key.astype(jnp.bfloat16), "w_value": w_value.astype(jnp.bfloat16), "w_out": w_out.astype(jnp.bfloat16)}


def reference(hidden, grad_out, w_query, w_key, w_value, w_out):
    q_scale = HEAD_DIM ** -0.5
    n_blocks = SEQ // Q_ROWS
    cos_tab, sin_tab = rope_tables(jnp.arange(SEQ))
    flat_hidden = hidden.reshape(BATCH * SEQ, D_MODEL)
    key_pre = jnp.dot(flat_hidden, w_key, preferred_element_type=jnp.float32).reshape(BATCH, SEQ, HEAD_DIM)
    key_rot = rotate(key_pre, cos_tab, sin_tab).astype(jnp.bfloat16).astype(jnp.float32)
    val_all = jnp.dot(flat_hidden, w_value, preferred_element_type=jnp.float32).reshape(BATCH, SEQ, HEAD_DIM).astype(jnp.bfloat16).astype(jnp.float32)
    key_pos = jnp.arange(SEQ)
    hid_blocks = hidden.reshape(BATCH, n_blocks, Q_ROWS, D_MODEL).transpose(1, 0, 2, 3)
    grad_blocks = grad_out.reshape(BATCH, n_blocks, Q_ROWS, D_MODEL).transpose(1, 0, 2, 3)
    cos_blocks = cos_tab.reshape(n_blocks, Q_ROWS, HEAD_DIM // 2)
    sin_blocks = sin_tab.reshape(n_blocks, Q_ROWS, HEAD_DIM // 2)
    row_starts = jnp.arange(n_blocks) * Q_ROWS
    kv_zero = jnp.zeros((BATCH, SEQ, HEAD_DIM), jnp.float32)
    big_zero = jnp.zeros((BATCH, SEQ, D_MODEL), jnp.float32)

    def head_step(carry_in, head_weights):
        out_acc, dh_acc, dk_acc, dv_acc = carry_in
        wq_head, wo_head = head_weights

        def block_step(block_carry, block_in):
            dk_run, dv_run, dwq_run, dwo_run = block_carry
            hid_blk, grad_blk, cos_blk, sin_blk, row_start = block_in
            hid_flat = hid_blk.reshape(BATCH * Q_ROWS, D_MODEL)
            grad_flat = grad_blk.reshape(BATCH * Q_ROWS, D_MODEL)
            q_pre = jnp.dot(hid_flat, wq_head, preferred_element_type=jnp.float32).reshape(BATCH, Q_ROWS, HEAD_DIM)
            q_rot = (rotate(q_pre, cos_blk, sin_blk) * q_scale).astype(jnp.bfloat16).astype(jnp.float32)
            scores = jnp.einsum("bqe,bke->bqk", q_rot, key_rot)
            q_pos = row_start + jnp.arange(Q_ROWS)
            allowed = key_pos[None, :] <= q_pos[:, None]
            scores = jnp.where(allowed[None], scores, -jnp.inf)
            probs_blk = jax.nn.softmax(scores, axis=-1)
            attn_blk = jnp.einsum("bqk,bke->bqe", probs_blk, val_all).astype(jnp.bfloat16)
            d_attn = jnp.dot(grad_flat, wo_head.T, preferred_element_type=jnp.float32).astype(jnp.bfloat16)
            attn_f = attn_blk.astype(jnp.float32)
            d_attn_f = d_attn.astype(jnp.float32).reshape(BATCH, Q_ROWS, HEAD_DIM)
            d_prob = jnp.einsum("bqe,bke->bqk", d_attn_f, val_all)
            row_delta = jnp.sum(d_attn_f * attn_f, axis=-1, keepdims=True)
            d_score = probs_blk * (d_prob - row_delta)
            dq_blk = jnp.einsum("bqk,bke->bqe", d_score, key_rot)
            dk_run = dk_run + jnp.einsum("bqk,bqe->bke", d_score, q_rot)
            dv_run = dv_run + jnp.einsum("bqk,bqe->bke", probs_blk, d_attn_f)
            dq_pre = (unrotate(dq_blk, cos_blk, sin_blk) * q_scale).astype(jnp.bfloat16).reshape(BATCH * Q_ROWS, HEAD_DIM)
            attn_flat = attn_blk.reshape(BATCH * Q_ROWS, HEAD_DIM)
            dwq_run = dwq_run + jnp.dot(hid_flat.T, dq_pre, preferred_element_type=jnp.float32)
            dwo_run = dwo_run + jnp.dot(attn_flat.T, grad_flat, preferred_element_type=jnp.float32)
            out_part = jnp.dot(attn_flat, wo_head, preferred_element_type=jnp.float32)
            dh_part = jnp.dot(dq_pre, wq_head.T, preferred_element_type=jnp.float32)
            return (dk_run, dv_run, dwq_run, dwo_run), (out_part, dh_part)

        block_init = (kv_zero, kv_zero, jnp.zeros((D_MODEL, HEAD_DIM), jnp.float32), jnp.zeros((HEAD_DIM, D_MODEL), jnp.float32))
        block_out, block_ys = lax.scan(block_step, block_init, (hid_blocks, grad_blocks, cos_blocks, sin_blocks, row_starts))
        dk_run, dv_run, dwq_run, dwo_run = block_out
        out_parts, dh_parts = block_ys
        out_head = out_parts.reshape(n_blocks, BATCH, Q_ROWS, D_MODEL).transpose(1, 0, 2, 3).reshape(BATCH, SEQ, D_MODEL)
        dh_head = dh_parts.reshape(n_blocks, BATCH, Q_ROWS, D_MODEL).transpose(1, 0, 2, 3).reshape(BATCH, SEQ, D_MODEL)
        new_carry = (out_acc + out_head, dh_acc + dh_head, dk_acc + dk_run, dv_acc + dv_run)
        return new_carry, (dwq_run, dwo_run)

    head_init = (big_zero, big_zero, kv_zero, kv_zero)
    head_out, head_ys = lax.scan(head_step, head_init, (w_query.transpose(1, 0, 2), w_out))
    out_acc, dh_acc, dk_acc, dv_acc = head_out
    d_w_query = head_ys[0].transpose(1, 0, 2)
    d_w_out = head_ys[1]
    dk_pre = unrotate(dk_acc, cos_tab, sin_tab).astype(jnp.bfloat16).reshape(BATCH * SEQ, HEAD_DIM)
    dv_pre = dv_acc.astype(jnp.bfloat16).reshape(BATCH * SEQ, HEAD_DIM)
    d_w_key = jnp.dot(flat_hidden.T, dk_pre, preferred_element_type=jnp.float32)
    d_w_value = jnp.dot(flat_hidden.T, dv_pre, preferred_element_type=jnp.float32)
    dh_kv = jnp.dot(dk_pre, w_key.T, preferred_element_type=jnp.float32) + jnp.dot(dv_pre, w_value.T, preferred_element_type=jnp.float32)
    d_hidden = (dh_acc + dh_kv.reshape(BATCH, SEQ, D_MODEL)).astype(jnp.bfloat16)
    attn_out = out_acc.astype(jnp.bfloat16)
    return attn_out, d_hidden, d_w_query, d_w_key, d_w_value, d_w_out
```

```python
import jax
import jax.numpy as jnp
from jax import lax
from jax.experimental import pallas as pl
from jax.experimental.pallas import tpu as pltpu
from jax.sharding import PartitionSpec as P

ROPE_BASE = 10000.0
BLK = 128
TILE = 512
COLS = 256
F32 = jnp.float32
BF16 = jnp.bfloat16


def rope_tables(positions, head_dim):
    half_dim = head_dim // 2
    inv_freq = 1.0 / jnp.power(ROPE_BASE, jnp.arange(half_dim, dtype=F32) * (2.0 / head_dim))
    angles = positions.astype(F32)[:, None] * inv_freq[None, :]
    return jnp.cos(angles), jnp.sin(angles)


def rotate(rot_in, cos_tab, sin_tab):
    half_dim = rot_in.shape[-1] // 2
    low_half = rot_in[..., :half_dim]
    high_half = rot_in[..., half_dim:]
    return jnp.concatenate([low_half * cos_tab - high_half * sin_tab, high_half * cos_tab + low_half * sin_tab], axis=-1)


def unrotate(rot_in, cos_tab, sin_tab):
    return rotate(rot_in, cos_tab, -sin_tab)


def dot(a, b):
    return jnp.dot(a, b, preferred_element_type=F32)


def dot_ta(a, b):
    return lax.dot_general(a, b, (((0,), (0,)), ((), ())), preferred_element_type=F32)


def causal_mask(k_start, q_start, cols):
    k_pos = k_start + lax.broadcasted_iota(jnp.int32, (TILE, cols), 0)
    q_pos = q_start + lax.broadcasted_iota(jnp.int32, (TILE, cols), 1) % BLK
    return k_pos <= q_pos


def fwd_kernel(piece_ref, kv_ref, q_ref, o_ref, lse_ref, qt_scr, acc_scr, m_scr, l_scr):
    n_groups, n_cols, e_dim = q_ref.shape
    per_tile = TILE // BLK
    for grp in range(n_groups):
        piece = piece_ref[grp]
        qt_scr[...] = q_ref[grp].T
        acc_scr[...] = jnp.zeros_like(acc_scr)
        m_scr[...] = jnp.full_like(m_scr, -jnp.inf)
        l_scr[...] = jnp.zeros_like(l_scr)

        def tile_step(tile_idx, masked):
            row0 = pl.multiple_of(tile_idx * TILE, TILE)
            k_t = kv_ref[pl.ds(row0, TILE), :e_dim]
            v_t = kv_ref[pl.ds(row0, TILE), e_dim:]
            for c0 in range(0, n_cols, COLS):
                cs = slice(c0, c0 + COLS)
                s = dot(k_t, qt_scr[:, cs])
                if masked:
                    s = jnp.where(causal_mask(row0, piece * BLK, COLS), s, -jnp.inf)
                m_old = m_scr[:, cs]
                m_new = jnp.maximum(m_old, jnp.max(s, axis=0, keepdims=True))
                p = jnp.exp(s - m_new)
                alpha = jnp.exp(m_old - m_new)
                m_scr[:, cs] = m_new
                l_scr[:, cs] = l_scr[:, cs] * alpha + jnp.sum(p, axis=0, keepdims=True)
                acc_scr[:, cs] = acc_scr[:, cs] * alpha + dot_ta(v_t, p.astype(BF16))

        n_full = piece // per_tile

        def body(tile_idx, carry):
            tile_step(tile_idx, False)
            return carry

        lax.fori_loop(0, n_full, body, 0)
        tile_step(n_full, True)
        o_ref[grp] = (acc_scr[...] / l_scr[...]).T.astype(BF16)
        lse_ref[grp] = m_scr[...] + jnp.log(l_scr[...])


def bwd_kernel(piece_ref, kv_ref, q_ref, do_ref, o_ref, lse_ref, dq_ref, dkv_ref, qt_scr, dot_scr, dqt_scr, p_scr, ds_scr):
    n_groups, n_cols, e_dim = q_ref.shape
    per_tile = TILE // BLK
    dkv_ref[...] = jnp.zeros_like(dkv_ref)
    for grp in range(n_groups):
        piece = piece_ref[grp]
        qt_scr[...] = q_ref[grp].T
        dot_scr[...] = do_ref[grp].T
        dqt_scr[...] = jnp.zeros_like(dqt_scr)
        delta = jnp.sum(dot_scr[...].astype(F32) * o_ref[grp].T.astype(F32), axis=0, keepdims=True)

        def tile_step(tile_idx, masked):
            row0 = pl.multiple_of(tile_idx * TILE, TILE)
            k_t = kv_ref[pl.ds(row0, TILE), :e_dim]
            v_t = kv_ref[pl.ds(row0, TILE), e_dim:]
            for c0 in range(0, n_cols, COLS):
                cs = slice(c0, c0 + COLS)
                s = dot(k_t, qt_scr[:, cs])
                p = jnp.exp(s - lse_ref[grp, :, cs])
                if masked:
                    p = jnp.where(causal_mask(row0, piece * BLK, COLS), p, 0.0)
                d_p = dot(v_t, dot_scr[:, cs])
                p_scr[:, cs] = p.astype(BF16)
                ds_scr[:, cs] = (p * (d_p - delta[:, cs])).astype(BF16)
            rows = pl.ds(row0, TILE)
            dkv_ref[rows, :e_dim] += dot(ds_scr[...], q_ref[grp])
            dkv_ref[rows, e_dim:] += dot(p_scr[...], do_ref[grp])
            dqt_scr[...] += dot_ta(k_t, ds_scr[...])

        n_full = piece // per_tile

        def body(tile_idx, carry):
            tile_step(tile_idx, False)
            return carry

        lax.fori_loop(0, n_full, body, 0)
        tile_step(n_full, True)
        dq_ref[grp] = dqt_scr[...].T


def attention_forward(pieces, kv_all, q_grp):
    n_groups, n_cols, e_dim = q_grp.shape
    seq = kv_all.shape[0]
    vmem = pl.BlockSpec(memory_space=pltpu.VMEM)
    work = n_groups * n_cols * seq // 2
    return pl.pallas_call(
        fwd_kernel,
        out_shape=(jax.ShapeDtypeStruct(q_grp.shape, BF16), jax.ShapeDtypeStruct((n_groups, 1, n_cols), F32)),
        in_specs=[pl.BlockSpec(memory_space=pltpu.SMEM), vmem, vmem],
        out_specs=(vmem, vmem),
        scratch_shapes=[
            pltpu.VMEM((e_dim, n_cols), BF16),
            pltpu.VMEM((e_dim, n_cols), F32),
            pltpu.VMEM((1, n_cols), F32),
            pltpu.VMEM((1, n_cols), F32),
        ],
        compiler_params=pltpu.CompilerParams(vmem_limit_bytes=40 << 20),
        cost_estimate=pl.CostEstimate(flops=4 * work * e_dim, bytes_accessed=kv_all.size * 2, transcendentals=work),
        name="attn_fwd",
    )(pieces, kv_all, q_grp)


def attention_backward(pieces, kv_all, q_grp, do_grp, o_grp, lse):
    n_groups, n_cols, e_dim = q_grp.shape
    seq = kv_all.shape[0]
    vmem = pl.BlockSpec(memory_space=pltpu.VMEM)
    work = n_groups * n_cols * seq // 2
    return pl.pallas_call(
        bwd_kernel,
        out_shape=(jax.ShapeDtypeStruct(q_grp.shape, F32), jax.ShapeDtypeStruct((seq, 2 * e_dim), F32)),
        in_specs=[pl.BlockSpec(memory_space=pltpu.SMEM)] + [vmem] * 5,
        out_specs=(vmem, vmem),
        scratch_shapes=[
            pltpu.VMEM((e_dim, n_cols), BF16),
            pltpu.VMEM((e_dim, n_cols), BF16),
            pltpu.VMEM((e_dim, n_cols), F32),
            pltpu.VMEM((TILE, n_cols), BF16),
            pltpu.VMEM((TILE, n_cols), BF16),
        ],
        compiler_params=pltpu.CompilerParams(vmem_limit_bytes=48 << 20),
        cost_estimate=pl.CostEstimate(flops=10 * work * e_dim, bytes_accessed=kv_all.size * 6, transcendentals=work),
        name="attn_bwd",
    )(pieces, kv_all, q_grp, do_grp, o_grp, lse)


RING = 4
AXIS_STRIDE = (RING * RING, RING, 1)
ORDERS = ((0, 1, 2), (1, 2, 0), (2, 0, 1))
MESH = pl.DeviceIdType.MESH


def ring_of(axis):
    cp, tp = lax.axis_index("cp"), lax.axis_index("tp")
    stride = AXIS_STRIDE[axis]
    pos = (cp // stride) % RING
    right = cp + ((pos + 1) % RING - pos) * stride
    left = cp + ((pos + RING - 1) % RING - pos) * stride
    return pos, (tp, right), (tp, left)


def enter(with_partner=False):
    barrier = pltpu.get_barrier_semaphore()
    peers = []
    for axis in range(3):
        _, right, left = ring_of(axis)
        peers += [right, left]
    if with_partner:
        peers.append((1 - lax.axis_index("tp"), lax.axis_index("cp")))
    for peer in peers:
        pl.semaphore_signal(barrier, inc=1, device_id=peer, device_id_type=MESH)
    pl.semaphore_wait(barrier, len(peers))


def remote(src, dst, sems, idx, device):
    return pltpu.make_async_remote_copy(src_ref=src, dst_ref=dst, send_sem=sems[0].at[idx], recv_sem=sems[1].at[idx], device_id=device, device_id_type=MESH)


def add_rows(dst, dst0, srcs, n_rows, lanes):
    strip = next(s for s in (64, 48, 40, 32, 24, 16, 8) if n_rows % s == 0)
    if lanes[1] > 256:
        strip = next(s for s in (16, 8) if n_rows % s == 0)

    def body(i, carry):
        off = pl.multiple_of(dst0 + i * strip, 8)
        total = dst[pl.ds(off, strip), pl.ds(*lanes)]
        for ref, start in srcs:
            total = total + ref[pl.ds(pl.multiple_of(start + i * strip, 8), strip), :]
        dst[pl.ds(off, strip), pl.ds(*lanes)] = total
        return carry

    lax.fori_loop(0, n_rows // strip, body, 0)


class Part:
    def __init__(self, order, rb, sems, x=None, y=None, recv=None, row0=0, lanes=None, align=8):
        self.order, self.rb, self.sems, self.x, self.y, self.recv = order, rb, sems, x, y, recv
        self.row0, self.lanes, self.align = row0, lanes, align
        self.sent = []

    def view(self, ref, start, n_rows):
        return ref.at[pl.ds(pl.multiple_of(start, self.align), n_rows), pl.ds(*self.lanes)]

    def place(self, phase):
        base = self.row0
        for j in range(phase):
            base = base + ring_of(self.order[j])[0] * (self.rb * RING ** (2 - j))
        slab = self.rb * RING ** (2 - phase)
        h0 = -(-slab // (2 * self.align)) * self.align
        pos, right, left = ring_of(self.order[phase])
        starts = [base + ((pos + d) % RING) * slab for d in range(RING)]
        return slab, h0, slab - h0, starts, right, left

    def go(self, copy):
        copy.start()
        self.sent.append(copy)
        return copy

    def rs_start(self, phase):
        slab, h0, h1, (own, rgt, opp, lft), right, left = self.place(phase)
        buf, k = self.recv[phase], 10 * phase
        self.c = [
            self.go(remote(self.view(self.x, opp, h0), buf.at[pl.ds(0, h0)], self.sems, k, right)),
            self.go(remote(self.view(self.x, opp + h0, h1), buf.at[pl.ds(h0, h1)], self.sems, k + 1, left)),
            self.go(remote(self.view(self.x, rgt + h0, h1), buf.at[pl.ds(slab + h0, h1)], self.sems, k + 2, right)),
            self.go(remote(self.view(self.x, lft, h0), buf.at[pl.ds(2 * slab, h0)], self.sems, k + 3, left)),
        ]

    def rs_mid(self, phase):
        slab, h0, h1, (own, rgt, opp, lft), right, left = self.place(phase)
        buf, k = self.recv[phase], 10 * phase
        self.c[0].wait_recv()
        add_rows(self.x, rgt, [(buf, 0)], h0, self.lanes)
        self.c.append(self.go(remote(self.view(self.x, rgt, h0), buf.at[pl.ds(slab, h0)], self.sems, k + 4, right)))
        self.c[1].wait_recv()
        add_rows(self.x, lft + h0, [(buf, h0)], h1, self.lanes)
        self.c.append(self.go(remote(self.view(self.x, lft + h0, h1), buf.at[pl.ds(2 * slab + h0, h1)], self.sems, k + 5, left)))

    def rs_end(self, phase):
        slab, h0, h1, (own, rgt, opp, lft), right, left = self.place(phase)
        for copy in self.c[2:]:
            copy.wait_recv()
        buf = self.recv[phase]
        add_rows(self.x, own, [(buf, slab), (buf, 2 * slab)], slab, self.lanes)

    def ag_start(self, phase):
        slab, h0, h1, (own, rgt, opp, lft), right, left = self.place(phase)
        mine, k = self.view(self.y, own, slab), 10 * phase
        self.g = [
            self.go(remote(mine, mine, self.sems, k + 6, right)),
            self.go(remote(mine, mine, self.sems, k + 7, left)),
        ]

    def ag_mid(self, phase):
        slab, h0, h1, (own, rgt, opp, lft), right, left = self.place(phase)
        k = 10 * phase
        self.g[0].wait_recv()
        fwd = self.view(self.y, lft, h0)
        self.g.append(self.go(remote(fwd, fwd, self.sems, k + 8, right)))
        self.g[1].wait_recv()
        fwd = self.view(self.y, rgt + h0, h1)
        self.g.append(self.go(remote(fwd, fwd, self.sems, k + 9, left)))

    def ag_end(self, phase):
        self.g[2].wait_recv()
        self.g[3].wait_recv()

    def own_rows(self):
        return self.place(2)[3][0]

    def drain(self):
        for copy in self.sent:
            copy.wait_send()


def reduce_scatter(parts):
    for phase in range(3):
        for stage in ("rs_start", "rs_mid", "rs_end"):
            for part in parts:
                getattr(part, stage)(phase)


def all_gather(parts):
    for phase in (2, 1, 0):
        for stage in ("ag_start", "ag_mid", "ag_end"):
            for part in parts:
                getattr(part, stage)(phase)


def slab_rows(rb):
    return [3 * rb * RING ** (2 - phase) for phase in range(3)]


def place_in_order(block, order):
    digit = [(block // s) % RING for s in AXIS_STRIDE]
    return (digit[order[0]] * RING + digit[order[1]]) * RING + digit[order[2]]


def by_rows(n_rows, align):
    unit = n_rows // align
    counts = [(unit + 2 - c) // 3 for c in range(3)]
    starts = [sum(counts[:c]) * align for c in range(3)]
    return [(starts[c], counts[c] * align) for c in range(3)]


def pair(n):
    return [pltpu.SemaphoreType.DMA((n,)), pltpu.SemaphoreType.DMA((n,))]


def kv_gather_kernel(own_ref, all_ref, y0, y1, y2, s0, r0, s1, r1, s2, r2, out_sem):
    rows, lanes = own_ref.shape
    n_blk = RING ** 3
    split = by_rows(rows, 16)
    parts = []
    for c, (y, s, r) in enumerate(((y0, s0, r0), (y1, s1, r1), (y2, s2, r2))):
        part = Part(ORDERS[c], split[c][1], (s, r), y=y, lanes=(0, lanes), align=16)
        y[pl.ds(pl.multiple_of(part.own_rows(), 16), split[c][1]), :] = own_ref[pl.ds(*split[c]), :]
        parts.append(part)
    enter()
    all_gather(parts)

    def body(blk, carry):
        for c, y in enumerate((y0, y1, y2)):
            at, rb = split[c]
            src = y.at[pl.ds(pl.multiple_of(place_in_order(blk, ORDERS[c]) * rb, 16), rb)]
            pltpu.make_async_copy(src, all_ref.at[pl.ds(pl.multiple_of(blk * rows + at, 16), rb)], out_sem.at[c]).start()
        return carry

    lax.fori_loop(0, n_blk, body, 0)
    for c, y in enumerate((y0, y1, y2)):
        pltpu.make_async_copy(y, all_ref.at[pl.ds(0, n_blk * split[c][1])], out_sem.at[c]).wait()
    for part in parts:
        part.drain()


def kv_gather(own):
    rows, lanes = own.shape
    n_blk = RING ** 3
    split = by_rows(rows, 16)
    return pl.pallas_call(
        kv_gather_kernel,
        out_shape=jax.ShapeDtypeStruct((n_blk * rows, lanes), own.dtype),
        in_specs=[pl.BlockSpec(memory_space=pltpu.VMEM)],
        out_specs=pl.BlockSpec(memory_space=pl.ANY),
        scratch_shapes=[pltpu.VMEM((n_blk * rb, lanes), own.dtype) for _, rb in split] + pair(30) * 3 + [pltpu.SemaphoreType.DMA((3,))],
        compiler_params=pltpu.CompilerParams(collective_id=1, has_side_effects=True, vmem_limit_bytes=16 << 20),
        name="kv_gather",
    )(own)


def dkv_scatter_kernel(dkv_ref, out_ref, x0, x1, x2, *rest):
    recv, sems, in_sem = rest[:9], rest[9:15], rest[15]
    rows, lanes = out_ref.shape
    n_blk = RING ** 3
    split = by_rows(rows, 8)
    xs = (x0, x1, x2)
    parts = [Part(ORDERS[c], split[c][1], sems[2 * c:2 * c + 2], x=xs[c], recv=recv[3 * c:3 * c + 3], lanes=(0, lanes)) for c in range(3)]

    def body(blk, carry):
        for c in range(3):
            at, rb = split[c]
            dst = xs[c].at[pl.ds(pl.multiple_of(place_in_order(blk, ORDERS[c]) * rb, 8), rb)]
            pltpu.make_async_copy(dkv_ref.at[pl.ds(pl.multiple_of(blk * rows + at, 8), rb)], dst, in_sem.at[c]).start()
        return carry

    lax.fori_loop(0, n_blk, body, 0)
    enter()
    for c in range(3):
        pltpu.make_async_copy(dkv_ref.at[pl.ds(0, n_blk * split[c][1])], xs[c], in_sem.at[c]).wait()
    reduce_scatter(parts)
    for c in range(3):
        out_ref[pl.ds(*split[c]), :] = xs[c][pl.ds(pl.multiple_of(parts[c].own_rows(), 8), split[c][1]), :]
    for part in parts:
        part.drain()


def dkv_scatter(dkv):
    n_blk = RING ** 3
    rows, lanes = dkv.shape[0] // n_blk, dkv.shape[1]
    split = by_rows(rows, 8)
    return pl.pallas_call(
        dkv_scatter_kernel,
        out_shape=jax.ShapeDtypeStruct((rows, lanes), F32),
        in_specs=[pl.BlockSpec(memory_space=pl.ANY)],
        out_specs=pl.BlockSpec(memory_space=pltpu.VMEM),
        scratch_shapes=[pltpu.VMEM((n_blk * rb, lanes), F32) for _, rb in split]
        + [pltpu.VMEM((n, lanes), F32) for _, rb in split for n in slab_rows(rb)]
        + pair(30) * 3
        + [pltpu.SemaphoreType.DMA((3,))],
        compiler_params=pltpu.CompilerParams(collective_id=2, has_side_effects=True, vmem_limit_bytes=32 << 20),
        name="dkv_scatter",
    )(dkv)


def grad_sum_layout(d_model, n_local):
    n_blk = RING ** 3
    q_tiles = d_model * n_local // 8 // n_blk
    o_tiles = d_model // 128
    q_count = [q_tiles * 13 // 32, q_tiles * 11 // 32]
    q_count.append(q_tiles - sum(q_count))
    o_count = [o_tiles * 5 // 16, o_tiles * 6 // 16]
    o_count.append(o_tiles - sum(o_count))
    q_rows = [8 * n for n in q_count]
    q_first = [n_blk * sum(q_rows[:c]) for c in range(3)]
    o_lanes = [(128 * sum(o_count[:c]), 128 * o_count[c]) for c in range(3)]
    return q_rows, q_first, o_lanes


def grad_sum_kernel(hid_ref, grad_ref, dq_ref, o_ref, dkv_ref, gq_ref, go_ref, gk_ref, gv_ref, xq, xo, xk, yq, yo, yk, yp, tok_scr, *rest):
    n_parts = 7
    recv, sems, out_sem, swap_s, swap_r = rest[:3 * n_parts], rest[3 * n_parts:5 * n_parts], rest[-3], rest[-2], rest[-1]
    n_blk = RING ** 3
    n_tok, d_model = hid_ref.shape
    n_batch, n_local, block_len, head_dim = dq_ref.shape
    n_cols = n_local * head_dim
    q_rows, q_first, o_lanes = grad_sum_layout(d_model, n_local)
    parts = []
    for c in range(3):
        i = len(parts)
        parts.append(Part(ORDERS[c], q_rows[c], sems[2 * i:2 * i + 2], x=xq, y=yq, recv=recv[3 * i:3 * i + 3], row0=q_first[c], lanes=(0, 128)))
        i += 1
        parts.append(Part(ORDERS[c], n_cols // n_blk, sems[2 * i:2 * i + 2], x=xo, y=yo, recv=recv[3 * i:3 * i + 3], lanes=o_lanes[c]))
    i = 6
    parts.append(Part(ORDERS[2], d_model // n_blk, sems[2 * i:2 * i + 2], x=xk, y=yk, recv=recv[3 * i:3 * i + 3], lanes=(0, 128)))

    for b in range(n_batch):
        for h in range(n_local):
            tok_scr[pl.ds(b * block_len, block_len), pl.ds(h * head_dim, head_dim)] = dq_ref[b, h]
    d_tile = 256

    def q_body(i, carry):
        cols = pl.ds(pl.multiple_of(i * d_tile, d_tile), d_tile)
        hid_t = hid_ref[:, cols]
        res = dot_ta(hid_t, tok_scr[...])
        for h in range(n_local):
            xq[pl.ds(i * d_tile * n_local + h, d_tile, stride=n_local), :] = res[:, h * head_dim:(h + 1) * head_dim]
        xk[cols, :] = dot_ta(hid_t, dkv_ref[...])
        return carry

    lax.fori_loop(0, d_model // d_tile, q_body, 0)
    for b in range(n_batch):
        for h in range(n_local):
            tok_scr[pl.ds(b * block_len, block_len), pl.ds(h * head_dim, head_dim)] = o_ref[b, h]

    def o_body(i, carry):
        cols = pl.ds(pl.multiple_of(i * d_tile, d_tile), d_tile)
        xo[:, cols] = dot_ta(tok_scr[...], grad_ref[:, cols])
        return carry

    lax.fori_loop(0, d_model // d_tile, o_body, 0)

    enter(with_partner=True)
    reduce_scatter(parts)
    for part in parts:
        rows = pl.ds(pl.multiple_of(part.own_rows(), 8), part.rb)
        part.y[rows, pl.ds(*part.lanes)] = part.x[rows, pl.ds(*part.lanes)]
    all_gather(parts)
    partner = (1 - lax.axis_index("tp"), lax.axis_index("cp"))
    swap = pltpu.make_async_remote_copy(src_ref=yk, dst_ref=yp, send_sem=swap_s, recv_sem=swap_r, device_id=partner, device_id_type=MESH)
    swap.start()
    outs = [pltpu.make_async_copy(yq, gq_ref, out_sem.at[0]), pltpu.make_async_copy(yo, go_ref, out_sem.at[1])]
    for copy in outs:
        copy.start()
    swap.wait()
    first = lax.axis_index("tp") == 0

    @pl.when(first)
    def _():
        outs_k = [pltpu.make_async_copy(yk, gk_ref, out_sem.at[2]), pltpu.make_async_copy(yp, gv_ref, out_sem.at[3])]
        for copy in outs_k:
            copy.start()
        for copy in outs_k:
            copy.wait()

    @pl.when(jnp.logical_not(first))
    def _():
        outs_k = [pltpu.make_async_copy(yp, gk_ref, out_sem.at[2]), pltpu.make_async_copy(yk, gv_ref, out_sem.at[3])]
        for copy in outs_k:
            copy.start()
        for copy in outs_k:
            copy.wait()

    for copy in outs:
        copy.wait()
    for part in parts:
        part.drain()


def grad_sum(hid, grad, dq, o, dkv):
    n_tok, d_model = hid.shape
    n_batch, n_local, block_len, head_dim = dq.shape
    n_cols = n_local * head_dim
    n_blk = RING ** 3
    q_rows, _, o_lanes = grad_sum_layout(d_model, n_local)
    recv = []
    for c in range(3):
        recv += [pltpu.VMEM((n, 128), F32) for n in slab_rows(q_rows[c])]
        recv += [pltpu.VMEM((n, o_lanes[c][1]), F32) for n in slab_rows(n_cols // n_blk)]
    recv += [pltpu.VMEM((n, 128), F32) for n in slab_rows(d_model // n_blk)]
    vmem, anyspace = pl.BlockSpec(memory_space=pltpu.VMEM), pl.BlockSpec(memory_space=pl.ANY)
    xq, xo, xk = (pltpu.VMEM(s, F32) for s in ((d_model * n_local, 128), (n_cols, d_model), (d_model, 128)))
    return pl.pallas_call(
        grad_sum_kernel,
        out_shape=(
            jax.ShapeDtypeStruct((d_model * n_local, 128), F32),
            jax.ShapeDtypeStruct((n_cols, d_model), F32),
            jax.ShapeDtypeStruct((d_model, 128), F32),
            jax.ShapeDtypeStruct((d_model, 128), F32),
        ),
        in_specs=[vmem] * 5,
        out_specs=(anyspace,) * 4,
        scratch_shapes=[xq, xo, xk, xq, xo, xk, xk, pltpu.VMEM((n_tok, n_cols), BF16)] + recv + pair(30) * 7 + [pltpu.SemaphoreType.DMA((4,)), pltpu.SemaphoreType.DMA, pltpu.SemaphoreType.DMA],
        compiler_params=pltpu.CompilerParams(collective_id=3, has_side_effects=True, vmem_limit_bytes=67000000),
        name="grad_sum",
    )(hid, grad, dq, o, dkv)


def solution(mesh):
    cp_size = mesh.shape["cp"]
    half = cp_size // 2
    axes = ("tp", "cp")

    def flat(tp, cp):
        return tp * cp_size + cp

    route_a, route_b = [], []
    for cp in range(cp_size):
        mine, mirror = int(cp >= half), cp_size - 1 - cp
        route_b.append((flat(mine, cp), flat(1 - mine, cp)))
        route_b.append((flat(1 - mine, cp), flat(1 - mine, mirror)))
        route_a.append((flat(1 - mine, cp), flat(mine, mirror)))
    back_a = [(dst, src) for src, dst in route_a]
    back_b = [(dst, src) for src, dst in route_b]
    partner = [(0, 1), (1, 0)]

    def exchange(own_of, is_mine, plan_a, plan_b, send_a, send_b):
        got_a = lax.ppermute(send_a, axes, plan_a)
        got_b = lax.ppermute(send_b, axes, plan_b)
        return jnp.where(is_mine, own_of, got_b), jnp.where(is_mine, got_b, got_a)

    def local_program(hidden, grad_out, w_query, w_key, w_value, w_out):
        block_len = hidden.shape[1]
        n_local = w_query.shape[1]
        head_dim = w_key.shape[1]
        q_scale = head_dim ** -0.5
        cp_idx = lax.axis_index("cp")
        tp_idx = lax.axis_index("tp")
        is_mine = tp_idx == (cp_idx >= half).astype(jnp.int32)
        mirror_idx = cp_size - 1 - cp_idx
        pieces = jnp.stack([cp_idx, mirror_idx]).astype(jnp.int32)
        cos_tab, sin_tab = rope_tables(cp_idx * block_len + jnp.arange(block_len), head_dim)
        cos_mir, sin_mir = rope_tables(mirror_idx * block_len + jnp.arange(block_len), head_dim)
        cos_grp = jnp.stack([cos_tab, cos_mir])[:, None]
        sin_grp = jnp.stack([sin_tab, sin_mir])[:, None]

        def pick(pair, idx):
            return lax.dynamic_index_in_dim(pair, idx, 0, keepdims=False)

        def to_workers(x):
            own, other = pick(x, tp_idx), pick(x, 1 - tp_idx)
            return exchange(own, is_mine, route_a, route_b, other, jnp.where(is_mine, other, own))

        def to_homes(own_piece, mir_piece):
            mine, other = exchange(own_piece, is_mine, back_a, back_b, mir_piece, jnp.where(is_mine, mir_piece, own_piece))
            first = tp_idx == 0
            return jnp.stack([jnp.where(first, mine, other), jnp.where(first, other, mine)])

        def sum_over_tp(part, extra=None):
            total = pick(part, tp_idx) + lax.ppermute(pick(part, 1 - tp_idx), "tp", partner)
            if extra is not None:
                total = total + extra
            mine = total.astype(BF16)
            other = lax.ppermute(mine, "tp", partner)
            first = tp_idx == 0
            return jnp.stack([jnp.where(first, mine, other), jnp.where(first, other, mine)])

        hid_b = pick(hidden, tp_idx)
        key_loc = rotate(dot(hid_b, w_key), cos_tab, sin_tab).astype(BF16)
        val_loc = dot(hid_b, w_value).astype(BF16)
        kv_all = kv_gather(jnp.concatenate([key_loc, val_loc], axis=1))

        q_pre = jnp.einsum("bsd,dhe->bhse", hidden, w_query, preferred_element_type=F32)
        queries = (rotate(q_pre, cos_tab, sin_tab) * q_scale).astype(BF16)
        d_out = jnp.einsum("bsd,hed->bhse", grad_out, w_out, preferred_element_type=F32).astype(BF16)
        own_qd, mir_qd = to_workers(jnp.stack([queries, d_out], axis=1))
        grp_shape = (2, n_local * block_len, head_dim)
        q_grp = jnp.stack([own_qd[0], mir_qd[0]]).reshape(grp_shape)
        do_grp = jnp.stack([own_qd[1], mir_qd[1]]).reshape(grp_shape)

        o_grp, lse = attention_forward(pieces, kv_all, q_grp)
        o_split = o_grp.reshape(2, n_local, block_len, head_dim)
        attn_heads = to_homes(o_split[0], o_split[1])
        attn_out = sum_over_tp(jnp.einsum("cirf,ife->cre", attn_heads, w_out, preferred_element_type=F32))

        dq_grp, dkv = attention_backward(pieces, kv_all, q_grp, do_grp, o_grp, lse)
        dkv_loc = dkv_scatter(dkv)
        dq_rot = (unrotate(dq_grp.reshape(2, n_local, block_len, head_dim), cos_grp, sin_grp) * q_scale).astype(BF16)
        dq_pre = to_homes(dq_rot[0], dq_rot[1])
        dk_pre = unrotate(dkv_loc[:, :head_dim], cos_tab, sin_tab).astype(BF16)
        dv_pre = dkv_loc[:, head_dim:].astype(BF16)
        first = tp_idx == 0
        mine_kv = jnp.where(first, dk_pre, dv_pre)
        other_kv = lax.ppermute(jnp.where(first, dv_pre, dk_pre), "tp", partner)
        dkv_pair = jnp.concatenate([jnp.where(first, mine_kv, other_kv), jnp.where(first, other_kv, mine_kv)], axis=0)
        grad_q, grad_o, d_w_key, d_w_value = grad_sum(hidden.reshape(-1, hidden.shape[-1]), grad_out.reshape(-1, hidden.shape[-1]), dq_pre, attn_heads, dkv_pair)
        d_w_query = grad_q.reshape(w_query.shape)
        d_w_out = grad_o.reshape(w_out.shape)
        dh_kv = dot(dk_pre, w_key.T) + dot(dv_pre, w_value.T)
        d_hidden = sum_over_tp(jnp.einsum("cirf,eif->cre", dq_pre, w_query, preferred_element_type=F32), dh_kv)
        return attn_out, d_hidden, d_w_query, d_w_key, d_w_value, d_w_out

    row_spec = P(None, "cp", None)
    return jax.shard_map(local_program, mesh=mesh, in_specs=(row_spec, row_spec, P(None, "tp", None), P(), P(), P("tp", None, None)), out_specs=(row_spec, row_spec, P(None, "tp", None), P(), P(), P("tp", None, None)), check_vma=False)
```

```python
import jax
import jax.numpy as jnp
from jax import lax
from jax.experimental import pallas as pl
from jax.experimental.pallas import tpu as pltpu
from jax.sharding import PartitionSpec as P

ROPE_BASE = 10000.0
BLK = 128
TILE = 512
COLS = 256
F32 = jnp.float32
BF16 = jnp.bfloat16


def rope_tables(positions, head_dim):
    half_dim = head_dim // 2
    inv_freq = 1.0 / jnp.power(ROPE_BASE, jnp.arange(half_dim, dtype=F32) * (2.0 / head_dim))
    angles = positions.astype(F32)[:, None] * inv_freq[None, :]
    return jnp.cos(angles), jnp.sin(angles)


def rotate(rot_in, cos_tab, sin_tab):
    half_dim = rot_in.shape[-1] // 2
    low_half = rot_in[..., :half_dim]
    high_half = rot_in[..., half_dim:]
    return jnp.concatenate([low_half * cos_tab - high_half * sin_tab, high_half * cos_tab + low_half * sin_tab], axis=-1)


def unrotate(rot_in, cos_tab, sin_tab):
    return rotate(rot_in, cos_tab, -sin_tab)


def dot(a, b):
    return jnp.dot(a, b, preferred_element_type=F32)


def dot_ta(a, b):
    return lax.dot_general(a, b, (((0,), (0,)), ((), ())), preferred_element_type=F32)


def causal_mask(k_start, q_start, cols):
    k_pos = k_start + lax.broadcasted_iota(jnp.int32, (TILE, cols), 0)
    q_pos = q_start + lax.broadcasted_iota(jnp.int32, (TILE, cols), 1) % BLK
    return k_pos <= q_pos


def fwd_kernel(piece_ref, kv_ref, q_ref, o_ref, lse_ref, qt_scr, acc_scr, m_scr, l_scr):
    n_groups, n_cols, e_dim = q_ref.shape
    per_tile = TILE // BLK
    for grp in range(n_groups):
        piece = piece_ref[grp]
        qt_scr[...] = q_ref[grp].T
        acc_scr[...] = jnp.zeros_like(acc_scr)
        m_scr[...] = jnp.full_like(m_scr, -jnp.inf)
        l_scr[...] = jnp.zeros_like(l_scr)

        def tile_step(tile_idx, masked):
            row0 = pl.multiple_of(tile_idx * TILE, TILE)
            k_t = kv_ref[pl.ds(row0, TILE), :e_dim]
            v_t = kv_ref[pl.ds(row0, TILE), e_dim:]
            for c0 in range(0, n_cols, COLS):
                cs = slice(c0, c0 + COLS)
                s = dot(k_t, qt_scr[:, cs])
                if masked:
                    s = jnp.where(causal_mask(row0, piece * BLK, COLS), s, -jnp.inf)
                m_old = m_scr[:, cs]
                m_new = jnp.maximum(m_old, jnp.max(s, axis=0, keepdims=True))
                p = jnp.exp(s - m_new)
                alpha = jnp.exp(m_old - m_new)
                m_scr[:, cs] = m_new
                l_scr[:, cs] = l_scr[:, cs] * alpha + jnp.sum(p, axis=0, keepdims=True)
                acc_scr[:, cs] = acc_scr[:, cs] * alpha + dot_ta(v_t, p.astype(BF16))

        n_full = piece // per_tile

        def body(tile_idx, carry):
            tile_step(tile_idx, False)
            return carry

        lax.fori_loop(0, n_full, body, 0)
        tile_step(n_full, True)
        o_ref[grp] = (acc_scr[...] / l_scr[...]).T.astype(BF16)
        lse_ref[grp] = m_scr[...] + jnp.log(l_scr[...])


def attention_forward(pieces, kv_all, q_grp):
    n_groups, n_cols, e_dim = q_grp.shape
    seq = kv_all.shape[0]
    vmem = pl.BlockSpec(memory_space=pltpu.VMEM)
    work = n_groups * n_cols * seq // 2
    return pl.pallas_call(
        fwd_kernel,
        out_shape=(jax.ShapeDtypeStruct(q_grp.shape, BF16), jax.ShapeDtypeStruct((n_groups, 1, n_cols), F32)),
        in_specs=[pl.BlockSpec(memory_space=pltpu.SMEM), vmem, vmem],
        out_specs=(vmem, vmem),
        scratch_shapes=[
            pltpu.VMEM((e_dim, n_cols), BF16),
            pltpu.VMEM((e_dim, n_cols), F32),
            pltpu.VMEM((1, n_cols), F32),
            pltpu.VMEM((1, n_cols), F32),
        ],
        compiler_params=pltpu.CompilerParams(vmem_limit_bytes=40 << 20),
        cost_estimate=pl.CostEstimate(flops=4 * work * e_dim, bytes_accessed=kv_all.size * 2, transcendentals=work),
        name="attn_fwd",
    )(pieces, kv_all, q_grp)


RING = 4
AXIS_STRIDE = (RING * RING, RING, 1)
ORDERS = ((0, 1, 2), (1, 2, 0), (2, 0, 1))
MESH = pl.DeviceIdType.MESH


def ring_of(axis):
    cp, tp = lax.axis_index("cp"), lax.axis_index("tp")
    stride = AXIS_STRIDE[axis]
    pos = (cp // stride) % RING
    right = cp + ((pos + 1) % RING - pos) * stride
    left = cp + ((pos + RING - 1) % RING - pos) * stride
    return pos, (tp, right), (tp, left)


def enter(rings, with_partner=False, with_mirror=False):
    barrier = pltpu.get_barrier_semaphore()
    peers = []
    for _, right, left in rings:
        peers += [right, left]
    if with_partner:
        peers.append((1 - lax.axis_index("tp"), lax.axis_index("cp")))
    if with_mirror:
        mirror = RING ** 3 - 1 - lax.axis_index("cp")
        peers += [(0, mirror), (1, mirror)]
    for peer in peers:
        pl.semaphore_signal(barrier, inc=1, device_id=peer, device_id_type=MESH)
    pl.semaphore_wait(barrier, len(peers))


def remote(src, dst, sems, idx, device):
    return pltpu.make_async_remote_copy(src_ref=src, dst_ref=dst, send_sem=sems[0].at[idx], recv_sem=sems[1].at[idx], device_id=device, device_id_type=MESH)


def add_rows(dst, dst0, srcs, n_rows, lanes):
    strip = next(s for s in (64, 48, 40, 32, 24, 16, 8) if n_rows % s == 0)
    if lanes[1] > 256:
        strip = next(s for s in (16, 8) if n_rows % s == 0)

    def body(i, carry):
        off = pl.multiple_of(dst0 + i * strip, 8)
        total = dst[pl.ds(off, strip), pl.ds(*lanes)]
        for ref, start in srcs:
            total = total + ref[pl.ds(pl.multiple_of(start + i * strip, 8), strip), :]
        dst[pl.ds(off, strip), pl.ds(*lanes)] = total
        return carry

    lax.fori_loop(0, n_rows // strip, body, 0)


class Part:
    def __init__(self, rings, order, rb, sems, x=None, y=None, recv=None, row0=0, lanes=None, align=8):
        self.rb, self.sems, self.x, self.y, self.recv = rb, sems, x, y, recv
        self.row0, self.lanes, self.align = row0, lanes, align
        self.places = []
        base = row0
        for phase in range(3):
            slab = rb * RING ** (2 - phase)
            h0 = -(-slab // (2 * align)) * align
            pos, right, left = rings[order[phase]]
            starts = [base + ((pos + d) % RING) * slab for d in range(RING)]
            self.places.append((slab, h0, slab - h0, starts, right, left))
            base = starts[0]

    def view(self, ref, start, n_rows):
        return ref.at[pl.ds(pl.multiple_of(start, self.align), n_rows), pl.ds(*self.lanes)]

    def place(self, phase):
        return self.places[phase]

    def hop(self, phase, i):
        slab, h0, h1, (own, rgt, opp, lft), right, left = self.place(phase)
        if i < 6:
            start, n_rows, at, device = (
                (opp, h0, 0, right),
                (opp + h0, h1, h0, left),
                (rgt + h0, h1, slab + h0, right),
                (lft, h0, 2 * slab, left),
                (rgt, h0, slab, right),
                (lft + h0, h1, 2 * slab + h0, left),
            )[i]
            src, dst = self.view(self.x, start, n_rows), self.recv[phase].at[pl.ds(at, n_rows)]
        else:
            start, n_rows, device = ((own, slab, right), (own, slab, left), (lft, h0, right), (rgt + h0, h1, left))[i - 6]
            src = dst = self.view(self.y, start, n_rows)
        return remote(src, dst, self.sems, 10 * phase + i, device)

    def rs_start(self, phase):
        for i in range(4):
            self.hop(phase, i).start()

    def rs_mid(self, phase):
        slab, h0, h1, (own, rgt, opp, lft), _, _ = self.place(phase)
        buf = self.recv[phase]
        self.hop(phase, 0).wait_recv()
        add_rows(self.x, rgt, [(buf, 0)], h0, self.lanes)
        self.hop(phase, 4).start()
        self.hop(phase, 1).wait_recv()
        add_rows(self.x, lft + h0, [(buf, h0)], h1, self.lanes)
        self.hop(phase, 5).start()

    def rs_end(self, phase):
        slab, _, _, (own, _, _, _), _, _ = self.place(phase)
        for i in range(2, 6):
            self.hop(phase, i).wait_recv()
        buf = self.recv[phase]
        add_rows(self.x, own, [(buf, slab), (buf, 2 * slab)], slab, self.lanes)

    def ag_start(self, phase):
        self.hop(phase, 6).start()
        self.hop(phase, 7).start()

    def ag_mid(self, phase):
        self.hop(phase, 6).wait_recv()
        self.hop(phase, 8).start()
        self.hop(phase, 7).wait_recv()
        self.hop(phase, 9).start()

    def ag_end(self, phase):
        self.hop(phase, 8).wait_recv()
        self.hop(phase, 9).wait_recv()

    def own_rows(self):
        return self.place(2)[3][0]

    def drain(self, first=0, last=10):
        for phase in range(3):
            for i in range(first, last):
                self.hop(phase, i).wait_send()


def stage(parts, name, phase):
    for part in parts:
        getattr(part, name)(phase)


def reduce_scatter(parts):
    for phase in range(3):
        for name in ("rs_start", "rs_mid", "rs_end"):
            stage(parts, name, phase)


def all_gather(parts):
    for phase in (2, 1, 0):
        for name in ("ag_start", "ag_mid", "ag_end"):
            stage(parts, name, phase)


def slab_rows(rb):
    return [3 * rb * RING ** (2 - phase) for phase in range(3)]


def place_in_order(block, order):
    digit = [(block // s) % RING for s in AXIS_STRIDE]
    return (digit[order[0]] * RING + digit[order[1]]) * RING + digit[order[2]]


def by_rows(n_rows, align):
    unit = n_rows // align
    counts = [(unit + 2 - c) // 3 for c in range(3)]
    starts = [sum(counts[:c]) * align for c in range(3)]
    return [(starts[c], counts[c] * align) for c in range(3)]


def pair(n):
    return [pltpu.SemaphoreType.DMA((n,)), pltpu.SemaphoreType.DMA((n,))]


def kv_gather_kernel(own_ref, all_ref, y0, y1, y2, s0, r0, s1, r1, s2, r2, out_sem):
    rows, lanes = own_ref.shape
    n_blk = RING ** 3
    split = by_rows(rows, 16)
    parts = []
    rings = [ring_of(axis) for axis in range(3)]
    for c, (y, s, r) in enumerate(((y0, s0, r0), (y1, s1, r1), (y2, s2, r2))):
        part = Part(rings, ORDERS[c], split[c][1], (s, r), y=y, lanes=(0, lanes), align=16)
        y[pl.ds(pl.multiple_of(part.own_rows(), 16), split[c][1]), :] = own_ref[pl.ds(*split[c]), :]
        parts.append(part)
    enter(rings)
    all_gather(parts)

    def body(blk, carry):
        for c, y in enumerate((y0, y1, y2)):
            at, rb = split[c]
            src = y.at[pl.ds(pl.multiple_of(place_in_order(blk, ORDERS[c]) * rb, 16), rb)]
            pltpu.make_async_copy(src, all_ref.at[pl.ds(pl.multiple_of(blk * rows + at, 16), rb)], out_sem.at[c]).start()
        return carry

    lax.fori_loop(0, n_blk, body, 0)
    for c, y in enumerate((y0, y1, y2)):
        pltpu.make_async_copy(y, all_ref.at[pl.ds(0, n_blk * split[c][1])], out_sem.at[c]).wait()
    for part in parts:
        part.drain(6, 10)


def kv_gather(own):
    rows, lanes = own.shape
    n_blk = RING ** 3
    split = by_rows(rows, 16)
    return pl.pallas_call(
        kv_gather_kernel,
        out_shape=jax.ShapeDtypeStruct((n_blk * rows, lanes), own.dtype),
        in_specs=[pl.BlockSpec(memory_space=pltpu.VMEM)],
        out_specs=pl.BlockSpec(memory_space=pl.ANY),
        scratch_shapes=[pltpu.VMEM((n_blk * rb, lanes), own.dtype) for _, rb in split] + pair(30) * 3 + [pltpu.SemaphoreType.DMA((3,))],
        compiler_params=pltpu.CompilerParams(collective_id=1, has_side_effects=True, vmem_limit_bytes=16 << 20),
        name="kv_gather",
    )(own)


def grad_layout(d_model, n_local):
    n_blk = RING ** 3
    q_tiles = d_model * n_local // 8 // n_blk
    o_tiles = d_model // 128
    q_count = [q_tiles * 13 // 32, q_tiles * 11 // 32]
    q_count.append(q_tiles - sum(q_count))
    o_count = [o_tiles * 5 // 16, o_tiles * 6 // 16]
    o_count.append(o_tiles - sum(o_count))
    q_rows = [8 * n for n in q_count]
    q_first = [n_blk * sum(q_rows[:c]) for c in range(3)]
    o_lanes = [(128 * sum(o_count[:c]), 128 * o_count[c]) for c in range(3)]
    return q_rows, q_first, o_lanes


def place_heads(dst, src):
    n_batch, n_local, block_len, head_dim = src.shape
    for b in range(n_batch):
        for h in range(n_local):
            dst[pl.ds(b * block_len, block_len), pl.ds(h * head_dim, head_dim)] = src[b, h]


D_TILE = 256


def bwd_kernel(kv_ref, q_ref, do_ref, o_ref, lse_ref, home_ref, grad_ref, cos_ref, sin_ref, dq_ref, dkv_ref, red0, red1, red2, qt_scr, dot_scr, dqt_scr, delta_scr, p_scr, ds_scr, xo, tok_scr, rot_scr, dqh_scr, *rest):
    recv, sems, ex_s, ex_r = rest[:9], rest[9:15], rest[15], rest[16]
    n_groups, n_cols, e_dim = q_ref.shape
    per_tile = TILE // BLK
    n_blk = RING ** 3
    d_model = grad_ref.shape[1]
    n_local, block_len = rot_scr.shape[1], rot_scr.shape[2]
    cp, tp = lax.axis_index("cp"), lax.axis_index("tp")
    mirror = n_blk - 1 - cp
    rings = [ring_of(axis) for axis in range(3)]
    group = cp // (n_blk // 2)
    _, _, o_lanes = grad_layout(d_model, n_local)
    parts = [Part(rings, ORDERS[c], n_cols // n_blk, sems[2 * c:2 * c + 2], x=xo, recv=recv[3 * c:3 * c + 3], lanes=o_lanes[c]) for c in range(3)]

    place_heads(tok_scr, home_ref)

    def o_body(i, carry):
        cols = pl.ds(pl.multiple_of(i * D_TILE, D_TILE), D_TILE)
        xo[:, cols] = dot_ta(tok_scr[...], grad_ref[:, cols])
        return carry

    lax.fori_loop(0, d_model // D_TILE, o_body, 0)
    enter(rings, with_partner=True, with_mirror=True)
    stage(parts, "rs_start", 0)

    for grp in range(n_groups):
        qt_scr[grp] = q_ref[grp].T
        dot_scr[grp] = do_ref[grp].T
        delta_scr[grp] = jnp.sum(dot_scr[grp].astype(F32) * o_ref[grp].T.astype(F32), axis=0, keepdims=True)
    dqt_scr[...] = jnp.zeros_like(dqt_scr)
    dkv_ref[...] = jnp.zeros_like(dkv_ref)

    def tile_step(grp, tile_idx, piece, masked):
        row0 = pl.multiple_of(tile_idx * TILE, TILE)
        k_t = kv_ref[pl.ds(row0, TILE), :e_dim]
        v_t = kv_ref[pl.ds(row0, TILE), e_dim:]
        for c0 in range(0, n_cols, COLS):
            cs = slice(c0, c0 + COLS)
            s = dot(k_t, qt_scr[grp, :, cs])
            p = jnp.exp(s - lse_ref[grp, :, cs])
            if masked:
                p = jnp.where(causal_mask(row0, piece * BLK, COLS), p, 0.0)
            d_p = dot(v_t, dot_scr[grp, :, cs])
            p_scr[:, cs] = p.astype(BF16)
            ds_scr[:, cs] = (p * (d_p - delta_scr[grp, :, cs])).astype(BF16)
        rows = pl.ds(row0, TILE)
        dkv_ref[rows, :e_dim] += dot(ds_scr[...], q_ref[grp])
        dkv_ref[rows, e_dim:] += dot(p_scr[...], do_ref[grp])
        dqt_scr[grp] += dot_ta(k_t, ds_scr[...])

    n_first = cp // per_tile + 1
    n_steps = n_blk // per_tile + 1

    def body(t, carry):
        grp = (t - n_first + n_steps) // n_steps
        piece = cp + grp * (mirror - cp)
        tile_idx = t - grp * n_first
        last = tile_idx == piece // per_tile

        @pl.when(jnp.logical_not(last))
        def _():
            tile_step(grp, tile_idx, piece, False)

        @pl.when(last)
        def _():
            tile_step(grp, tile_idx, piece, True)

        @pl.when(t == 5)
        def _():
            stage(parts, "rs_mid", 0)

        @pl.when(t == 13)
        def _():
            stage(parts, "rs_end", 0)
            stage(parts, "rs_start", 1)

        return carry

    lax.fori_loop(0, n_steps, body, 0)
    stage(parts, "rs_mid", 1)

    scale = e_dim ** -0.5
    half_dim = e_dim // 2
    for grp in range(n_groups):
        cos_t, sin_t = cos_ref[grp], sin_ref[grp]
        for h in range(n_local):
            cols = slice(h * block_len, (h + 1) * block_len)
            low, high = dqt_scr[grp, :half_dim, cols], dqt_scr[grp, half_dim:, cols]
            turned = jnp.concatenate([low * cos_t + high * sin_t, high * cos_t - low * sin_t], axis=0) * scale
            rot_scr[grp, h] = turned.T.astype(BF16)
    is_mine = tp == group

    def give(piece_idx, sem, device):
        return pltpu.make_async_remote_copy(src_ref=rot_scr.at[piece_idx], dst_ref=dqh_scr.at[tp], send_sem=ex_s.at[sem], recv_sem=ex_r.at[tp], device_id=device, device_id_type=MESH)

    def take(batch):
        return pltpu.make_async_remote_copy(src_ref=rot_scr.at[0], dst_ref=dqh_scr.at[batch], send_sem=ex_s.at[0], recv_sem=ex_r.at[batch], device_id=(group, mirror), device_id_type=MESH)

    give(1, 1, (group, mirror)).start()

    @pl.when(jnp.logical_not(is_mine))
    def _():
        give(0, 0, (1 - tp, cp)).start()

    @pl.when(is_mine)
    def _():
        dqh_scr[tp] = rot_scr[0]

    stage(parts, "rs_end", 1)
    for name in ("rs_start", "rs_mid", "rs_end"):
        stage(parts, name, 2)
    for part, out, lanes in zip(parts, (red0, red1, red2), o_lanes):
        out[...] = xo[pl.ds(pl.multiple_of(part.own_rows(), 8), part.rb), pl.ds(*lanes)]
    take(1 - tp).wait_recv()

    @pl.when(jnp.logical_not(is_mine))
    def _():
        take(tp).wait_recv()
        give(0, 0, (1 - tp, cp)).wait_send()

    give(1, 1, (group, mirror)).wait_send()
    dq_ref[...] = dqh_scr[...]
    for part in parts:
        part.drain(0, 6)


def attention_backward(kv_all, q_grp, do_grp, o_grp, lse, o_home, grad, cos_t, sin_t):
    n_groups, n_cols, e_dim = q_grp.shape
    n_tok, d_model = grad.shape
    n_blk = RING ** 3
    seq = kv_all.shape[0]
    _, _, o_lanes = grad_layout(d_model, o_home.shape[1])
    rb = n_cols // n_blk
    vmem = pl.BlockSpec(memory_space=pltpu.VMEM)
    return pl.pallas_call(
        bwd_kernel,
        out_shape=(jax.ShapeDtypeStruct(o_home.shape, BF16), jax.ShapeDtypeStruct((seq, 2 * e_dim), F32)) + tuple(jax.ShapeDtypeStruct((rb, n), F32) for _, n in o_lanes),
        in_specs=[vmem] * 9,
        out_specs=(vmem,) * 5,
        scratch_shapes=[
            pltpu.VMEM((n_groups, e_dim, n_cols), BF16),
            pltpu.VMEM((n_groups, e_dim, n_cols), BF16),
            pltpu.VMEM((n_groups, e_dim, n_cols), F32),
            pltpu.VMEM((n_groups, 1, n_cols), F32),
            pltpu.VMEM((TILE, n_cols), BF16),
            pltpu.VMEM((TILE, n_cols), BF16),
            pltpu.VMEM((n_cols, d_model), F32),
            pltpu.VMEM((n_tok, n_cols), BF16),
            pltpu.VMEM(o_home.shape, BF16),
            pltpu.VMEM(o_home.shape, BF16),
        ]
        + [pltpu.VMEM((n, lanes), F32) for _, lanes in o_lanes for n in slab_rows(rb)]
        + pair(30) * 3
        + pair(2),
        compiler_params=pltpu.CompilerParams(collective_id=2, has_side_effects=True, vmem_limit_bytes=60 << 20),
        name="attn_bwd",
    )(kv_all, q_grp, do_grp, o_grp, lse, o_home, grad, cos_t, sin_t)


def grad_kernel(dkv_ref, hid_ref, dqh_ref, red0, red1, red2, cos_ref, sin_ref, gq_ref, go_ref, gk_ref, gv_ref, dkd_ref, x0, x1, x2, xq, xk, yq, yo, yk, yp, tok_scr, mine_scr, give_scr, got_scr, *rest):
    n_parts = 10
    recv, sems, in_sem, out_sem, swap_s, swap_r = rest[:21], rest[21:21 + 2 * n_parts], rest[-4], rest[-3], rest[-2], rest[-1]
    n_blk = RING ** 3
    n_tok, d_model = hid_ref.shape
    n_batch, n_local, block_len, head_dim = dqh_ref.shape
    n_cols = n_local * head_dim
    rows, lanes = block_len, 2 * head_dim
    q_rows, q_first, o_lanes = grad_layout(d_model, n_local)
    split = by_rows(rows, 8)
    tp, cp = lax.axis_index("tp"), lax.axis_index("cp")
    partner = (1 - tp, cp)
    xs = (x0, x1, x2)
    rings = [ring_of(axis) for axis in range(3)]

    def sem(i):
        return sems[2 * i:2 * i + 2]

    p_d = [Part(rings, ORDERS[c], split[c][1], sem(c), x=xs[c], recv=recv[3 * c:3 * c + 3], lanes=(0, lanes)) for c in range(3)]
    p_q = [Part(rings, ORDERS[c], q_rows[c], sem(3 + c), x=xq, y=yq, recv=recv[9 + 3 * c:12 + 3 * c], row0=q_first[c], lanes=(0, 128)) for c in range(3)]
    p_o = [Part(rings, ORDERS[c], n_cols // n_blk, sem(6 + c), y=yo, lanes=o_lanes[c]) for c in range(3)]
    p_k = Part(rings, ORDERS[2], d_model // n_blk, sem(9), x=xk, y=yk, recv=recv[18:21], lanes=(0, 128))
    p_qo = p_q + p_o

    def load(blk, carry):
        for c in range(3):
            at, rb = split[c]
            dst = xs[c].at[pl.ds(pl.multiple_of(place_in_order(blk, ORDERS[c]) * rb, 8), rb)]
            pltpu.make_async_copy(dkv_ref.at[pl.ds(pl.multiple_of(blk * rows + at, 8), rb)], dst, in_sem.at[c]).start()
        return carry

    lax.fori_loop(0, n_blk, load, 0)
    enter(rings, with_partner=True)
    for c in range(3):
        pltpu.make_async_copy(dkv_ref.at[pl.ds(0, n_blk * split[c][1])], xs[c], in_sem.at[c]).wait()
        p_d[c].rs_start(0)

    place_heads(tok_scr, dqh_ref)

    def q_body(i, carry):
        cols = pl.ds(pl.multiple_of(i * D_TILE, D_TILE), D_TILE)
        res = dot_ta(hid_ref[:, cols], tok_scr[...])
        for h in range(n_local):
            xq[pl.ds(i * D_TILE * n_local + h, D_TILE, stride=n_local), :] = res[:, h * head_dim:(h + 1) * head_dim]
        return carry

    lax.fori_loop(0, d_model // D_TILE, q_body, 0)
    stage(p_d, "rs_mid", 0)
    stage(p_q, "rs_start", 0)
    for part, red in zip(p_o, (red0, red1, red2)):
        part.y[pl.ds(pl.multiple_of(part.own_rows(), 8), part.rb), pl.ds(*part.lanes)] = red[...]
    stage(p_d, "rs_end", 0)
    stage(p_d, "rs_start", 1)
    stage(p_q, "rs_mid", 0)
    stage(p_d, "rs_mid", 1)
    stage(p_d, "rs_end", 1)
    stage(p_d, "rs_start", 2)
    stage(p_q, "rs_end", 0)
    stage(p_q, "rs_start", 1)
    stage(p_d, "rs_mid", 2)
    stage(p_d, "rs_end", 2)

    half_dim = head_dim // 2
    first = tp == 0
    for c in range(3):
        at, rb = split[c]
        own = xs[c][pl.ds(pl.multiple_of(p_d[c].own_rows(), 8), rb), :]
        cos_tab, sin_tab = cos_ref[pl.ds(at, rb), :], sin_ref[pl.ds(at, rb), :]
        low, high = own[:, :half_dim], own[:, half_dim:head_dim]
        mine_scr[pl.ds(at, rb), :head_dim] = jnp.concatenate([low * cos_tab + high * sin_tab, high * cos_tab - low * sin_tab], axis=1)
        mine_scr[pl.ds(at, rb), head_dim:] = own[:, head_dim:]
    both = mine_scr[...].astype(BF16)
    dkd_ref[...] = both
    dk_new, dv_new = both[:, :head_dim], both[:, head_dim:]
    give_scr[...] = jnp.where(first, dv_new, dk_new)
    keep = jnp.where(first, dk_new, dv_new)
    swap_small = pltpu.make_async_remote_copy(src_ref=give_scr, dst_ref=got_scr, send_sem=swap_s.at[0], recv_sem=swap_r.at[0], device_id=partner, device_id_type=MESH)
    swap_small.start()
    stage(p_q, "rs_mid", 1)
    swap_small.wait()
    got = got_scr[...]
    kv_tok = jnp.concatenate([jnp.where(first, keep, got), jnp.where(first, got, keep)], axis=0)
    for i in range(d_model // D_TILE):
        xk[pl.ds(i * D_TILE, D_TILE), :] = dot_ta(hid_ref[:, i * D_TILE:(i + 1) * D_TILE], kv_tok)
    p_k.rs_start(0)
    stage(p_q, "rs_end", 1)
    stage(p_q, "rs_start", 2)
    p_k.rs_mid(0)
    stage(p_q, "rs_mid", 2)
    p_k.rs_end(0)
    p_k.rs_start(1)
    stage(p_q, "rs_end", 2)
    for part in p_q:
        own = pl.ds(pl.multiple_of(part.own_rows(), 8), part.rb)
        yq[own, :] = xq[own, :]
    stage(p_qo, "ag_start", 2)
    p_k.rs_mid(1)
    stage(p_qo, "ag_mid", 2)
    p_k.rs_end(1)
    p_k.rs_start(2)
    stage(p_qo, "ag_end", 2)
    stage(p_qo, "ag_start", 1)
    p_k.rs_mid(2)
    stage(p_qo, "ag_mid", 1)
    p_k.rs_end(2)
    own = pl.ds(pl.multiple_of(p_k.own_rows(), 8), p_k.rb)
    yk[own, :] = xk[own, :]
    p_k.ag_start(2)
    stage(p_qo, "ag_end", 1)
    p_k.ag_mid(2)
    p_k.ag_end(2)
    for name in ("ag_start", "ag_mid", "ag_end"):
        getattr(p_k, name)(1)
    p_all = p_qo + [p_k]
    stage(p_all, "ag_start", 0)

    def put(part, which):
        out = gq_ref if part.y is yq else go_ref
        slab, _, _, starts, _, _ = part.place(0)
        src, dst = part.view(part.y, starts[which], slab), part.view(out, starts[which], slab)
        pltpu.make_async_copy(src, dst, out_sem.at[p_qo.index(part)]).start()

    for part in p_qo:
        put(part, 0)
    stage(p_all, "ag_mid", 0)
    for part in p_qo:
        put(part, 1)
        put(part, 3)
    p_k.ag_end(0)
    swap = pltpu.make_async_remote_copy(src_ref=yk, dst_ref=yp, send_sem=swap_s.at[1], recv_sem=swap_r.at[1], device_id=partner, device_id_type=MESH)
    swap.start()
    for part in p_qo:
        part.ag_end(0)
        put(part, 2)
    swap.wait()

    def put_kv(k_src, v_src):
        outs = [pltpu.make_async_copy(k_src, gk_ref, out_sem.at[6]), pltpu.make_async_copy(v_src, gv_ref, out_sem.at[7])]
        for copy in outs:
            copy.start()
        for copy in outs:
            copy.wait()

    @pl.when(first)
    def _():
        put_kv(yk, yp)

    @pl.when(jnp.logical_not(first))
    def _():
        put_kv(yp, yk)

    for i, part in enumerate(p_qo):
        out = gq_ref if part.y is yq else go_ref
        span = n_blk * part.rb
        pltpu.make_async_copy(part.view(part.y, part.row0, span), part.view(out, part.row0, span), out_sem.at[i]).wait()
    for part in p_d:
        part.drain(0, 6)
    for part in p_q + [p_k]:
        part.drain(0, 10)
    for part in p_o:
        part.drain(6, 10)


def grad_sums(dkv, hid, dq_home, reds, cos_tab, sin_tab):
    n_tok, d_model = hid.shape
    n_batch, n_local, block_len, head_dim = dq_home.shape
    n_cols = n_local * head_dim
    n_blk = RING ** 3
    lanes = 2 * head_dim
    q_rows, _, _ = grad_layout(d_model, n_local)
    split = by_rows(block_len, 8)
    recv = [pltpu.VMEM((n, lanes), F32) for _, rb in split for n in slab_rows(rb)]
    recv += [pltpu.VMEM((n, 128), F32) for rb in q_rows for n in slab_rows(rb)]
    recv += [pltpu.VMEM((n, 128), F32) for n in slab_rows(d_model // n_blk)]
    vmem, anyspace = pl.BlockSpec(memory_space=pltpu.VMEM), pl.BlockSpec(memory_space=pl.ANY)
    xq, xo, xk = (pltpu.VMEM(s, F32) for s in ((d_model * n_local, 128), (n_cols, d_model), (d_model, 128)))
    small = pltpu.VMEM((block_len, head_dim), BF16)
    return pl.pallas_call(
        grad_kernel,
        out_shape=(
            jax.ShapeDtypeStruct((d_model * n_local, 128), F32),
            jax.ShapeDtypeStruct((n_cols, d_model), F32),
            jax.ShapeDtypeStruct((d_model, 128), F32),
            jax.ShapeDtypeStruct((d_model, 128), F32),
            jax.ShapeDtypeStruct((block_len, lanes), BF16),
        ),
        in_specs=[anyspace] + [vmem] * 7,
        out_specs=(anyspace,) * 4 + (vmem,),
        scratch_shapes=[pltpu.VMEM((n_blk * rb, lanes), F32) for _, rb in split]
        + [xq, xk, xq, xo, xk, xk, pltpu.VMEM((n_tok, n_cols), BF16), pltpu.VMEM((block_len, lanes), F32), small, small]
        + recv
        + pair(30) * 10
        + [pltpu.SemaphoreType.DMA((3,)), pltpu.SemaphoreType.DMA((8,))]
        + pair(2),
        compiler_params=pltpu.CompilerParams(collective_id=3, has_side_effects=True, vmem_limit_bytes=67000000),
        name="grad_sums",
    )(dkv, hid, dq_home, *reds, cos_tab, sin_tab)


def solution(mesh):
    cp_size = mesh.shape["cp"]
    half = cp_size // 2
    axes = ("tp", "cp")

    def flat(tp, cp):
        return tp * cp_size + cp

    route_a, route_b = [], []
    for cp in range(cp_size):
        mine, mirror = int(cp >= half), cp_size - 1 - cp
        route_b.append((flat(mine, cp), flat(1 - mine, cp)))
        route_b.append((flat(1 - mine, cp), flat(1 - mine, mirror)))
        route_a.append((flat(1 - mine, cp), flat(mine, mirror)))
    back_a = [(dst, src) for src, dst in route_a]
    back_b = [(dst, src) for src, dst in route_b]
    partner = [(0, 1), (1, 0)]

    def exchange(own_of, is_mine, plan_a, plan_b, send_a, send_b):
        got_a = lax.ppermute(send_a, axes, plan_a)
        got_b = lax.ppermute(send_b, axes, plan_b)
        return jnp.where(is_mine, own_of, got_b), jnp.where(is_mine, got_b, got_a)

    def local_program(hidden, grad_out, w_query, w_key, w_value, w_out):
        block_len = hidden.shape[1]
        n_local = w_query.shape[1]
        head_dim = w_key.shape[1]
        q_scale = head_dim ** -0.5
        cp_idx = lax.axis_index("cp")
        tp_idx = lax.axis_index("tp")
        is_mine = tp_idx == (cp_idx >= half).astype(jnp.int32)
        mirror_idx = cp_size - 1 - cp_idx
        pieces = jnp.stack([cp_idx, mirror_idx]).astype(jnp.int32)
        cos_tab, sin_tab = rope_tables(cp_idx * block_len + jnp.arange(block_len), head_dim)
        cos_mir, sin_mir = rope_tables(mirror_idx * block_len + jnp.arange(block_len), head_dim)

        def pick(pair, idx):
            return lax.dynamic_index_in_dim(pair, idx, 0, keepdims=False)

        def to_workers(x):
            own, other = pick(x, tp_idx), pick(x, 1 - tp_idx)
            return exchange(own, is_mine, route_a, route_b, other, jnp.where(is_mine, other, own))

        def to_homes(own_piece, mir_piece):
            mine, other = exchange(own_piece, is_mine, back_a, back_b, mir_piece, jnp.where(is_mine, mir_piece, own_piece))
            first = tp_idx == 0
            return jnp.stack([jnp.where(first, mine, other), jnp.where(first, other, mine)])

        def sum_over_tp(part, extra=None):
            total = pick(part, tp_idx) + lax.ppermute(pick(part, 1 - tp_idx), "tp", partner)
            if extra is not None:
                total = total + extra
            mine = total.astype(BF16)
            other = lax.ppermute(mine, "tp", partner)
            first = tp_idx == 0
            return jnp.stack([jnp.where(first, mine, other), jnp.where(first, other, mine)])

        hid_b = pick(hidden, tp_idx)
        key_loc = rotate(dot(hid_b, w_key), cos_tab, sin_tab).astype(BF16)
        val_loc = dot(hid_b, w_value).astype(BF16)
        kv_all = kv_gather(jnp.concatenate([key_loc, val_loc], axis=1))

        q_pre = jnp.einsum("bsd,dhe->bhse", hidden, w_query, preferred_element_type=F32)
        queries = (rotate(q_pre, cos_tab, sin_tab) * q_scale).astype(BF16)
        d_out = jnp.einsum("bsd,hed->bhse", grad_out, w_out, preferred_element_type=F32).astype(BF16)
        own_qd, mir_qd = to_workers(jnp.stack([queries, d_out], axis=1))
        grp_shape = (2, n_local * block_len, head_dim)
        q_grp = jnp.stack([own_qd[0], mir_qd[0]]).reshape(grp_shape)
        do_grp = jnp.stack([own_qd[1], mir_qd[1]]).reshape(grp_shape)

        o_grp, lse = attention_forward(pieces, kv_all, q_grp)
        o_split = o_grp.reshape(2, n_local, block_len, head_dim)
        attn_heads = to_homes(o_split[0], o_split[1])
        attn_out = sum_over_tp(jnp.einsum("cirf,ife->cre", attn_heads, w_out, preferred_element_type=F32))

        tabs_t = [jnp.stack(pair_t) for pair_t in ((cos_tab.T, cos_mir.T), (sin_tab.T, sin_mir.T))]
        dq_pre, dkv, *reds = attention_backward(kv_all, q_grp, do_grp, o_grp, lse, attn_heads, grad_out.reshape(-1, grad_out.shape[-1]), *tabs_t)
        grad_q, grad_o, d_w_key, d_w_value, dkv_new = grad_sums(dkv, hidden.reshape(-1, hidden.shape[-1]), dq_pre, reds, cos_tab, sin_tab)
        d_w_query = grad_q.reshape(w_query.shape)
        d_w_out = grad_o.reshape(w_out.shape)
        dk_pre, dv_pre = dkv_new[:, :head_dim], dkv_new[:, head_dim:]
        dh_kv = dot(dk_pre, w_key.T) + dot(dv_pre, w_value.T)
        d_hidden = sum_over_tp(jnp.einsum("cirf,eif->cre", dq_pre, w_query, preferred_element_type=F32), dh_kv)
        return attn_out, d_hidden, d_w_query, d_w_key, d_w_value, d_w_out

    row_spec = P(None, "cp", None)
    return jax.shard_map(local_program, mesh=mesh, in_specs=(row_spec, row_spec, P(None, "tp", None), P(), P(), P("tp", None, None)), out_specs=(row_spec, row_spec, P(None, "tp", None), P(), P(), P("tp", None, None)), check_vma=False)
```

```python
import jax
import jax.numpy as jnp
from jax import lax
from jax.experimental import pallas as pl
from jax.experimental.pallas import tpu as pltpu
from jax.sharding import PartitionSpec as P

ROPE_BASE = 10000.0
BLK = 128
TILE = 512
COLS = 256
F32 = jnp.float32
BF16 = jnp.bfloat16


def rope_tables(positions, head_dim):
    half_dim = head_dim // 2
    inv_freq = 1.0 / jnp.power(ROPE_BASE, jnp.arange(half_dim, dtype=F32) * (2.0 / head_dim))
    angles = positions.astype(F32)[:, None] * inv_freq[None, :]
    return jnp.cos(angles), jnp.sin(angles)


def rotate(rot_in, cos_tab, sin_tab):
    half_dim = rot_in.shape[-1] // 2
    low_half = rot_in[..., :half_dim]
    high_half = rot_in[..., half_dim:]
    return jnp.concatenate([low_half * cos_tab - high_half * sin_tab, high_half * cos_tab + low_half * sin_tab], axis=-1)


def unrotate(rot_in, cos_tab, sin_tab):
    return rotate(rot_in, cos_tab, -sin_tab)


def dot(a, b):
    return jnp.dot(a, b, preferred_element_type=F32)


def dot_ta(a, b):
    return lax.dot_general(a, b, (((0,), (0,)), ((), ())), preferred_element_type=F32)


def causal_mask(k_start, q_start, cols):
    k_pos = k_start + lax.broadcasted_iota(jnp.int32, (TILE, cols), 0)
    q_pos = q_start + lax.broadcasted_iota(jnp.int32, (TILE, cols), 1) % BLK
    return k_pos <= q_pos


RING = 4
AXIS_STRIDE = (RING * RING, RING, 1)
ORDERS = ((0, 1, 2), (1, 2, 0), (2, 0, 1))
MESH = pl.DeviceIdType.MESH


def ring_of(axis):
    cp, tp = lax.axis_index("cp"), lax.axis_index("tp")
    stride = AXIS_STRIDE[axis]
    pos = (cp // stride) % RING
    right = cp + ((pos + 1) % RING - pos) * stride
    left = cp + ((pos + RING - 1) % RING - pos) * stride
    across = cp + ((pos + 2) % RING - pos) * stride
    return pos, (tp, right), (tp, left), (tp, across)


def enter(rings, with_partner=False, with_mirror=False):
    barrier = pltpu.get_barrier_semaphore()
    peers = []
    for _, *others in rings:
        peers += others
    if with_partner:
        peers.append((1 - lax.axis_index("tp"), lax.axis_index("cp")))
    if with_mirror:
        mirror = RING ** 3 - 1 - lax.axis_index("cp")
        peers += [(0, mirror), (1, mirror)]
    for peer in peers:
        pl.semaphore_signal(barrier, inc=1, device_id=peer, device_id_type=MESH)
    pl.semaphore_wait(barrier, len(peers))


def remote(src, dst, sems, idx, device):
    return pltpu.make_async_remote_copy(src_ref=src, dst_ref=dst, send_sem=sems[0].at[idx], recv_sem=sems[1].at[idx], device_id=device, device_id_type=MESH)


def add_rows(dst, dst0, srcs, n_rows, lanes):
    strip = next(s for s in (64, 48, 40, 32, 24, 16, 8) if n_rows % s == 0)
    if lanes[1] > 256:
        strip = next(s for s in (16, 8) if n_rows % s == 0)

    def body(i, carry):
        off = pl.multiple_of(dst0 + i * strip, 8)
        total = dst[pl.ds(off, strip), pl.ds(*lanes)]
        for ref, start in srcs:
            total = total + ref[pl.ds(pl.multiple_of(start + i * strip, 8), strip), :]
        dst[pl.ds(off, strip), pl.ds(*lanes)] = total
        return carry

    lax.fori_loop(0, n_rows // strip, body, 0)


class Part:
    def __init__(self, rings, order, rb, sems, x=None, y=None, recv=None, row0=0, lanes=None, align=8, direct=2):
        self.direct = direct
        self.rb, self.sems, self.x, self.y, self.recv = rb, sems, x, y, recv
        self.row0, self.lanes, self.align = row0, lanes, align
        self.places = []
        base = row0
        for phase in range(3):
            slab = rb * RING ** (2 - phase)
            h0 = -(-slab // (2 * align)) * align
            pos, right, left, across = rings[order[phase]]
            starts = [base + ((pos + d) % RING) * slab for d in range(RING)]
            self.places.append((slab, h0, slab - h0, starts, right, left, across))
            base = starts[0]

    def view(self, ref, start, n_rows):
        return ref.at[pl.ds(pl.multiple_of(start, self.align), n_rows), pl.ds(*self.lanes)]

    def place(self, phase):
        return self.places[phase]

    def hop(self, phase, i):
        slab, h0, h1, (own, rgt, opp, lft), right, left, across = self.place(phase)
        if phase >= self.direct:
            start, n_rows, at, device = {
                0: (opp, slab, 0, across),
                2: (rgt, slab, slab, right),
                3: (lft, slab, 2 * slab, left),
                6: (own, slab, 0, right),
                7: (own, slab, 0, left),
                8: (own, slab, 0, across),
            }[i]
        else:
            start, n_rows, at, device = (
                (opp, h0, 0, right),
                (opp + h0, h1, h0, left),
                (rgt + h0, h1, slab + h0, right),
                (lft, h0, 2 * slab, left),
                (rgt, h0, slab, right),
                (lft + h0, h1, 2 * slab + h0, left),
                (own, slab, 0, right),
                (own, slab, 0, left),
                (lft, h0, 0, right),
                (rgt + h0, h1, 0, left),
            )[i]
        if i < 6:
            src, dst = self.view(self.x, start, n_rows), self.recv[phase].at[pl.ds(at, n_rows)]
        else:
            src = dst = self.view(self.y, start, n_rows)
        return remote(src, dst, self.sems, 10 * phase + i, device)

    def rs_start(self, phase):
        for i in (0, 2, 3) if phase >= self.direct else range(4):
            self.hop(phase, i).start()

    def rs_mid(self, phase):
        if phase >= self.direct:
            return
        slab, h0, h1, (own, rgt, opp, lft), *_ = self.place(phase)
        buf = self.recv[phase]
        self.hop(phase, 0).wait_recv()
        add_rows(self.x, rgt, [(buf, 0)], h0, self.lanes)
        self.hop(phase, 4).start()
        self.hop(phase, 1).wait_recv()
        add_rows(self.x, lft + h0, [(buf, h0)], h1, self.lanes)
        self.hop(phase, 5).start()

    def rs_end(self, phase):
        slab, _, _, (own, _, _, _), *_ = self.place(phase)
        buf = self.recv[phase]
        terms = [(buf, slab), (buf, 2 * slab)]
        if phase >= self.direct:
            terms.append((buf, 0))
        for i in (0, 2, 3) if phase >= self.direct else range(2, 6):
            self.hop(phase, i).wait_recv()
        add_rows(self.x, own, terms, slab, self.lanes)

    def ag_start(self, phase):
        for i in (6, 7, 8) if phase >= self.direct else (6, 7):
            self.hop(phase, i).start()

    def ag_mid(self, phase):
        if phase >= self.direct:
            return
        self.hop(phase, 6).wait_recv()
        self.hop(phase, 8).start()
        self.hop(phase, 7).wait_recv()
        self.hop(phase, 9).start()

    def ag_end(self, phase):
        for i in (6, 7, 8) if phase >= self.direct else (8, 9):
            self.hop(phase, i).wait_recv()

    def own_rows(self):
        return self.place(2)[3][0]

    def drain(self, rs=(), ag=()):
        for phase in rs:
            for i in (0, 2, 3) if phase >= self.direct else range(6):
                self.hop(phase, i).wait_send()
        for phase in ag:
            for i in (6, 7, 8) if phase >= self.direct else range(6, 10):
                self.hop(phase, i).wait_send()


def stage(parts, step):
    for part in parts:
        getattr(part, step[:-1])(int(step[-1]))


def slab_rows(rb):
    return [3 * rb * RING ** (2 - phase) for phase in range(3)]


def place_in_order(block, order):
    digit = [(block // s) % RING for s in AXIS_STRIDE]
    return (digit[order[0]] * RING + digit[order[1]]) * RING + digit[order[2]]


def by_rows(n_rows, align):
    unit = n_rows // align
    counts = [(unit + 2 - c) // 3 for c in range(3)]
    starts = [sum(counts[:c]) * align for c in range(3)]
    return [(starts[c], counts[c] * align) for c in range(3)]


def pair(n):
    return [pltpu.SemaphoreType.DMA((n,)), pltpu.SemaphoreType.DMA((n,))]


def grad_layout(d_model, n_local):
    n_blk = RING ** 3
    q_tiles = d_model * n_local // 8 // n_blk
    o_tiles = d_model // 128
    q_count = [q_tiles * 13 // 32, q_tiles * 11 // 32]
    q_count.append(q_tiles - sum(q_count))
    o_count = [o_tiles * 5 // 16, o_tiles * 6 // 16]
    o_count.append(o_tiles - sum(o_count))
    q_rows = [8 * n for n in q_count]
    q_first = [n_blk * sum(q_rows[:c]) for c in range(3)]
    o_lanes = [(128 * sum(o_count[:c]), 128 * o_count[c]) for c in range(3)]
    return q_rows, q_first, o_lanes


def place_heads(dst, src):
    n_batch, n_rows, head_dim = src.shape
    for b in range(n_batch):
        for h in range(n_rows // BLK):
            dst[pl.ds(b * BLK, BLK), pl.ds(h * head_dim, head_dim)] = src[b, h * BLK:(h + 1) * BLK, :]


D_TILE = 256


class Return:
    def __init__(self, src, dst, sems):
        self.src, self.dst, self.sems = src, dst, sems
        self.cp, self.tp = lax.axis_index("cp"), lax.axis_index("tp")
        self.mirror = RING ** 3 - 1 - self.cp
        self.group = self.cp // (RING ** 3 // 2)
        self.is_mine = self.tp == self.group

    def give(self, piece_idx):
        device = (self.group, self.mirror) if piece_idx else (1 - self.tp, self.cp)
        return pltpu.make_async_remote_copy(src_ref=self.src.at[piece_idx], dst_ref=self.dst.at[self.tp], send_sem=self.sems[0].at[piece_idx], recv_sem=self.sems[1].at[self.tp], device_id=device, device_id_type=MESH)

    def take(self, batch):
        return pltpu.make_async_remote_copy(src_ref=self.src.at[1], dst_ref=self.dst.at[batch], send_sem=self.sems[0].at[1], recv_sem=self.sems[1].at[batch], device_id=(self.group, self.mirror), device_id_type=MESH)

    def start(self):
        self.give(1).start()

        @pl.when(jnp.logical_not(self.is_mine))
        def _():
            self.give(0).start()

        @pl.when(self.is_mine)
        def _():
            self.dst[self.tp] = self.src[0]

    def wait(self):
        self.take(1 - self.tp).wait_recv()

        @pl.when(jnp.logical_not(self.is_mine))
        def _():
            self.take(self.tp).wait_recv()

    def drain(self):
        self.give(1).wait_send()

        @pl.when(jnp.logical_not(self.is_mine))
        def _():
            self.give(0).wait_send()


class Handout:
    def __init__(self, src, dst, sems):
        self.src, self.dst, self.sems = src, dst, sems
        self.cp, self.tp = lax.axis_index("cp"), lax.axis_index("tp")
        self.mirror = RING ** 3 - 1 - self.cp
        self.is_mine = self.tp == self.cp // (RING ** 3 // 2)

    def copy(self, kind, batch, slot, device, sem):
        return pltpu.make_async_remote_copy(src_ref=self.src.at[batch, kind], dst_ref=self.dst.at[slot, kind], send_sem=self.sems[0].at[2 * kind + sem], recv_sem=self.sems[1].at[2 * kind + slot], device_id=device, device_id_type=MESH)

    def near(self, kind):
        return self.copy(kind, 1 - self.tp, 0, (1 - self.tp, self.cp), 0)

    def far(self, kind, batch):
        return self.copy(kind, batch, 1, (batch, self.mirror), batch)

    def start(self, kind):
        @pl.when(self.is_mine)
        def _():
            self.near(kind).start()
            self.dst[0, kind] = self.src[self.tp, kind]

        @pl.when(jnp.logical_not(self.is_mine))
        def _():
            self.far(kind, 0).start()
            self.far(kind, 1).start()

    def wait(self, kind):
        self.far(kind, 0).wait_recv()

        @pl.when(jnp.logical_not(self.is_mine))
        def _():
            self.near(kind).wait_recv()

    def drain(self, kind):
        @pl.when(self.is_mine)
        def _():
            self.near(kind).wait_send()

        @pl.when(jnp.logical_not(self.is_mine))
        def _():
            self.far(kind, 0).wait_send()
            self.far(kind, 1).wait_send()


D_TILE = 256


def attn_kernel(own_ref, qd_ref, grad_ref, cos_ref, sin_ref, oh_ref, dqh_ref, dkv_ref, red0, red1, red2, y0, y1, y2, kv_scr, qd_scr, o_scr, qt_scr, dot_scr, dqt_scr, m_scr, l_scr, delta_scr, p_scr, ds_scr, xo, tok_scr, rot_scr, oh_scr, dqh_scr, *rest):
    recv, k_sems, o_sems = rest[:3], rest[3:9], rest[9:15]
    hand_sems, oh_sems, dqh_sems = rest[15:17], rest[17:19], rest[19:21]
    n_groups, _, n_cols, e_dim = qd_scr.shape
    rows = own_ref.shape[0]
    per_tile = TILE // BLK
    n_blk = RING ** 3
    d_model = grad_ref.shape[1]
    cp = lax.axis_index("cp")
    mirror = n_blk - 1 - cp
    rings = [ring_of(axis) for axis in range(3)]
    _, _, o_lanes = grad_layout(d_model, n_cols // rows)
    ys = (y0, y1, y2)
    split = by_rows(rows, 16)
    p_kv = [Part(rings, ORDERS[c], split[c][1], k_sems[2 * c:2 * c + 2], y=ys[c], lanes=(0, 2 * e_dim), align=16, direct=1) for c in range(3)]
    p_o = [Part(rings, ORDERS[c], n_cols // n_blk, o_sems[2 * c:2 * c + 2], x=xo, recv=[recv[c]], lanes=o_lanes[c]) for c in range(3)]
    hand = Handout(qd_ref, qd_scr, hand_sems)
    o_back = Return(o_scr, oh_scr, oh_sems)
    dq_back = Return(rot_scr, dqh_scr, dqh_sems)

    for c in range(3):
        ys[c][pl.ds(pl.multiple_of(p_kv[c].own_rows(), 16), split[c][1]), :] = own_ref[pl.ds(*split[c]), :]
    enter(rings, with_partner=True, with_mirror=True)
    stage(p_kv, "ag_start2")
    stage(p_kv, "ag_end2")
    stage(p_kv, "ag_start1")
    hand.start(0)
    stage(p_kv, "ag_end1")
    stage(p_kv, "ag_start0")
    dqt_scr[...] = jnp.zeros_like(dqt_scr)
    dkv_ref[...] = jnp.zeros_like(dkv_ref)
    m_scr[...] = jnp.full_like(m_scr, -jnp.inf)
    l_scr[...] = jnp.zeros_like(l_scr)
    hand.wait(0)
    for grp in range(n_groups):
        qt_scr[grp] = qd_scr[grp, 0].T
    stage(p_kv, "ag_mid0")
    hand.start(1)
    stage(p_kv, "ag_end0")

    def place_kv(blk, carry):
        for c in range(3):
            at, rb = split[c]
            src = pl.ds(pl.multiple_of(place_in_order(blk, ORDERS[c]) * rb, 16), rb)
            kv_scr[pl.ds(pl.multiple_of(blk * rows + at, 16), rb), :] = ys[c][src, :]
        return carry

    lax.fori_loop(0, n_blk, place_kv, 0)

    n_first = cp // per_tile + 1
    n_steps = n_blk // per_tile + 1

    def over_tiles(tile_step, extra):
        def body(t, carry):
            grp = (t - n_first + n_steps) // n_steps
            piece = cp + grp * (mirror - cp)
            tile_idx = t - grp * n_first
            last = tile_idx == piece // per_tile

            @pl.when(jnp.logical_not(last))
            def _():
                tile_step(grp, tile_idx, piece, False)

            @pl.when(last)
            def _():
                tile_step(grp, tile_idx, piece, True)

            for when, action in extra:
                pl.when(t == when)(action)
            return carry

        lax.fori_loop(0, n_steps, body, 0)

    def fwd_step(grp, tile_idx, piece, masked):
        row0 = pl.multiple_of(tile_idx * TILE, TILE)
        k_t = kv_scr[pl.ds(row0, TILE), :e_dim]
        v_t = kv_scr[pl.ds(row0, TILE), e_dim:]
        for c0 in range(0, n_cols, COLS):
            cs = slice(c0, c0 + COLS)
            s = dot(k_t, qt_scr[grp, :, cs])
            if masked:
                s = jnp.where(causal_mask(row0, piece * BLK, COLS), s, -jnp.inf)
            m_old = m_scr[grp, :, cs]
            m_new = jnp.maximum(m_old, jnp.max(s, axis=0, keepdims=True))
            p = jnp.exp(s - m_new)
            alpha = jnp.exp(m_old - m_new)
            m_scr[grp, :, cs] = m_new
            l_scr[grp, :, cs] = l_scr[grp, :, cs] * alpha + jnp.sum(p, axis=0, keepdims=True)
            dqt_scr[grp, :, cs] = dqt_scr[grp, :, cs] * alpha + dot_ta(v_t, p.astype(BF16))

    over_tiles(fwd_step, ())
    hand.wait(1)
    for grp in range(n_groups):
        o_t = (dqt_scr[grp] / l_scr[grp]).astype(BF16)
        o_scr[grp] = o_t.T
        dot_scr[grp] = qd_scr[grp, 1].T
        delta_scr[grp] = jnp.sum(dot_scr[grp].astype(F32) * o_t.astype(F32), axis=0, keepdims=True)
    o_back.start()
    m_scr[...] = m_scr[...] + jnp.log(l_scr[...])
    dqt_scr[...] = jnp.zeros_like(dqt_scr)

    def bwd_step(grp, tile_idx, piece, masked):
        row0 = pl.multiple_of(tile_idx * TILE, TILE)
        k_t = kv_scr[pl.ds(row0, TILE), :e_dim]
        v_t = kv_scr[pl.ds(row0, TILE), e_dim:]
        for c0 in range(0, n_cols, COLS):
            cs = slice(c0, c0 + COLS)
            s = dot(k_t, qt_scr[grp, :, cs])
            p = jnp.exp(s - m_scr[grp, :, cs])
            if masked:
                p = jnp.where(causal_mask(row0, piece * BLK, COLS), p, 0.0)
            d_p = dot(v_t, dot_scr[grp, :, cs])
            p_scr[:, cs] = p.astype(BF16)
            ds_scr[:, cs] = (p * (d_p - delta_scr[grp, :, cs])).astype(BF16)
        at = pl.ds(row0, TILE)
        dkv_ref[at, :e_dim] += dot(ds_scr[...], qd_scr[grp, 0])
        dkv_ref[at, e_dim:] += dot(p_scr[...], qd_scr[grp, 1])
        dqt_scr[grp] += dot_ta(k_t, ds_scr[...])

    def sum_wo_start():
        o_back.wait()
        place_heads(tok_scr, oh_scr)

        def o_body(i, carry):
            cols = pl.ds(pl.multiple_of(i * D_TILE, D_TILE), D_TILE)
            xo[:, cols] = dot_ta(tok_scr[...], grad_ref[:, cols])
            return carry

        lax.fori_loop(0, d_model // D_TILE, o_body, 0)
        stage(p_o, "rs_start0")

    over_tiles(bwd_step, ((3, sum_wo_start), (9, lambda: stage(p_o, "rs_mid0"))))

    scale = e_dim ** -0.5
    half_dim = e_dim // 2
    for grp in range(n_groups):
        cos_t, sin_t = cos_ref[grp], sin_ref[grp]
        for h in range(n_cols // rows):
            cols = slice(h * rows, (h + 1) * rows)
            low, high = dqt_scr[grp, :half_dim, cols], dqt_scr[grp, half_dim:, cols]
            turned = jnp.concatenate([low * cos_t + high * sin_t, high * cos_t - low * sin_t], axis=0) * scale
            rot_scr[grp, cols, :] = turned.T.astype(BF16)
    dq_back.start()
    oh_ref[...] = oh_scr[...]
    stage(p_o, "rs_end0")
    for part, out, lanes in zip(p_o, (red0, red1, red2), o_lanes):
        slab, _, _, starts, *_ = part.place(0)
        out[...] = xo[pl.ds(pl.multiple_of(starts[0], 8), slab), pl.ds(*lanes)]
    dq_back.wait()
    dqh_ref[...] = dqh_scr[...]
    for part in p_kv:
        part.drain(ag=range(3))
    for part in p_o:
        part.drain(rs=(0,))
    for kind in range(2):
        hand.drain(kind)
    o_back.drain()
    dq_back.drain()


def attention(own_kv, qd_home, grad, cos_t, sin_t):
    n_batch, _, n_cols, e_dim = qd_home.shape
    rows = own_kv.shape[0]
    n_tok, d_model = grad.shape
    n_blk = RING ** 3
    seq = n_blk * rows
    _, _, o_lanes = grad_layout(d_model, n_cols // rows)
    slab = n_cols // RING
    vmem = pl.BlockSpec(memory_space=pltpu.VMEM)
    heads = (2, n_cols, e_dim)
    work = 2 * n_cols * seq // 2
    return pl.pallas_call(
        attn_kernel,
        out_shape=(jax.ShapeDtypeStruct(heads, BF16), jax.ShapeDtypeStruct(heads, BF16), jax.ShapeDtypeStruct((seq, 2 * e_dim), F32)) + tuple(jax.ShapeDtypeStruct((slab, n), F32) for _, n in o_lanes),
        in_specs=[vmem] * 5,
        out_specs=(vmem,) * 6,
        scratch_shapes=[pltpu.VMEM((n_blk * rb, 2 * e_dim), BF16) for _, rb in by_rows(rows, 16)]
        + [
            pltpu.VMEM((seq, 2 * e_dim), BF16),
            pltpu.VMEM((2, 2, n_cols, e_dim), BF16),
            pltpu.VMEM(heads, BF16),
            pltpu.VMEM((2, e_dim, n_cols), BF16),
            pltpu.VMEM((2, e_dim, n_cols), BF16),
            pltpu.VMEM((2, e_dim, n_cols), F32),
            pltpu.VMEM((2, 1, n_cols), F32),
            pltpu.VMEM((2, 1, n_cols), F32),
            pltpu.VMEM((2, 1, n_cols), F32),
            pltpu.VMEM((TILE, n_cols), BF16),
            pltpu.VMEM((TILE, n_cols), BF16),
            pltpu.VMEM((n_cols, d_model), F32),
            pltpu.VMEM((n_tok, n_cols), BF16),
            pltpu.VMEM(heads, BF16),
            pltpu.VMEM(heads, BF16),
            pltpu.VMEM(heads, BF16),
        ]
        + [pltpu.VMEM((3 * slab, lanes), F32) for _, lanes in o_lanes]
        + pair(30) * 6
        + pair(4)
        + pair(2) * 2,
        compiler_params=pltpu.CompilerParams(collective_id=2, has_side_effects=True, vmem_limit_bytes=64000000),
        cost_estimate=pl.CostEstimate(flops=14 * work * e_dim, bytes_accessed=seq * e_dim * 12, transcendentals=2 * work),
        name="attention",
    )(own_kv, qd_home, grad, cos_t, sin_t)


GRAD_PLAN = (
    "d.rs_start0", "d.rs_mid0", "weights.q", "r.rs_start1", "d.rs_end0", "d.rs_start1", "d.rs_mid1", "r.rs_mid1",
    "d.rs_end1", "d.rs_start2", "r.rs_end1", "q.rs_start0", "d.rs_end2", "weights.prep", "q.rs_mid0", "weights.kv",
    "k.rs_start0", "k.rs_mid0", "r.rs_start2", "q.rs_end0", "k.rs_end0", "k.rs_start1", "q.rs_start1", "k.rs_mid1",
    "q.rs_mid1", "r.rs_end2", "o.ag_start2", "q.rs_end1", "q.rs_start2", "k.rs_end1", "o.ag_end2", "k.rs_start2",
    "o.ag_start1", "q.rs_end2", "k.rs_end2", "q.ag_start2", "k.ag_start2", "o.ag_mid1", "q.ag_end2", "k.ag_end2",
    "k.ag_start1", "q.ag_start1", "k.ag_mid1", "q.ag_mid1", "o.ag_end1", "k.ag_end1", "k.ag_start0", "o.ag_start0",
    "k.ag_mid0", "q.ag_end1", "q.ag_start0", "o.ag_mid0", "q.ag_mid0", "o.ag_end0", "k.ag_end0", "q.ag_end0",
)


def grad_kernel(dkv_ref, hid_ref, dqh_ref, red0, red1, red2, cos_ref, sin_ref, gq_ref, go_ref, gk_ref, gv_ref, dkd_ref, x0, x1, x2, xq, xk, yq, yo, yk, yp, xo0, xo1, xo2, tok_scr, mine_scr, give_scr, got_scr, *rest):
    n_parts = 10
    recv, sems, in_sem, out_sem, swap_s, swap_r = rest[:27], rest[27:27 + 2 * n_parts], rest[-4], rest[-3], rest[-2], rest[-1]
    n_blk = RING ** 3
    n_tok, d_model = hid_ref.shape
    n_batch, _, head_dim = dqh_ref.shape
    rows, lanes = n_tok // n_batch, 2 * head_dim
    n_local = dqh_ref.shape[1] // rows
    n_cols = n_local * head_dim
    q_rows, q_first, o_lanes = grad_layout(d_model, n_local)
    split = by_rows(rows, 8)
    tp, cp = lax.axis_index("tp"), lax.axis_index("cp")
    partner = (1 - tp, cp)
    xs = (x0, x1, x2)
    rings = [ring_of(axis) for axis in range(3)]

    def sem(i):
        return sems[2 * i:2 * i + 2]

    p_d = [Part(rings, ORDERS[c], split[c][1], sem(c), x=xs[c], recv=recv[3 * c:3 * c + 3], lanes=(0, lanes)) for c in range(3)]
    p_q = [Part(rings, ORDERS[c], q_rows[c], sem(3 + c), x=xq, y=yq, recv=recv[9 + 3 * c:12 + 3 * c], row0=q_first[c], lanes=(0, 128)) for c in range(3)]
    p_o = [Part(rings, ORDERS[c], n_cols // n_blk, sem(6 + c), y=yo, lanes=o_lanes[c]) for c in range(3)]
    xos = (xo0, xo1, xo2)
    o_slab = n_cols // RING
    p_r = [Part(rings, ORDERS[c], n_cols // n_blk, sem(6 + c), x=xos[c], recv=[None] + list(recv[21 + 2 * c:23 + 2 * c]), row0=0 - rings[ORDERS[c][0]][0] * o_slab, lanes=(0, o_lanes[c][1])) for c in range(3)]
    p_k = Part(rings, ORDERS[2], d_model // n_blk, sem(9), x=xk, y=yk, recv=recv[18:21], lanes=(0, 128))
    p_qo = p_q + p_o

    def load(blk, carry):
        for c in range(3):
            at, rb = split[c]
            dst = xs[c].at[pl.ds(pl.multiple_of(place_in_order(blk, ORDERS[c]) * rb, 8), rb)]
            pltpu.make_async_copy(dkv_ref.at[pl.ds(pl.multiple_of(blk * rows + at, 8), rb)], dst, in_sem.at[c]).start()
        return carry

    lax.fori_loop(0, n_blk, load, 0)
    for c, red in enumerate((red0, red1, red2)):
        pltpu.make_async_copy(red, xos[c], in_sem.at[3 + c]).start()
    enter(rings, with_partner=True)
    for c, red in enumerate((red0, red1, red2)):
        pltpu.make_async_copy(red, xos[c], in_sem.at[3 + c]).wait()
    for c in range(3):
        pltpu.make_async_copy(dkv_ref.at[pl.ds(0, n_blk * split[c][1])], xs[c], in_sem.at[c]).wait()
    half_dim = head_dim // 2
    first = tp == 0
    swap_small = pltpu.make_async_remote_copy(src_ref=give_scr, dst_ref=got_scr, send_sem=swap_s.at[0], recv_sem=swap_r.at[0], device_id=partner, device_id_type=MESH)
    swap = pltpu.make_async_remote_copy(src_ref=yk, dst_ref=yp, send_sem=swap_s.at[1], recv_sem=swap_r.at[1], device_id=partner, device_id_type=MESH)

    def put(parts, which):
        for part in parts:
            out = gq_ref if part.y is yq else go_ref
            slab, _, _, starts, *_ = part.place(0)
            for i in which:
                src, dst = part.view(part.y, starts[i], slab), part.view(out, starts[i], slab)
                pltpu.make_async_copy(src, dst, out_sem.at[p_qo.index(part)]).start()

    def own_block(parts, sums):
        for part, total in zip(parts, sums):
            at, lanes_y, lanes_x = part.own_rows(), pl.ds(*part.lanes), pl.ds(*total.lanes)
            part.y[pl.ds(pl.multiple_of(at, 8), part.rb), lanes_y] = total.x[pl.ds(pl.multiple_of(total.own_rows(), 8), part.rb), lanes_x]

    def weights_q():
        place_heads(tok_scr, dqh_ref)

        def q_body(i, carry):
            cols = pl.ds(pl.multiple_of(i * D_TILE, D_TILE), D_TILE)
            res = dot_ta(hid_ref[:, cols], tok_scr[...])
            for h in range(n_local):
                xq[pl.ds(i * D_TILE * n_local + h, D_TILE, stride=n_local), :] = res[:, h * head_dim:(h + 1) * head_dim]
            return carry

        lax.fori_loop(0, d_model // D_TILE, q_body, 0)

    def new_dkv():
        dkd_ref[...] = mine_scr[...].astype(BF16)
        return dkd_ref[:, :head_dim], dkd_ref[:, head_dim:]

    def weights_prep():
        for c in range(3):
            at, rb = split[c]
            own = xs[c][pl.ds(pl.multiple_of(p_d[c].own_rows(), 8), rb), :]
            cos_tab, sin_tab = cos_ref[pl.ds(at, rb), :], sin_ref[pl.ds(at, rb), :]
            low, high = own[:, :half_dim], own[:, half_dim:head_dim]
            mine_scr[pl.ds(at, rb), :head_dim] = jnp.concatenate([low * cos_tab + high * sin_tab, high * cos_tab - low * sin_tab], axis=1)
            mine_scr[pl.ds(at, rb), head_dim:] = own[:, head_dim:]
        dk_new, dv_new = new_dkv()
        give_scr[...] = jnp.where(first, dv_new, dk_new)
        swap_small.start()

    def weights_kv():
        swap_small.wait()
        got = got_scr[...]
        keep = jnp.where(first, dkd_ref[:, :head_dim], dkd_ref[:, head_dim:])
        kv_tok = jnp.concatenate([jnp.where(first, keep, got), jnp.where(first, got, keep)], axis=0)
        for i in range(d_model // D_TILE):
            xk[pl.ds(i * D_TILE, D_TILE), :] = dot_ta(hid_ref[:, i * D_TILE:(i + 1) * D_TILE], kv_tok)

    groups = {"d": p_d, "q": p_q, "r": p_r, "o": p_o, "k": [p_k]}
    after = {
        "weights.q": weights_q,
        "weights.prep": weights_prep,
        "weights.kv": weights_kv,
        "r.rs_end2": lambda: own_block(p_o, p_r),
        "q.rs_end2": lambda: own_block(p_q, p_q),
        "k.rs_end2": lambda: own_block([p_k], [p_k]),
        "o.ag_mid0": lambda: put(p_o, (0, 1, 3)),
        "o.ag_end0": lambda: put(p_o, (2,)),
        "q.ag_start0": lambda: put(p_q, (0,)),
        "q.ag_mid0": lambda: put(p_q, (1, 3)),
        "q.ag_end0": lambda: put(p_q, (2,)),
        "k.ag_end0": swap.start,
    }
    for step in GRAD_PLAN:
        who, what = step.split(".")
        if who in groups:
            stage(groups[who], what)
        if step in after:
            after[step]()
    swap.wait()

    def put_kv(k_src, v_src):
        outs = [pltpu.make_async_copy(k_src, gk_ref, out_sem.at[6]), pltpu.make_async_copy(v_src, gv_ref, out_sem.at[7])]
        for copy in outs:
            copy.start()
        for copy in outs:
            copy.wait()

    @pl.when(first)
    def _():
        put_kv(yk, yp)

    @pl.when(jnp.logical_not(first))
    def _():
        put_kv(yp, yk)

    for i, part in enumerate(p_qo):
        out = gq_ref if part.y is yq else go_ref
        span = n_blk * part.rb
        pltpu.make_async_copy(part.view(part.y, part.row0, span), part.view(out, part.row0, span), out_sem.at[i]).wait()
    for part in p_d:
        part.drain(rs=range(3))
    for part in p_q + [p_k]:
        part.drain(rs=range(3), ag=range(3))
    for part, red in zip(p_o, p_r):
        red.drain(rs=(1, 2))
        part.drain(ag=range(3))


def grad_sums(dkv, hid, dq_home, reds, cos_tab, sin_tab):
    n_tok, d_model = hid.shape
    n_batch, _, head_dim = dq_home.shape
    block_len = n_tok // n_batch
    n_local = dq_home.shape[1] // block_len
    n_cols = n_local * head_dim
    n_blk = RING ** 3
    lanes = 2 * head_dim
    q_rows, _, o_lanes = grad_layout(d_model, n_local)
    split = by_rows(block_len, 8)
    recv = [pltpu.VMEM((n, lanes), F32) for _, rb in split for n in slab_rows(rb)]
    recv += [pltpu.VMEM((n, 128), F32) for rb in q_rows for n in slab_rows(rb)]
    recv += [pltpu.VMEM((n, 128), F32) for n in slab_rows(d_model // n_blk)]
    recv += [pltpu.VMEM((n, w), F32) for _, w in o_lanes for n in slab_rows(n_cols // n_blk)[1:]]
    vmem, anyspace = pl.BlockSpec(memory_space=pltpu.VMEM), pl.BlockSpec(memory_space=pl.ANY)
    xq, xo, xk = (pltpu.VMEM(s, F32) for s in ((d_model * n_local, 128), (n_cols, d_model), (d_model, 128)))
    small = pltpu.VMEM((block_len, head_dim), BF16)
    return pl.pallas_call(
        grad_kernel,
        out_shape=(
            jax.ShapeDtypeStruct((d_model * n_local, 128), F32),
            jax.ShapeDtypeStruct((n_cols, d_model), F32),
            jax.ShapeDtypeStruct((d_model, 128), F32),
            jax.ShapeDtypeStruct((d_model, 128), F32),
            jax.ShapeDtypeStruct((block_len, lanes), BF16),
        ),
        in_specs=[anyspace] + [vmem] * 2 + [anyspace] * 3 + [vmem] * 2,
        out_specs=(anyspace,) * 4 + (vmem,),
        scratch_shapes=[pltpu.VMEM((n_blk * rb, lanes), F32) for _, rb in split]
        + [xq, xk, xq, xo, xk, xk]
        + [pltpu.VMEM((n_cols // RING, w), F32) for _, w in o_lanes]
        + [pltpu.VMEM((n_tok, n_cols), BF16), pltpu.VMEM((block_len, lanes), F32), small, small]
        + recv
        + pair(30) * 10
        + [pltpu.SemaphoreType.DMA((6,)), pltpu.SemaphoreType.DMA((8,))]
        + pair(2),
        compiler_params=pltpu.CompilerParams(collective_id=3, has_side_effects=True, vmem_limit_bytes=67000000),
        cost_estimate=pl.CostEstimate(flops=2 * n_tok * d_model * n_cols * 80, bytes_accessed=40 << 20, transcendentals=0),
        name="grad_sums",
    )(dkv, hid, dq_home, *reds, cos_tab, sin_tab)


def solution(mesh):
    cp_size = mesh.shape["cp"]
    partner = [(0, 1), (1, 0)]

    def local_program(hidden, grad_out, w_query, w_key, w_value, w_out):
        block_len = hidden.shape[1]
        n_local = w_query.shape[1]
        head_dim = w_key.shape[1]
        q_scale = head_dim ** -0.5
        cp_idx = lax.axis_index("cp")
        tp_idx = lax.axis_index("tp")
        mirror_idx = cp_size - 1 - cp_idx
        cos_tab, sin_tab = rope_tables(cp_idx * block_len + jnp.arange(block_len), head_dim)
        cos_mir, sin_mir = rope_tables(mirror_idx * block_len + jnp.arange(block_len), head_dim)

        def pick(pair, idx):
            return lax.dynamic_index_in_dim(pair, idx, 0, keepdims=False)

        def sum_over_tp(part, extra=None):
            total = pick(part, tp_idx) + lax.ppermute(pick(part, 1 - tp_idx), "tp", partner)
            if extra is not None:
                total = total + extra
            mine = total.astype(BF16)
            other = lax.ppermute(mine, "tp", partner)
            first = tp_idx == 0
            return jnp.stack([jnp.where(first, mine, other), jnp.where(first, other, mine)])

        hid_b = pick(hidden, tp_idx)
        key_loc = rotate(dot(hid_b, w_key), cos_tab, sin_tab).astype(BF16)
        val_loc = dot(hid_b, w_value).astype(BF16)
        own_kv = jnp.concatenate([key_loc, val_loc], axis=1)

        q_pre = jnp.einsum("bsd,dhe->bhse", hidden, w_query, preferred_element_type=F32)
        queries = (rotate(q_pre, cos_tab, sin_tab) * q_scale).astype(BF16)
        d_out = jnp.einsum("bsd,hed->bhse", grad_out, w_out, preferred_element_type=F32).astype(BF16)
        qd_home = jnp.stack([queries, d_out], axis=1).reshape(2, 2, n_local * block_len, head_dim)
        tabs_t = [jnp.stack(pair_t) for pair_t in ((cos_tab.T, cos_mir.T), (sin_tab.T, sin_mir.T))]
        o_home, dq_home, dkv, *reds = attention(own_kv, qd_home, grad_out.reshape(-1, grad_out.shape[-1]), *tabs_t)
        attn_heads = o_home.reshape(2, n_local, block_len, head_dim)
        dq_pre = dq_home.reshape(2, n_local, block_len, head_dim)
        attn_out = sum_over_tp(jnp.einsum("cirf,ife->cre", attn_heads, w_out, preferred_element_type=F32))
        grad_q, grad_o, d_w_key, d_w_value, dkv_new = grad_sums(dkv, hidden.reshape(-1, hidden.shape[-1]), dq_home, reds, cos_tab, sin_tab)
        d_w_query = grad_q.reshape(w_query.shape)
        d_w_out = grad_o.reshape(w_out.shape)
        dk_pre, dv_pre = dkv_new[:, :head_dim], dkv_new[:, head_dim:]
        dh_kv = dot(dk_pre, w_key.T) + dot(dv_pre, w_value.T)
        d_hidden = sum_over_tp(jnp.einsum("cirf,eif->cre", dq_pre, w_query, preferred_element_type=F32), dh_kv)
        return attn_out, d_hidden, d_w_query, d_w_key, d_w_value, d_w_out

    row_spec = P(None, "cp", None)
    return jax.shard_map(local_program, mesh=mesh, in_specs=(row_spec, row_spec, P(None, "tp", None), P(), P(), P("tp", None, None)), out_specs=(row_spec, row_spec, P(None, "tp", None), P(), P(), P("tp", None, None)), check_vma=False)
```

```python
import jax
import jax.numpy as jnp
from jax import lax
from jax.experimental import pallas as pl
from jax.experimental.pallas import tpu as pltpu
from jax.sharding import PartitionSpec as P

ROPE_BASE = 10000.0
BLK = 128
TILE = 512
COLS = 256
F32 = jnp.float32
BF16 = jnp.bfloat16


def rope_tables(positions, head_dim):
    half_dim = head_dim // 2
    inv_freq = 1.0 / jnp.power(ROPE_BASE, jnp.arange(half_dim, dtype=F32) * (2.0 / head_dim))
    angles = positions.astype(F32)[:, None] * inv_freq[None, :]
    return jnp.cos(angles), jnp.sin(angles)


def rotate(rot_in, cos_tab, sin_tab):
    half_dim = rot_in.shape[-1] // 2
    low_half = rot_in[..., :half_dim]
    high_half = rot_in[..., half_dim:]
    return jnp.concatenate([low_half * cos_tab - high_half * sin_tab, high_half * cos_tab + low_half * sin_tab], axis=-1)


def unrotate(rot_in, cos_tab, sin_tab):
    return rotate(rot_in, cos_tab, -sin_tab)


def dot(a, b):
    return jnp.dot(a, b, preferred_element_type=F32)


def dot_ta(a, b):
    return lax.dot_general(a, b, (((0,), (0,)), ((), ())), preferred_element_type=F32)


def causal_mask(k_start, q_start, cols):
    k_pos = k_start + lax.broadcasted_iota(jnp.int32, (TILE, cols), 0)
    q_pos = q_start + lax.broadcasted_iota(jnp.int32, (TILE, cols), 1) % BLK
    return k_pos <= q_pos


RING = 4
AXIS_STRIDE = (RING * RING, RING, 1)
ORDERS = ((0, 1, 2), (1, 2, 0), (2, 0, 1))
MESH = pl.DeviceIdType.MESH


def ring_of(axis):
    cp, tp = lax.axis_index("cp"), lax.axis_index("tp")
    stride = AXIS_STRIDE[axis]
    pos = (cp // stride) % RING
    right = cp + ((pos + 1) % RING - pos) * stride
    left = cp + ((pos + RING - 1) % RING - pos) * stride
    across = cp + ((pos + 2) % RING - pos) * stride
    return pos, (tp, right), (tp, left), (tp, across)


def enter(rings, with_partner=False, with_mirror=False):
    barrier = pltpu.get_barrier_semaphore()
    peers = []
    for _, *others in rings:
        peers += others
    if with_partner:
        peers.append((1 - lax.axis_index("tp"), lax.axis_index("cp")))
    if with_mirror:
        mirror = RING ** 3 - 1 - lax.axis_index("cp")
        peers += [(0, mirror), (1, mirror)]
    for peer in peers:
        pl.semaphore_signal(barrier, inc=1, device_id=peer, device_id_type=MESH)
    pl.semaphore_wait(barrier, len(peers))


def remote(src, dst, sems, idx, device):
    return pltpu.make_async_remote_copy(src_ref=src, dst_ref=dst, send_sem=sems[0].at[idx], recv_sem=sems[1].at[idx], device_id=device, device_id_type=MESH)


def add_rows(dst, dst0, srcs, n_rows, lanes):
    strip = next(s for s in (64, 48, 40, 32, 24, 16, 8) if n_rows % s == 0)
    if lanes[1] > 256:
        strip = next(s for s in (16, 8) if n_rows % s == 0)

    def body(i, carry):
        off = pl.multiple_of(dst0 + i * strip, 8)
        total = dst[pl.ds(off, strip), pl.ds(*lanes)]
        for ref, start in srcs:
            total = total + ref[pl.ds(pl.multiple_of(start + i * strip, 8), strip), :]
        dst[pl.ds(off, strip), pl.ds(*lanes)] = total
        return carry

    lax.fori_loop(0, n_rows // strip, body, 0)


class Part:
    def __init__(self, rings, order, rb, sems, x=None, y=None, recv=None, row0=0, lanes=None, align=8, direct=2):
        self.direct = direct
        self.rb, self.sems, self.x, self.y, self.recv = rb, sems, x, y, recv
        self.row0, self.lanes, self.align = row0, lanes, align
        self.places = []
        base = row0
        for phase in range(3):
            slab = rb * RING ** (2 - phase)
            h0 = -(-slab // (2 * align)) * align
            pos, right, left, across = rings[order[phase]]
            starts = [base + ((pos + d) % RING) * slab for d in range(RING)]
            self.places.append((slab, h0, slab - h0, starts, right, left, across))
            base = starts[0]

    def view(self, ref, start, n_rows):
        return ref.at[pl.ds(pl.multiple_of(start, self.align), n_rows), pl.ds(*self.lanes)]

    def place(self, phase):
        return self.places[phase]

    def hop(self, phase, i):
        slab, h0, h1, (own, rgt, opp, lft), right, left, across = self.place(phase)
        if phase >= self.direct:
            start, n_rows, at, device = {
                0: (opp, slab, 0, across),
                2: (rgt, slab, slab, right),
                3: (lft, slab, 2 * slab, left),
                6: (own, slab, 0, right),
                7: (own, slab, 0, left),
                8: (own, slab, 0, across),
            }[i]
        else:
            start, n_rows, at, device = (
                (opp, h0, 0, right),
                (opp + h0, h1, h0, left),
                (rgt + h0, h1, slab + h0, right),
                (lft, h0, 2 * slab, left),
                (rgt, h0, slab, right),
                (lft + h0, h1, 2 * slab + h0, left),
                (own, slab, 0, right),
                (own, slab, 0, left),
                (lft, h0, 0, right),
                (rgt + h0, h1, 0, left),
            )[i]
        if i < 6:
            src, dst = self.view(self.x, start, n_rows), self.recv[phase].at[pl.ds(at, n_rows)]
        else:
            src = dst = self.view(self.y, start, n_rows)
        return remote(src, dst, self.sems, 10 * phase + i, device)

    def rs_start(self, phase):
        for i in (0, 2, 3) if phase >= self.direct else range(4):
            self.hop(phase, i).start()

    def rs_mid(self, phase):
        if phase >= self.direct:
            return
        slab, h0, h1, (own, rgt, opp, lft), *_ = self.place(phase)
        buf = self.recv[phase]
        self.hop(phase, 0).wait_recv()
        add_rows(self.x, rgt, [(buf, 0)], h0, self.lanes)
        self.hop(phase, 4).start()
        self.hop(phase, 1).wait_recv()
        add_rows(self.x, lft + h0, [(buf, h0)], h1, self.lanes)
        self.hop(phase, 5).start()

    def rs_end(self, phase):
        slab, _, _, (own, _, _, _), *_ = self.place(phase)
        buf = self.recv[phase]
        terms = [(buf, slab), (buf, 2 * slab)]
        if phase >= self.direct:
            terms.append((buf, 0))
        for i in (0, 2, 3) if phase >= self.direct else range(2, 6):
            self.hop(phase, i).wait_recv()
        add_rows(self.x, own, terms, slab, self.lanes)

    def ag_start(self, phase):
        for i in (6, 7, 8) if phase >= self.direct else (6, 7):
            self.hop(phase, i).start()

    def ag_mid(self, phase):
        if phase >= self.direct:
            return
        self.hop(phase, 6).wait_recv()
        self.hop(phase, 8).start()
        self.hop(phase, 7).wait_recv()
        self.hop(phase, 9).start()

    def ag_end(self, phase):
        for i in (6, 7, 8) if phase >= self.direct else (8, 9):
            self.hop(phase, i).wait_recv()

    def own_rows(self):
        return self.place(2)[3][0]

    def drain(self, rs=(), ag=()):
        for phase in rs:
            for i in (0, 2, 3) if phase >= self.direct else range(6):
                self.hop(phase, i).wait_send()
        for phase in ag:
            for i in (6, 7, 8) if phase >= self.direct else range(6, 10):
                self.hop(phase, i).wait_send()


def stage(parts, step):
    for part in parts:
        getattr(part, step[:-1])(int(step[-1]))


def slab_rows(rb):
    return [3 * rb * RING ** (2 - phase) for phase in range(3)]


def place_in_order(block, order):
    digit = [(block // s) % RING for s in AXIS_STRIDE]
    return (digit[order[0]] * RING + digit[order[1]]) * RING + digit[order[2]]


def by_rows(n_rows, align):
    unit = n_rows // align
    counts = [(unit + 2 - c) // 3 for c in range(3)]
    starts = [sum(counts[:c]) * align for c in range(3)]
    return [(starts[c], counts[c] * align) for c in range(3)]


def pair(n):
    return [pltpu.SemaphoreType.DMA((n,)), pltpu.SemaphoreType.DMA((n,))]


def thirds(n, unit):
    most = n * 3 // 8
    sizes = (most, most, n - 2 * most)
    return [(unit * most * c, unit * size) for c, size in enumerate(sizes)]


def wide_lanes(d_model):
    few = d_model // 128 * 5 // 16 * 128
    sizes = (few, d_model - 2 * few, few)
    return [(sum(sizes[:c]), size) for c, size in enumerate(sizes)]


def spread(ring, src_of, dst, n_rows, sems):
    pos, right, left, across = ring
    rows = dst.at[pl.ds(pl.multiple_of(pos * n_rows, n_rows), n_rows)]
    hops = enumerate((right, across, left))
    return [remote(src_of((pos + i + 1) % RING), rows, sems, i, device) for i, device in hops]


def place_heads(dst, src):
    n_batch, n_rows, head_dim = src.shape
    for b in range(n_batch):
        for h in range(n_rows // BLK):
            dst[pl.ds(b * BLK, BLK), pl.ds(h * head_dim, head_dim)] = src[b, h * BLK:(h + 1) * BLK, :]


D_TILE = 256


class Return:
    def __init__(self, src, dst, sems):
        self.src, self.dst, self.sems = src, dst, sems
        self.cp, self.tp = lax.axis_index("cp"), lax.axis_index("tp")
        self.mirror = RING ** 3 - 1 - self.cp
        self.group = self.cp // (RING ** 3 // 2)
        self.is_mine = self.tp == self.group

    def give(self, piece_idx):
        device = (self.group, self.mirror) if piece_idx else (1 - self.tp, self.cp)
        return pltpu.make_async_remote_copy(src_ref=self.src.at[piece_idx], dst_ref=self.dst.at[self.tp], send_sem=self.sems[0].at[piece_idx], recv_sem=self.sems[1].at[self.tp], device_id=device, device_id_type=MESH)

    def take(self, batch):
        return pltpu.make_async_remote_copy(src_ref=self.src.at[1], dst_ref=self.dst.at[batch], send_sem=self.sems[0].at[1], recv_sem=self.sems[1].at[batch], device_id=(self.group, self.mirror), device_id_type=MESH)

    def start(self):
        self.give(1).start()

        @pl.when(jnp.logical_not(self.is_mine))
        def _():
            self.give(0).start()

        @pl.when(self.is_mine)
        def _():
            self.dst[self.tp] = self.src[0]

    def wait(self):
        self.take(1 - self.tp).wait_recv()

        @pl.when(jnp.logical_not(self.is_mine))
        def _():
            self.take(self.tp).wait_recv()

    def drain(self):
        self.give(1).wait_send()

        @pl.when(jnp.logical_not(self.is_mine))
        def _():
            self.give(0).wait_send()


class Handout:
    def __init__(self, src, dst, sems):
        self.src, self.dst, self.sems = src, dst, sems
        self.cp, self.tp = lax.axis_index("cp"), lax.axis_index("tp")
        self.mirror = RING ** 3 - 1 - self.cp
        self.is_mine = self.tp == self.cp // (RING ** 3 // 2)

    def copy(self, kind, batch, slot, device, sem):
        return pltpu.make_async_remote_copy(src_ref=self.src[kind].at[batch], dst_ref=self.dst.at[slot, kind], send_sem=self.sems[0].at[2 * kind + sem], recv_sem=self.sems[1].at[2 * kind + slot], device_id=device, device_id_type=MESH)

    def near(self, kind):
        return self.copy(kind, 1 - self.tp, 0, (1 - self.tp, self.cp), 0)

    def far(self, kind, batch):
        return self.copy(kind, batch, 1, (batch, self.mirror), batch)

    def start(self, kind):
        @pl.when(self.is_mine)
        def _():
            self.near(kind).start()
            self.dst[0, kind] = self.src[kind][self.tp]

        @pl.when(jnp.logical_not(self.is_mine))
        def _():
            self.far(kind, 0).start()
            self.far(kind, 1).start()

    def wait(self, kind):
        self.far(kind, 0).wait_recv()

        @pl.when(jnp.logical_not(self.is_mine))
        def _():
            self.near(kind).wait_recv()

    def drain(self, kind):
        @pl.when(self.is_mine)
        def _():
            self.near(kind).wait_send()

        @pl.when(jnp.logical_not(self.is_mine))
        def _():
            self.far(kind, 0).wait_send()
            self.far(kind, 1).wait_send()


D_TILE = 256


def attn_kernel(k_ref, v_ref, q_ref, hid_ref, grad_ref, wo_ref, cos_ref, sin_ref, oh_ref, dqh_ref, dkv_ref, red0, red1, red2, ho0, ho1, ho2, y0, y1, y2, kv_scr, qd_scr, o_scr, qt_scr, dot_scr, dqt_scr, m_scr, l_scr, delta_scr, p_scr, ds_scr, xo, tok_scr, rot_scr, oh_scr, dqh_scr, do_home, *rest):
    rest = list(rest)

    def grab(n):
        return [rest.pop(0) for _ in range(n)]

    recv, hr = grab(3), grab(3)
    k_sems, o_sems, h_sems = ([grab(2) for _ in range(3)] for _ in range(3))
    hand_sems, oh_sems, dqh_sems, (h_out,) = grab(2), grab(2), grab(2), rest
    n_groups, _, n_cols, e_dim = qd_scr.shape
    rows = k_ref.shape[0]
    per_tile = TILE // BLK
    n_blk = RING ** 3
    d_model = grad_ref.shape[1]
    cp = lax.axis_index("cp")
    mirror = n_blk - 1 - cp
    rings = [ring_of(axis) for axis in range(3)]
    o_lanes = wide_lanes(d_model)
    ys = (y0, y1, y2)
    split = by_rows(rows, 16)
    p_kv = [Part(rings, ORDERS[c], split[c][1], k_sems[c], y=ys[c], lanes=(0, 2 * e_dim), align=16, direct=1) for c in range(3)]
    p_o = [Part(rings, ORDERS[c], n_cols // n_blk, o_sems[c], x=xo, recv=[recv[c]], lanes=o_lanes[c]) for c in range(3)]
    hand = Handout((q_ref, do_home), qd_scr, hand_sems)
    o_back = Return(o_scr, oh_scr, oh_sems)
    dq_back = Return(rot_scr, dqh_scr, dqh_sems)

    for c in range(3):
        own = pl.ds(pl.multiple_of(p_kv[c].own_rows(), 16), split[c][1])
        ys[c][own, :e_dim] = k_ref[pl.ds(*split[c]), :]
        ys[c][own, e_dim:] = v_ref[pl.ds(*split[c]), :]
    enter(rings, with_partner=True, with_mirror=True)
    stage(p_kv, "ag_start2")
    stage(p_kv, "ag_end2")
    stage(p_kv, "ag_start1")
    hand.start(0)
    stage(p_kv, "ag_end1")
    stage(p_kv, "ag_start0")
    for cols in range(0, n_cols, COLS):
        res = lax.dot_general(grad_ref[...], wo_ref[pl.ds(cols, COLS), :], (((1,), (1,)), ((), ())), preferred_element_type=F32).astype(BF16)
        for b in range(n_groups):
            for h in range(COLS // e_dim):
                do_home[b, pl.ds(cols + h * rows, rows), :] = res[b * rows:(b + 1) * rows, h * e_dim:(h + 1) * e_dim]
    dqt_scr[...] = jnp.zeros_like(dqt_scr)
    dkv_ref[...] = jnp.zeros_like(dkv_ref)
    m_scr[...] = jnp.full_like(m_scr, -jnp.inf)
    l_scr[...] = jnp.zeros_like(l_scr)
    hand.wait(0)
    for grp in range(n_groups):
        qt_scr[grp] = qd_scr[grp, 0].T
    stage(p_kv, "ag_mid0")
    hand.start(1)
    stage(p_kv, "ag_end0")

    def place_kv(blk, carry):
        for c in range(3):
            at, rb = split[c]
            src = pl.ds(pl.multiple_of(place_in_order(blk, ORDERS[c]) * rb, 16), rb)
            kv_scr[pl.ds(pl.multiple_of(blk * rows + at, 16), rb), :] = ys[c][src, :]
        return carry

    h_slab = d_model // RING
    n_tok = hid_ref.shape[0]

    def hid_cols(pos):
        return hid_ref.at[:, pl.ds(pl.multiple_of(pos * h_slab, h_slab), h_slab)]

    h_sent = []
    for c in range(3):
        ring = rings[ORDERS[c][0]]
        h_sent += spread(ring, hid_cols, hr[c], n_tok, h_sems[c])
        hr[c][pl.ds(pl.multiple_of(ring[0] * n_tok, n_tok), n_tok), :] = hid_cols(ring[0])[...]
    for copy in h_sent:
        copy.start()
    lax.fori_loop(0, n_blk, place_kv, 0)

    n_first = cp // per_tile + 1
    n_steps = n_blk // per_tile + 1

    def over_tiles(tile_step, extra):
        def body(t, carry):
            grp = (t - n_first + n_steps) // n_steps
            piece = cp + grp * (mirror - cp)
            tile_idx = t - grp * n_first
            last = tile_idx == piece // per_tile

            @pl.when(jnp.logical_not(last))
            def _():
                tile_step(grp, tile_idx, piece, False)

            @pl.when(last)
            def _():
                tile_step(grp, tile_idx, piece, True)

            for when, action in extra:
                pl.when(t == when)(action)
            return carry

        lax.fori_loop(0, n_steps, body, 0)

    def fwd_step(grp, tile_idx, piece, masked):
        row0 = pl.multiple_of(tile_idx * TILE, TILE)
        k_t = kv_scr[pl.ds(row0, TILE), :e_dim]
        v_t = kv_scr[pl.ds(row0, TILE), e_dim:]
        for c0 in range(0, n_cols, COLS):
            cs = slice(c0, c0 + COLS)
            s = dot(k_t, qt_scr[grp, :, cs])
            if masked:
                s = jnp.where(causal_mask(row0, piece * BLK, COLS), s, -jnp.inf)
            m_old = m_scr[grp, :, cs]
            m_new = jnp.maximum(m_old, jnp.max(s, axis=0, keepdims=True))
            p = jnp.exp(s - m_new)
            alpha = jnp.exp(m_old - m_new)
            m_scr[grp, :, cs] = m_new
            l_scr[grp, :, cs] = l_scr[grp, :, cs] * alpha + jnp.sum(p, axis=0, keepdims=True)
            dqt_scr[grp, :, cs] = dqt_scr[grp, :, cs] * alpha + dot_ta(v_t, p.astype(BF16))

    over_tiles(fwd_step, ())
    hand.wait(1)
    for grp in range(n_groups):
        o_t = (dqt_scr[grp] / l_scr[grp]).astype(BF16)
        o_scr[grp] = o_t.T
        dot_scr[grp] = qd_scr[grp, 1].T
        delta_scr[grp] = jnp.sum(dot_scr[grp].astype(F32) * o_t.astype(F32), axis=0, keepdims=True)
    o_back.start()
    m_scr[...] = m_scr[...] + jnp.log(l_scr[...])
    dqt_scr[...] = jnp.zeros_like(dqt_scr)

    def bwd_step(grp, tile_idx, piece, masked):
        row0 = pl.multiple_of(tile_idx * TILE, TILE)
        k_t = kv_scr[pl.ds(row0, TILE), :e_dim]
        v_t = kv_scr[pl.ds(row0, TILE), e_dim:]
        for c0 in range(0, n_cols, COLS):
            cs = slice(c0, c0 + COLS)
            s = dot(k_t, qt_scr[grp, :, cs])
            p = jnp.exp(s - m_scr[grp, :, cs])
            if masked:
                p = jnp.where(causal_mask(row0, piece * BLK, COLS), p, 0.0)
            d_p = dot(v_t, dot_scr[grp, :, cs])
            p_scr[:, cs] = p.astype(BF16)
            ds_scr[:, cs] = (p * (d_p - delta_scr[grp, :, cs])).astype(BF16)
        at = pl.ds(row0, TILE)
        dkv_ref[at, :e_dim] += dot(ds_scr[...], qd_scr[grp, 0])
        dkv_ref[at, e_dim:] += dot(p_scr[...], qd_scr[grp, 1])
        dqt_scr[grp] += dot_ta(k_t, ds_scr[...])

    def sum_wo_start():
        o_back.wait()
        place_heads(tok_scr, oh_scr)

        def o_body(i, carry):
            cols = pl.ds(pl.multiple_of(i * D_TILE, D_TILE), D_TILE)
            xo[:, cols] = dot_ta(tok_scr[...], grad_ref[:, cols])
            return carry

        lax.fori_loop(0, d_model // D_TILE, o_body, 0)
        stage(p_o, "rs_start0")

    over_tiles(bwd_step, ((3, sum_wo_start), (9, lambda: stage(p_o, "rs_mid0"))))

    scale = e_dim ** -0.5
    half_dim = e_dim // 2
    for grp in range(n_groups):
        cos_t, sin_t = cos_ref[grp], sin_ref[grp]
        for h in range(n_cols // rows):
            cols = slice(h * rows, (h + 1) * rows)
            low, high = dqt_scr[grp, :half_dim, cols], dqt_scr[grp, half_dim:, cols]
            turned = jnp.concatenate([low * cos_t + high * sin_t, high * cos_t - low * sin_t], axis=0) * scale
            rot_scr[grp, cols, :] = turned.T.astype(BF16)
    dq_back.start()
    for copy in h_sent:
        copy.wait_recv()
    h_outs = [pltpu.make_async_copy(hr[c], out, h_out.at[c]) for c, out in enumerate((ho0, ho1, ho2))]
    for copy in h_outs:
        copy.start()
    oh_ref[...] = oh_scr[...]
    stage(p_o, "rs_end0")
    for part, out, lanes in zip(p_o, (red0, red1, red2), o_lanes):
        slab, _, _, starts, *_ = part.place(0)
        out[...] = xo[pl.ds(pl.multiple_of(starts[0], 8), slab), pl.ds(*lanes)]
    dq_back.wait()
    dqh_ref[...] = dqh_scr[...]
    for part in p_kv:
        part.drain(ag=range(3))
    for part in p_o:
        part.drain(rs=(0,))
    for kind in range(2):
        hand.drain(kind)
    for copy in h_sent:
        copy.wait_send()
    for copy in h_outs:
        copy.wait()
    o_back.drain()
    dq_back.drain()


def attention(key_loc, val_loc, q_home, hid, grad, w_out, cos_t, sin_t):
    n_batch, n_cols, e_dim = q_home.shape
    rows = key_loc.shape[0]
    n_tok, d_model = grad.shape
    n_blk = RING ** 3
    seq = n_blk * rows
    o_lanes = wide_lanes(d_model)
    slab = n_cols // RING
    vmem = pl.BlockSpec(memory_space=pltpu.VMEM)
    heads = (2, n_cols, e_dim)
    h_ring = (RING * n_tok, d_model // RING)
    work = n_cols * seq
    return pl.pallas_call(
        attn_kernel,
        out_shape=(jax.ShapeDtypeStruct(heads, BF16), jax.ShapeDtypeStruct(heads, BF16), jax.ShapeDtypeStruct((seq, 2 * e_dim), F32)) + tuple(jax.ShapeDtypeStruct((slab, n), F32) for _, n in o_lanes) + (jax.ShapeDtypeStruct(h_ring, BF16),) * 3,
        in_specs=[vmem] * 8,
        out_specs=(vmem,) * 6 + (pl.BlockSpec(memory_space=pl.ANY),) * 3,
        scratch_shapes=[pltpu.VMEM((n_blk * rb, 2 * e_dim), BF16) for _, rb in by_rows(rows, 16)]
        + [
            pltpu.VMEM((seq, 2 * e_dim), BF16),
            pltpu.VMEM((2, 2, n_cols, e_dim), BF16),
            pltpu.VMEM(heads, BF16),
            pltpu.VMEM((2, e_dim, n_cols), BF16),
            pltpu.VMEM((2, e_dim, n_cols), BF16),
            pltpu.VMEM((2, e_dim, n_cols), F32),
            pltpu.VMEM((2, 1, n_cols), F32),
            pltpu.VMEM((2, 1, n_cols), F32),
            pltpu.VMEM((2, 1, n_cols), F32),
            pltpu.VMEM((TILE, n_cols), BF16),
            pltpu.VMEM((TILE, n_cols), BF16),
            pltpu.VMEM((n_cols, d_model), F32),
            pltpu.VMEM((n_tok, n_cols), BF16),
        ]
        + [pltpu.VMEM(heads, BF16)] * 4
        + [pltpu.VMEM((3 * slab, lanes), F32) for _, lanes in o_lanes]
        + [pltpu.VMEM(h_ring, BF16)] * 3
        + pair(30) * 6
        + pair(3) * 3
        + pair(4)
        + pair(2) * 2
        + [pltpu.SemaphoreType.DMA((3,))],
        compiler_params=pltpu.CompilerParams(collective_id=2, has_side_effects=True, vmem_limit_bytes=64000000),
        cost_estimate=pl.CostEstimate(flops=14 * work * e_dim, bytes_accessed=seq * e_dim * 12, transcendentals=2 * work),
        name="attention",
    )(key_loc, val_loc, q_home, hid, grad, w_out, cos_t, sin_t)


GRAD_PLAN = (
    "r.rs_start1", "d.rs_start0", "weights.q", "d.rs_mid0", "r.rs_mid1", "s.rs_start1", "d.rs_end0", "d.rs_start1",
    "r.rs_end1", "s.rs_mid1", "d.rs_mid1", "r.rs_start2", "s.rs_end1", "d.rs_end1", "d.rs_start2", "s.rs_start2",
    "r.rs_end2", "o.ag_start2", "d.rs_end2", "weights.prep", "weights.kv", "s.rs_end2", "q.ag_start2", "o.ag_end2",
    "o.ag_start1", "weights.slab", "t.rs_start1", "q.ag_end2", "q.ag_start1", "t.rs_mid1", "o.ag_mid1", "t.rs_end1",
    "t.rs_start2", "q.ag_mid1", "t.rs_end2", "k.ag_start2", "o.ag_end1", "o.ag_start0", "k.ag_end2", "q.ag_end1",
    "k.ag_start1", "k.ag_mid1", "q.ag_start0", "k.ag_end1", "k.ag_start0", "o.ag_mid0", "k.ag_mid0", "q.ag_mid0",
    "k.ag_end0", "o.ag_end0", "q.ag_end0",
)


def grad_kernel(dkv_ref, dqh_ref, red0, red1, red2, hi0, hi1, hi2, cos_ref, sin_ref, gq_ref, go_ref, gk_ref, gv_ref, dkd_ref, yq, yo, yk, yp, turn_scr, tok_scr, kvt_scr, kvr_scr, mine_scr, give_scr, got_scr, xk, *rest):
    rest = list(rest)

    def grab(n):
        return [rest.pop(0) for _ in range(n)]

    n_blk = RING ** 3
    n_batch, _, head_dim = dqh_ref.shape
    n_tok, n_cols = tok_scr.shape
    d_model = yq.shape[0]
    rows, lanes = n_tok // n_batch, 2 * head_dim
    n_local = n_cols // head_dim
    q_lanes, o_lanes = thirds(n_local, head_dim), wide_lanes(d_model)
    split = by_rows(rows, 8)
    tp, cp = lax.axis_index("tp"), lax.axis_index("cp")
    partner = (1 - tp, cp)
    rings = [ring_of(axis) for axis in range(3)]
    colours = range(3)

    def shifted(c, n_rows):
        return 0 - rings[ORDERS[c][0]][0] * (n_rows // RING)

    xs, xos, xqs, hr, dqr = (grab(3) for _ in range(5))
    sem_d, sem_q, sem_o, sem_g = ([grab(2) for _ in colours] for _ in range(4))
    sem_k, sem_kr = grab(2), grab(2)
    p_d = [Part(rings, ORDERS[c], split[c][1], sem_d[c], x=xs[c], recv=grab(3), lanes=(0, lanes)) for c in colours]
    p_s = [Part(rings, ORDERS[c], d_model // n_blk, sem_q[c], x=xqs[c], recv=[None] + grab(2), row0=shifted(c, d_model), lanes=(0, q_lanes[c][1])) for c in colours]
    p_q = [Part(rings, ORDERS[c], d_model // n_blk, sem_q[c], y=yq, lanes=q_lanes[c]) for c in colours]
    p_r = [Part(rings, ORDERS[c], n_cols // n_blk, sem_o[c], x=xos[c], recv=[None] + grab(2), row0=shifted(c, n_cols), lanes=(0, o_lanes[c][1])) for c in colours]
    p_o = [Part(rings, ORDERS[c], n_cols // n_blk, sem_o[c], y=yo, lanes=o_lanes[c]) for c in colours]
    p_t = [Part(rings, ORDERS[2], d_model // n_blk, sem_k, x=xk, recv=[None] + grab(2), row0=shifted(2, d_model), lanes=(0, head_dim))]
    p_k = [Part(rings, ORDERS[2], d_model // n_blk, sem_k, y=yk, lanes=(0, head_dim))]
    in_sem, out_sem, swap_s, swap_r = rest

    def load(blk, carry):
        for c in range(3):
            at, rb = split[c]
            dst = xs[c].at[pl.ds(pl.multiple_of(place_in_order(blk, ORDERS[c]) * rb, 8), rb)]
            pltpu.make_async_copy(dkv_ref.at[pl.ds(pl.multiple_of(blk * rows + at, 8), rb)], dst, in_sem.at[c]).start()
        return carry

    lax.fori_loop(0, n_blk, load, 0)
    loads = [pltpu.make_async_copy(src, dst, in_sem.at[3 + i]) for i, (src, dst) in enumerate(zip((red0, red1, red2, hi0, hi1, hi2), xos + hr))]
    for copy in loads:
        copy.start()
    place_heads(tok_scr, dqh_ref)

    def tok_cols(c):
        return pl.ds(*q_lanes[c])

    dq_sent = []
    for c in colours:
        ring = rings[ORDERS[c][0]]
        dqr[c][pl.ds(pl.multiple_of(ring[0] * n_tok, n_tok), n_tok), :] = tok_scr[:, tok_cols(c)]
        dq_sent += spread(ring, lambda pos, c=c: tok_scr.at[:, tok_cols(c)], dqr[c], n_tok, sem_g[c])
    ring_k = rings[ORDERS[2][0]]
    kv_sent = spread(ring_k, lambda pos: kvt_scr, kvr_scr, n_tok, sem_kr)
    enter(rings, with_partner=True)
    for copy in dq_sent:
        copy.start()
    for copy in loads:
        copy.wait()
    for c in colours:
        pltpu.make_async_copy(dkv_ref.at[pl.ds(0, n_blk * split[c][1])], xs[c], in_sem.at[c]).wait()
    half_dim = head_dim // 2
    first = tp == 0
    swap_small = pltpu.make_async_remote_copy(src_ref=give_scr, dst_ref=got_scr, send_sem=swap_s.at[0], recv_sem=swap_r.at[0], device_id=partner, device_id_type=MESH)
    swap = pltpu.make_async_remote_copy(src_ref=yk, dst_ref=yp, send_sem=swap_s.at[1], recv_sem=swap_r.at[1], device_id=partner, device_id_type=MESH)

    def put_o(which):
        for c, part in enumerate(p_o):
            slab, _, _, starts, *_ = part.place(0)
            for i in which:
                pltpu.make_async_copy(part.view(yo, starts[i], slab), part.view(go_ref, starts[i], slab), out_sem.at[c]).start()

    def turn_q(which):
        for c, part in enumerate(p_q):
            slab, _, _, starts, *_ = part.place(0)
            for i in which:
                at = pl.multiple_of(starts[i], slab)
                for h in range(q_lanes[c][0] // head_dim, sum(q_lanes[c]) // head_dim):
                    turn_scr[pl.ds(at * n_local + h, slab, stride=n_local), :] = yq[pl.ds(at, slab), pl.ds(h * head_dim, head_dim)]

    def own_block(parts, sums):
        for part, total in zip(parts, sums):
            at, lanes_y, lanes_x = part.own_rows(), pl.ds(*part.lanes), pl.ds(*total.lanes)
            part.y[pl.ds(pl.multiple_of(at, 8), part.rb), lanes_y] = total.x[pl.ds(pl.multiple_of(total.own_rows(), 8), part.rb), lanes_x]

    def slab_term(dst, hid, other):
        for at in range(0, dst.shape[0], D_TILE):
            dst[pl.ds(at, D_TILE), :] = dot_ta(hid[:, at:at + D_TILE], other[...])

    def weights_q():
        for copy in dq_sent:
            copy.wait_recv()
        for c in colours:
            slab_term(xqs[c], hr[c], dqr[c])

    def new_dkv():
        dkd_ref[...] = mine_scr[...].astype(BF16)
        return dkd_ref[:, :head_dim], dkd_ref[:, head_dim:]

    def weights_prep():
        for c in range(3):
            at, rb = split[c]
            own = xs[c][pl.ds(pl.multiple_of(p_d[c].own_rows(), 8), rb), :]
            cos_tab, sin_tab = cos_ref[pl.ds(at, rb), :], sin_ref[pl.ds(at, rb), :]
            low, high = own[:, :half_dim], own[:, half_dim:head_dim]
            mine_scr[pl.ds(at, rb), :head_dim] = jnp.concatenate([low * cos_tab + high * sin_tab, high * cos_tab - low * sin_tab], axis=1)
            mine_scr[pl.ds(at, rb), head_dim:] = own[:, head_dim:]
        dk_new, dv_new = new_dkv()
        give_scr[...] = jnp.where(first, dv_new, dk_new)
        swap_small.start()

    def weights_kv():
        swap_small.wait()
        got = got_scr[...]
        keep = jnp.where(first, dkd_ref[:, :head_dim], dkd_ref[:, head_dim:])
        kvt_scr[...] = jnp.concatenate([jnp.where(first, keep, got), jnp.where(first, got, keep)], axis=0)
        kvr_scr[pl.ds(pl.multiple_of(ring_k[0] * n_tok, n_tok), n_tok), :] = kvt_scr[...]
        for copy in kv_sent:
            copy.start()

    def weights_slab():
        for copy in kv_sent:
            copy.wait_recv()
        slab_term(xk, hr[2], kvr_scr)

    groups = {"d": p_d, "s": p_s, "q": p_q, "r": p_r, "o": p_o, "t": p_t, "k": p_k}
    after = {
        "weights.q": weights_q,
        "weights.prep": weights_prep,
        "weights.kv": weights_kv,
        "weights.slab": weights_slab,
        "r.rs_end2": lambda: own_block(p_o, p_r),
        "s.rs_end2": lambda: own_block(p_q, p_s),
        "t.rs_end2": lambda: own_block(p_k, p_t),
        "o.ag_mid0": lambda: put_o((0, 1, 3)),
        "o.ag_end0": lambda: put_o((2,)),
        "q.ag_start0": lambda: turn_q((0,)),
        "q.ag_mid0": lambda: turn_q((1, 3)),
        "q.ag_end0": lambda: turn_q((2,)),
        "k.ag_end0": swap.start,
    }
    for step in GRAD_PLAN:
        who, what = step.split(".")
        if who in groups:
            stage(groups[who], what)
        if step in after:
            after[step]()
    out_q = pltpu.make_async_copy(turn_scr, gq_ref, out_sem.at[3])
    out_q.start()
    swap.wait()

    def put_kv(k_src, v_src):
        outs = [pltpu.make_async_copy(k_src, gk_ref, out_sem.at[4]), pltpu.make_async_copy(v_src, gv_ref, out_sem.at[5])]
        for copy in outs:
            copy.start()
        for copy in outs:
            copy.wait()

    @pl.when(first)
    def _():
        put_kv(yk, yp)

    @pl.when(jnp.logical_not(first))
    def _():
        put_kv(yp, yk)

    out_q.wait()
    for c, part in enumerate(p_o):
        pltpu.make_async_copy(part.view(yo, 0, n_cols), part.view(go_ref, 0, n_cols), out_sem.at[c]).wait()
    for part in p_d:
        part.drain(rs=range(3))
    for part in p_s + p_r + p_t:
        part.drain(rs=(1, 2))
    for part in p_q + p_o + p_k:
        part.drain(ag=range(3))
    for copy in dq_sent + kv_sent:
        copy.wait_send()


def grad_sums(dkv, dq_home, reds, h_rings, cos_tab, sin_tab, d_model):
    n_batch, n_rows, head_dim = dq_home.shape
    rows = cos_tab.shape[0]
    n_tok, n_cols = n_batch * rows, n_rows // rows * head_dim
    n_blk = RING ** 3
    lanes = 2 * head_dim
    q_lanes, o_lanes = thirds(n_cols // head_dim, head_dim), wide_lanes(d_model)
    split = by_rows(rows, 8)
    vmem, anyspace = pl.BlockSpec(memory_space=pltpu.VMEM), pl.BlockSpec(memory_space=pl.ANY)

    def full(*shape):
        return pltpu.VMEM(shape, F32)

    def half(*shape):
        return pltpu.VMEM(shape, BF16)

    def later(rb, width):
        return [full(n, width) for n in slab_rows(rb)[1:]]

    slab, ring_tok = d_model // RING, RING * n_tok
    scratch = [full(d_model, n_cols), full(n_cols, d_model), full(d_model, head_dim), full(d_model, head_dim), full(d_model * n_cols // head_dim, head_dim)]
    scratch += [half(n_tok, n_cols), half(n_tok, head_dim), half(ring_tok, head_dim), full(rows, lanes), half(rows, head_dim), half(rows, head_dim), full(slab, head_dim)]
    scratch += [full(n_blk * rb, lanes) for _, rb in split]
    scratch += [full(n_cols // RING, w) for _, w in o_lanes] + [full(slab, w) for _, w in q_lanes]
    scratch += [half(ring_tok, slab)] * 3 + [half(ring_tok, w) for _, w in q_lanes]
    scratch += pair(30) * 9 + pair(3) * 3 + pair(30) + pair(3)
    scratch += [full(n, lanes) for _, rb in split for n in slab_rows(rb)]
    for _, w in q_lanes:
        scratch += later(d_model // n_blk, w)
    for _, w in o_lanes:
        scratch += later(n_cols // n_blk, w)
    scratch += later(d_model // n_blk, head_dim)
    scratch += [pltpu.SemaphoreType.DMA((9,)), pltpu.SemaphoreType.DMA((6,))] + pair(2)
    return pl.pallas_call(
        grad_kernel,
        out_shape=(
            jax.ShapeDtypeStruct((d_model * n_cols // head_dim, head_dim), F32),
            jax.ShapeDtypeStruct((n_cols, d_model), F32),
            jax.ShapeDtypeStruct((d_model, head_dim), F32),
            jax.ShapeDtypeStruct((d_model, head_dim), F32),
            jax.ShapeDtypeStruct((rows, lanes), BF16),
        ),
        in_specs=[anyspace, vmem] + [anyspace] * 6 + [vmem] * 2,
        out_specs=(anyspace,) * 4 + (vmem,),
        scratch_shapes=scratch,
        compiler_params=pltpu.CompilerParams(collective_id=3, has_side_effects=True, vmem_limit_bytes=67000000),
        cost_estimate=pl.CostEstimate(flops=n_tok * d_model * n_cols * 160, bytes_accessed=40 << 20, transcendentals=0),
        name="grad_sums",
    )(dkv, dq_home, *reds, *h_rings, cos_tab, sin_tab)


def solution(mesh):
    cp_size = mesh.shape["cp"]
    partner = [(0, 1), (1, 0)]

    def local_program(hidden, grad_out, w_query, w_key, w_value, w_out):
        block_len = hidden.shape[1]
        n_local = w_query.shape[1]
        head_dim = w_key.shape[1]
        q_scale = head_dim ** -0.5
        cp_idx = lax.axis_index("cp")
        tp_idx = lax.axis_index("tp")
        mirror_idx = cp_size - 1 - cp_idx
        cos_tab, sin_tab = rope_tables(cp_idx * block_len + jnp.arange(block_len), head_dim)
        cos_mir, sin_mir = rope_tables(mirror_idx * block_len + jnp.arange(block_len), head_dim)

        def pick(pair, idx):
            return lax.dynamic_index_in_dim(pair, idx, 0, keepdims=False)

        def sum_over_tp(part, extra=None):
            total = pick(part, tp_idx) + lax.ppermute(pick(part, 1 - tp_idx), "tp", partner)
            if extra is not None:
                total = total + extra
            mine = total.astype(BF16)
            other = lax.ppermute(mine, "tp", partner)
            first = tp_idx == 0
            return jnp.stack([jnp.where(first, mine, other), jnp.where(first, other, mine)])

        hid_b = pick(hidden, tp_idx)
        key_loc = rotate(dot(hid_b, w_key), cos_tab, sin_tab).astype(BF16)
        val_loc = dot(hid_b, w_value).astype(BF16)
        q_pre = jnp.einsum("bsd,dhe->bhse", hidden, w_query, preferred_element_type=F32)
        queries = (rotate(q_pre, cos_tab, sin_tab) * q_scale).astype(BF16)
        q_home = queries.reshape(2, n_local * block_len, head_dim)
        d_model = hidden.shape[-1]
        hid, grad = hidden.reshape(-1, d_model), grad_out.reshape(-1, d_model)
        tabs_t = [jnp.stack(pair_t) for pair_t in ((cos_tab.T, cos_mir.T), (sin_tab.T, sin_mir.T))]
        o_home, dq_home, dkv, *more = attention(key_loc, val_loc, q_home, hid, grad, w_out.reshape(-1, d_model), *tabs_t)
        attn_heads = o_home.reshape(2, n_local, block_len, head_dim)
        dq_pre = dq_home.reshape(2, n_local, block_len, head_dim)
        attn_out = sum_over_tp(jnp.einsum("cirf,ife->cre", attn_heads, w_out, preferred_element_type=F32))
        grad_q, grad_o, d_w_key, d_w_value, dkv_new = grad_sums(dkv, dq_home, more[:3], more[3:], cos_tab, sin_tab, d_model)
        d_w_query = grad_q.reshape(w_query.shape)
        d_w_out = grad_o.reshape(w_out.shape)
        dk_pre, dv_pre = dkv_new[:, :head_dim], dkv_new[:, head_dim:]
        dh_kv = dot(dk_pre, w_key.T) + dot(dv_pre, w_value.T)
        d_hidden = sum_over_tp(jnp.einsum("cirf,eif->cre", dq_pre, w_query, preferred_element_type=F32), dh_kv)
        return attn_out, d_hidden, d_w_query, d_w_key, d_w_value, d_w_out

    row_spec = P(None, "cp", None)
    return jax.shard_map(local_program, mesh=mesh, in_specs=(row_spec, row_spec, P(None, "tp", None), P(), P(), P("tp", None, None)), out_specs=(row_spec, row_spec, P(None, "tp", None), P(), P(), P("tp", None, None)), check_vma=False)
```

```python
import jax
import jax.numpy as jnp
from jax import lax
from jax.experimental import pallas as pl
from jax.experimental.pallas import tpu as pltpu
from jax.sharding import PartitionSpec as P

ROPE_BASE = 10000.0
BLK = 128
TILE = 512
COLOURS = range(3)
VMEM_LIMIT = 67000000
COLS = 256
F32 = jnp.float32
BF16 = jnp.bfloat16


def rope_tables(positions, head_dim):
    half_dim = head_dim // 2
    inv_freq = 1.0 / jnp.power(ROPE_BASE, jnp.arange(half_dim, dtype=F32) * (2.0 / head_dim))
    angles = positions.astype(F32)[:, None] * inv_freq[None, :]
    return jnp.cos(angles), jnp.sin(angles)


def rotate(rot_in, cos_tab, sin_tab):
    half_dim = rot_in.shape[-1] // 2
    low_half = rot_in[..., :half_dim]
    high_half = rot_in[..., half_dim:]
    return jnp.concatenate([low_half * cos_tab - high_half * sin_tab, high_half * cos_tab + low_half * sin_tab], axis=-1)


def unrotate(rot_in, cos_tab, sin_tab):
    return rotate(rot_in, cos_tab, -sin_tab)


def dot(a, b):
    return jnp.dot(a, b, preferred_element_type=F32)


def dot_ta(a, b):
    return lax.dot_general(a, b, (((0,), (0,)), ((), ())), preferred_element_type=F32)


def causal_mask(k_start, q_start, cols):
    k_pos = k_start + lax.broadcasted_iota(jnp.int32, (TILE, cols), 0)
    q_pos = q_start + lax.broadcasted_iota(jnp.int32, (TILE, cols), 1) % BLK
    return k_pos <= q_pos


RING = 4
AXIS_STRIDE = (RING * RING, RING, 1)
ORDERS = ((0, 1, 2), (1, 2, 0), (2, 0, 1))
MESH = pl.DeviceIdType.MESH


def ring_of(axis):
    cp, tp = lax.axis_index("cp"), lax.axis_index("tp")
    stride = AXIS_STRIDE[axis]
    pos = (cp // stride) % RING
    right = cp + ((pos + 1) % RING - pos) * stride
    left = cp + ((pos + RING - 1) % RING - pos) * stride
    across = cp + ((pos + 2) % RING - pos) * stride
    return pos, (tp, right), (tp, left), (tp, across)


def enter(rings, with_partner=False, with_mirror=False):
    barrier = pltpu.get_barrier_semaphore()
    peers = []
    for _, *others in rings:
        peers += others
    if with_partner:
        peers.append((1 - lax.axis_index("tp"), lax.axis_index("cp")))
    if with_mirror:
        mirror = RING ** 3 - 1 - lax.axis_index("cp")
        peers += [(0, mirror), (1, mirror)]
    for peer in peers:
        pl.semaphore_signal(barrier, inc=1, device_id=peer, device_id_type=MESH)
    pl.semaphore_wait(barrier, len(peers))


def remote(src, dst, sems, idx, device):
    return pltpu.make_async_remote_copy(src_ref=src, dst_ref=dst, send_sem=sems[0].at[idx], recv_sem=sems[1].at[idx], device_id=device, device_id_type=MESH)


def add_rows(dst, dst0, srcs, n_rows, lanes):
    strip = next(s for s in (64, 48, 40, 32, 24, 16, 8) if n_rows % s == 0)
    if lanes[1] > 256:
        strip = next(s for s in (16, 8) if n_rows % s == 0)

    def body(i, carry):
        off = pl.multiple_of(dst0 + i * strip, 8)
        total = dst[pl.ds(off, strip), pl.ds(*lanes)]
        for ref, start in srcs:
            total = total + ref[pl.ds(pl.multiple_of(start + i * strip, 8), strip), :]
        dst[pl.ds(off, strip), pl.ds(*lanes)] = total
        return carry

    lax.fori_loop(0, n_rows // strip, body, 0)


class Part:
    def __init__(self, rings, order, rb, sems, x=None, y=None, recv=None, row0=0, lanes=None, align=8, direct=2):
        self.direct = direct
        self.rb, self.sems, self.x, self.y, self.recv = rb, sems, x, y, recv
        self.row0, self.lanes, self.align = row0, lanes, align
        self.places = []
        base = row0
        for phase in COLOURS:
            slab = rb * RING ** (2 - phase)
            h0 = -(-slab // (2 * align)) * align
            pos, right, left, across = rings[order[phase]]
            starts = [base + ((pos + d) % RING) * slab for d in range(RING)]
            self.places.append((slab, h0, slab - h0, starts, right, left, across))
            base = starts[0]

    def view(self, ref, start, n_rows):
        return ref.at[pl.ds(pl.multiple_of(start, self.align), n_rows), pl.ds(*self.lanes)]

    def place(self, phase):
        return self.places[phase]

    def hop(self, phase, i):
        slab, h0, h1, (own, rgt, opp, lft), right, left, across = self.place(phase)
        if phase >= self.direct:
            start, n_rows, at, device = {
                0: (opp, slab, 0, across),
                2: (rgt, slab, slab, right),
                3: (lft, slab, 2 * slab, left),
                6: (own, slab, 0, right),
                7: (own, slab, 0, left),
                8: (own, slab, 0, across),
            }[i]
        else:
            start, n_rows, at, device = (
                (opp, h0, 0, right),
                (opp + h0, h1, h0, left),
                (rgt + h0, h1, slab + h0, right),
                (lft, h0, 2 * slab, left),
                (rgt, h0, slab, right),
                (lft + h0, h1, 2 * slab + h0, left),
                (own, slab, 0, right),
                (own, slab, 0, left),
                (lft, h0, 0, right),
                (rgt + h0, h1, 0, left),
            )[i]
        if i < 6:
            src, dst = self.view(self.x, start, n_rows), self.recv[phase].at[pl.ds(at, n_rows)]
        else:
            src = dst = self.view(self.y, start, n_rows)
        return remote(src, dst, self.sems, 10 * phase + i, device)

    def rs_start(self, phase):
        for i in (0, 2, 3) if phase >= self.direct else range(4):
            self.hop(phase, i).start()

    def rs_mid(self, phase):
        if phase >= self.direct:
            return
        slab, h0, h1, (own, rgt, opp, lft), *_ = self.place(phase)
        buf = self.recv[phase]
        self.hop(phase, 0).wait_recv()
        add_rows(self.x, rgt, [(buf, 0)], h0, self.lanes)
        self.hop(phase, 4).start()
        self.hop(phase, 1).wait_recv()
        add_rows(self.x, lft + h0, [(buf, h0)], h1, self.lanes)
        self.hop(phase, 5).start()

    def rs_end(self, phase):
        slab, _, _, (own, _, _, _), *_ = self.place(phase)
        buf = self.recv[phase]
        terms = [(buf, slab), (buf, 2 * slab)]
        if phase >= self.direct:
            terms.append((buf, 0))
        for i in (0, 2, 3) if phase >= self.direct else range(2, 6):
            self.hop(phase, i).wait_recv()
        add_rows(self.x, own, terms, slab, self.lanes)

    def ag_start(self, phase):
        for i in (6, 7, 8) if phase >= self.direct else (6, 7):
            self.hop(phase, i).start()

    def ag_mid(self, phase):
        if phase >= self.direct:
            return
        self.hop(phase, 6).wait_recv()
        self.hop(phase, 8).start()
        self.hop(phase, 7).wait_recv()
        self.hop(phase, 9).start()

    def ag_end(self, phase):
        for i in (6, 7, 8) if phase >= self.direct else (8, 9):
            self.hop(phase, i).wait_recv()

    def own_rows(self):
        return self.place(2)[3][0]

    def drain(self, rs=(), ag=()):
        for phase in rs:
            for i in (0, 2, 3) if phase >= self.direct else range(6):
                self.hop(phase, i).wait_send()
        for phase in ag:
            for i in (6, 7, 8) if phase >= self.direct else range(6, 10):
                self.hop(phase, i).wait_send()


def stage(parts, step):
    for part in parts:
        getattr(part, step[:-1])(int(step[-1]))


def slab_rows(rb):
    return [3 * rb * RING ** (2 - phase) for phase in COLOURS]


def place_in_order(block, order):
    digit = [(block // s) % RING for s in AXIS_STRIDE]
    return (digit[order[0]] * RING + digit[order[1]]) * RING + digit[order[2]]


def by_rows(n_rows, align):
    unit = n_rows // align
    counts = [(unit + 2 - c) // 3 for c in COLOURS]
    starts = [sum(counts[:c]) * align for c in COLOURS]
    return [(starts[c], counts[c] * align) for c in COLOURS]


def pair(n):
    return [pltpu.SemaphoreType.DMA((n,)), pltpu.SemaphoreType.DMA((n,))]


def thirds(n, unit):
    most = n * 3 // 8
    sizes = (most, most, n - 2 * most)
    return [(unit * most * c, unit * size) for c, size in enumerate(sizes)]


def wide_lanes(d_model):
    few = d_model // 128 * 5 // 16 * 128
    sizes = (few, d_model - 2 * few, few)
    return [(sum(sizes[:c]), size) for c, size in enumerate(sizes)]


def spread(ring, src_of, dst, n_rows, sems):
    pos, right, left, across = ring
    rows = dst.at[pl.ds(pl.multiple_of(pos * n_rows, n_rows), n_rows)]
    hops = enumerate((right, across, left))
    return [remote(src_of((pos + i + 1) % RING), rows, sems, i, device) for i, device in hops]


def place_heads(dst, src):
    n_batch, n_rows, head_dim = src.shape
    for b in range(n_batch):
        for h in range(n_rows // BLK):
            dst[pl.ds(b * BLK, BLK), pl.ds(h * head_dim, head_dim)] = src[b, h * BLK:(h + 1) * BLK, :]


D_TILE = 256


class Return:
    def __init__(self, src, dst, sems):
        self.src, self.dst, self.sems = src, dst, sems
        self.cp, self.tp = lax.axis_index("cp"), lax.axis_index("tp")
        self.mirror = RING ** 3 - 1 - self.cp
        self.group = self.cp // (RING ** 3 // 2)
        self.is_mine = self.tp == self.group

    def give(self, piece_idx):
        device = (self.group, self.mirror) if piece_idx else (1 - self.tp, self.cp)
        return pltpu.make_async_remote_copy(src_ref=self.src.at[piece_idx], dst_ref=self.dst.at[self.tp], send_sem=self.sems[0].at[piece_idx], recv_sem=self.sems[1].at[self.tp], device_id=device, device_id_type=MESH)

    def take(self, batch):
        return pltpu.make_async_remote_copy(src_ref=self.src.at[1], dst_ref=self.dst.at[batch], send_sem=self.sems[0].at[1], recv_sem=self.sems[1].at[batch], device_id=(self.group, self.mirror), device_id_type=MESH)

    def start(self):
        self.give(1).start()

        @pl.when(jnp.logical_not(self.is_mine))
        def _():
            self.give(0).start()

        @pl.when(self.is_mine)
        def _():
            self.dst[self.tp] = self.src[0]

    def wait(self):
        self.take(1 - self.tp).wait_recv()

        @pl.when(jnp.logical_not(self.is_mine))
        def _():
            self.take(self.tp).wait_recv()

    def drain(self):
        self.give(1).wait_send()

        @pl.when(jnp.logical_not(self.is_mine))
        def _():
            self.give(0).wait_send()


class Handout:
    def __init__(self, src, dst, sems):
        self.src, self.dst, self.sems = src, dst, sems
        self.cp, self.tp = lax.axis_index("cp"), lax.axis_index("tp")
        self.mirror = RING ** 3 - 1 - self.cp
        self.is_mine = self.tp == self.cp // (RING ** 3 // 2)

    def copy(self, kind, batch, slot, device, sem):
        return pltpu.make_async_remote_copy(src_ref=self.src[kind].at[batch], dst_ref=self.dst.at[slot, kind], send_sem=self.sems[0].at[2 * kind + sem], recv_sem=self.sems[1].at[2 * kind + slot], device_id=device, device_id_type=MESH)

    def near(self, kind):
        return self.copy(kind, 1 - self.tp, 0, (1 - self.tp, self.cp), 0)

    def far(self, kind, batch):
        return self.copy(kind, batch, 1, (batch, self.mirror), batch)

    def start(self, kind):
        @pl.when(self.is_mine)
        def _():
            self.near(kind).start()
            self.dst[0, kind] = self.src[kind][self.tp]

        @pl.when(jnp.logical_not(self.is_mine))
        def _():
            self.far(kind, 0).start()
            self.far(kind, 1).start()

    def wait(self, kind):
        self.far(kind, 0).wait_recv()

        @pl.when(jnp.logical_not(self.is_mine))
        def _():
            self.near(kind).wait_recv()

    def drain(self, kind):
        @pl.when(self.is_mine)
        def _():
            self.near(kind).wait_send()

        @pl.when(jnp.logical_not(self.is_mine))
        def _():
            self.far(kind, 0).wait_send()
            self.far(kind, 1).wait_send()


D_TILE = 256


def attn_kernel(k_ref, v_ref, q_ref, hid_ref, grad_ref, wo_ref, cos_ref, sin_ref, dqh_ref, out_ref, sl0, sl1, sl2, red0, red1, red2, ho0, ho1, ho2, y0, y1, y2, kv_scr, qd_scr, o_scr, qt_scr, dot_scr, dqt_scr, m_scr, l_scr, delta_scr, p_scr, ds_scr, dkv_scr, tok_scr, part_scr, got_scr, out_scr, rot_scr, oh_scr, dqh_scr, do_home, *rest):
    rest = list(rest)

    def grab(n):
        return [rest.pop(0) for _ in range(n)]

    hr, gr, orr, xs = (grab(3) for _ in range(4))
    k_sems, d_sems, h_sems, g_sems, or_sems = ([grab(2) for _ in COLOURS] for _ in range(5))
    hand_sems, oh_sems, dqh_sems, swap_sems = (grab(2) for _ in range(4))
    n_groups, _, n_cols, e_dim = qd_scr.shape
    rows = k_ref.shape[0]
    per_tile = TILE // BLK
    n_blk = RING ** 3
    d_model = grad_ref.shape[1]
    cp = lax.axis_index("cp")
    mirror = n_blk - 1 - cp
    rings = [ring_of(axis) for axis in COLOURS]
    o_lanes = wide_lanes(d_model)
    ys = (y0, y1, y2)
    split = by_rows(rows, 16)
    p_kv = [Part(rings, ORDERS[c], split[c][1], k_sems[c], y=ys[c], lanes=(0, 2 * e_dim), align=16, direct=1) for c in COLOURS]
    rows_d = by_rows(rows, 8)
    p_d = [Part(rings, ORDERS[c], rows_d[c][1], d_sems[c], x=xs[c], recv=grab(1), lanes=(0, 2 * e_dim)) for c in COLOURS]
    h_out, = rest
    hand = Handout((q_ref, do_home), qd_scr, hand_sems)
    o_back = Return(o_scr, oh_scr, oh_sems)
    dq_back = Return(rot_scr, dqh_scr, dqh_sems)

    for c in COLOURS:
        own = pl.ds(pl.multiple_of(p_kv[c].own_rows(), 16), split[c][1])
        ys[c][own, :e_dim] = k_ref[pl.ds(*split[c]), :]
        ys[c][own, e_dim:] = v_ref[pl.ds(*split[c]), :]
    enter(rings, with_partner=True, with_mirror=True)
    stage(p_kv, "ag_start2")
    stage(p_kv, "ag_end2")
    stage(p_kv, "ag_start1")
    hand.start(0)
    stage(p_kv, "ag_end1")
    stage(p_kv, "ag_start0")
    for cols in range(0, n_cols, COLS):
        res = lax.dot_general(grad_ref[...], wo_ref[pl.ds(cols, COLS), :], (((1,), (1,)), ((), ())), preferred_element_type=F32).astype(BF16)
        for b in range(n_groups):
            for h in range(COLS // e_dim):
                do_home[b, pl.ds(cols + h * rows, rows), :] = res[b * rows:(b + 1) * rows, h * e_dim:(h + 1) * e_dim]
    dqt_scr[...] = jnp.zeros_like(dqt_scr)
    dkv_scr[...] = jnp.zeros_like(dkv_scr)
    m_scr[...] = jnp.full_like(m_scr, -jnp.inf)
    l_scr[...] = jnp.zeros_like(l_scr)
    hand.wait(0)
    for grp in range(n_groups):
        qt_scr[grp] = qd_scr[grp, 0].T
    stage(p_kv, "ag_mid0")
    hand.start(1)
    stage(p_kv, "ag_end0")

    def place_kv(blk, carry):
        for c in COLOURS:
            at, rb = split[c]
            src = pl.ds(pl.multiple_of(place_in_order(blk, ORDERS[c]) * rb, 16), rb)
            kv_scr[pl.ds(pl.multiple_of(blk * rows + at, 16), rb), :] = ys[c][src, :]
        return carry

    h_slab = d_model // RING
    n_tok = hid_ref.shape[0]

    def hid_cols(pos):
        return hid_ref.at[:, pl.ds(pl.multiple_of(pos * h_slab, h_slab), h_slab)]

    def grad_cols(c):
        return grad_ref.at[:, pl.ds(*o_lanes[c])]

    h_sent, g_sent = [], []
    for c in COLOURS:
        ring = rings[ORDERS[c][0]]
        here = pl.ds(pl.multiple_of(ring[0] * n_tok, n_tok), n_tok)
        h_sent += spread(ring, hid_cols, hr[c], n_tok, h_sems[c])
        g_sent += spread(ring, lambda pos, c=c: grad_cols(c), gr[c], n_tok, g_sems[c])
        hr[c][here, :] = hid_cols(ring[0])[...]
        gr[c][here, :] = grad_cols(c)[...]
    for copy in g_sent:
        copy.start()
    for copy in h_sent:
        copy.start()
    lax.fori_loop(0, n_blk, place_kv, 0)

    n_first = cp // per_tile + 1
    n_steps = n_blk // per_tile + 1

    def over_tiles(tile_step, extra):
        def body(t, carry):
            grp = (t - n_first + n_steps) // n_steps
            piece = cp + grp * (mirror - cp)
            tile_idx = t - grp * n_first
            last = tile_idx == piece // per_tile

            @pl.when(jnp.logical_not(last))
            def _():
                tile_step(grp, tile_idx, piece, False)

            @pl.when(last)
            def _():
                tile_step(grp, tile_idx, piece, True)

            for when, action in extra:
                pl.when(t == when)(action)
            return carry

        lax.fori_loop(0, n_steps, body, 0)

    def fwd_step(grp, tile_idx, piece, masked):
        row0 = pl.multiple_of(tile_idx * TILE, TILE)
        k_t = kv_scr[pl.ds(row0, TILE), :e_dim]
        v_t = kv_scr[pl.ds(row0, TILE), e_dim:]
        for c0 in range(0, n_cols, COLS):
            cs = slice(c0, c0 + COLS)
            s = dot(k_t, qt_scr[grp, :, cs])
            if masked:
                s = jnp.where(causal_mask(row0, piece * BLK, COLS), s, -jnp.inf)
            m_old = m_scr[grp, :, cs]
            m_new = jnp.maximum(m_old, jnp.max(s, axis=0, keepdims=True))
            p = jnp.exp(s - m_new)
            alpha = jnp.exp(m_old - m_new)
            m_scr[grp, :, cs] = m_new
            l_scr[grp, :, cs] = l_scr[grp, :, cs] * alpha + jnp.sum(p, axis=0, keepdims=True)
            dqt_scr[grp, :, cs] = dqt_scr[grp, :, cs] * alpha + dot_ta(v_t, p.astype(BF16))

    over_tiles(fwd_step, ())
    hand.wait(1)
    for grp in range(n_groups):
        o_t = (dqt_scr[grp] / l_scr[grp]).astype(BF16)
        o_scr[grp] = o_t.T
        dot_scr[grp] = qd_scr[grp, 1].T
        delta_scr[grp] = jnp.sum(dot_scr[grp].astype(F32) * o_t.astype(F32), axis=0, keepdims=True)
    o_back.start()
    m_scr[...] = m_scr[...] + jnp.log(l_scr[...])
    dqt_scr[...] = jnp.zeros_like(dqt_scr)

    def bwd_step(grp, tile_idx, piece, masked):
        row0 = pl.multiple_of(tile_idx * TILE, TILE)
        k_t = kv_scr[pl.ds(row0, TILE), :e_dim]
        v_t = kv_scr[pl.ds(row0, TILE), e_dim:]
        for c0 in range(0, n_cols, COLS):
            cs = slice(c0, c0 + COLS)
            s = dot(k_t, qt_scr[grp, :, cs])
            p = jnp.exp(s - m_scr[grp, :, cs])
            if masked:
                p = jnp.where(causal_mask(row0, piece * BLK, COLS), p, 0.0)
            d_p = dot(v_t, dot_scr[grp, :, cs])
            p_scr[:, cs] = p.astype(BF16)
            ds_scr[:, cs] = (p * (d_p - delta_scr[grp, :, cs])).astype(BF16)
        at = pl.ds(row0, TILE)
        dkv_scr[at, :e_dim] += dot(ds_scr[...], qd_scr[grp, 0])
        dkv_scr[at, e_dim:] += dot(p_scr[...], qd_scr[grp, 1])
        dqt_scr[grp] += dot_ta(k_t, ds_scr[...])

    o_slab = n_cols // RING

    def o_cols(pos):
        return tok_scr.at[:, pl.ds(pl.multiple_of(pos * o_slab, o_slab), o_slab)]

    def o_spread():
        return [copy for c in COLOURS for copy in spread(rings[ORDERS[c][0]], o_cols, orr[c], n_tok, or_sems[c])]

    def send_o():
        o_back.wait()
        place_heads(tok_scr, oh_scr)
        for c in COLOURS:
            pos = rings[ORDERS[c][0]][0]
            orr[c][pl.ds(pl.multiple_of(pos * n_tok, n_tok), n_tok), :] = o_cols(pos)[...]
        for copy in o_spread():
            copy.start()

    def slab_wo():
        for copy in o_spread() + g_sent:
            copy.wait_recv()
        for c, red in enumerate((red0, red1, red2)):
            for at in range(0, red.shape[1], 128):
                red[:, at:at + 128] = dot_ta(orr[c][...], gr[c][:, at:at + 128])

    over_tiles(bwd_step, ((3, send_o), (8, slab_wo)))

    def place_dkv(blk, carry):
        for c in COLOURS:
            at, rb = rows_d[c]
            dst = pl.ds(pl.multiple_of(place_in_order(blk, ORDERS[c]) * rb, 8), rb)
            xs[c][dst, :] = dkv_scr[pl.ds(pl.multiple_of(blk * rows + at, 8), rb), :]
        return carry

    lax.fori_loop(0, n_blk, place_dkv, 0)
    stage(p_d, "rs_start0")

    scale = e_dim ** -0.5
    half_dim = e_dim // 2
    for grp in range(n_groups):
        cos_t, sin_t = cos_ref[grp], sin_ref[grp]
        for h in range(n_cols // rows):
            cols = slice(h * rows, (h + 1) * rows)
            low, high = dqt_scr[grp, :half_dim, cols], dqt_scr[grp, half_dim:, cols]
            turned = jnp.concatenate([low * cos_t + high * sin_t, high * cos_t - low * sin_t], axis=0) * scale
            rot_scr[grp, cols, :] = turned.T.astype(BF16)
    dq_back.start()
    for copy in h_sent:
        copy.wait_recv()
    h_outs = [pltpu.make_async_copy(hr[c], out, h_out.at[c]) for c, out in enumerate((ho0, ho1, ho2))]
    for copy in h_outs:
        copy.start()

    tp = lax.axis_index("tp")
    partner = (1 - tp, cp)
    for at in range(0, d_model, D_TILE):
        cols = slice(at, at + D_TILE)
        res = dot(tok_scr[...], wo_ref[:, cols])
        for b in range(n_groups):
            part_scr[b, :, cols] = res[b * rows:(b + 1) * rows]

    def swap(src, dst, i):
        return pltpu.make_async_remote_copy(src_ref=src, dst_ref=dst, send_sem=swap_sems[0].at[i], recv_sem=swap_sems[1].at[i], device_id=partner, device_id_type=MESH)

    swap_part = swap(part_scr.at[1 - tp], got_scr, 0)
    swap_part.start()
    stage(p_d, "rs_mid0")
    swap_part.wait()
    out_scr[tp] = (part_scr[tp] + got_scr[...]).astype(BF16)
    swap_out = swap(out_scr.at[tp], out_scr.at[tp], 1)
    swap_out.start()
    dq_back.wait()

    def put(src, dst):
        copy = pltpu.make_async_copy(src, dst, h_out.at[len(h_outs)])
        copy.start()
        h_outs.append(copy)

    put(dqh_scr, dqh_ref)
    swap_out.wait()
    put(out_scr, out_ref)
    stage(p_d, "rs_end0")
    for part, out in zip(p_d, (sl0, sl1, sl2)):
        slab, _, _, starts, *_ = part.place(0)
        put(part.view(part.x, starts[0], slab), out)
    for part in p_kv:
        part.drain(ag=COLOURS)
    for part in p_d:
        part.drain(rs=(0,))
    for kind in range(2):
        hand.drain(kind)
    for copy in h_sent + g_sent + o_spread():
        copy.wait_send()
    for copy in h_outs:
        copy.wait()
    o_back.drain()
    dq_back.drain()


def attention(key_loc, val_loc, q_home, hid, grad, w_out, cos_t, sin_t):
    n_batch, n_cols, e_dim = q_home.shape
    rows = key_loc.shape[0]
    n_tok, d_model = grad.shape
    n_blk = RING ** 3
    seq = n_blk * rows
    o_lanes = wide_lanes(d_model)
    slab = n_cols // RING
    vmem, anyspace = pl.BlockSpec(memory_space=pltpu.VMEM), pl.BlockSpec(memory_space=pl.ANY)
    heads = (2, n_cols, e_dim)
    h_ring = (RING * n_tok, d_model // RING)
    work = n_cols * seq
    return pl.pallas_call(
        attn_kernel,
        out_shape=(jax.ShapeDtypeStruct(heads, BF16), jax.ShapeDtypeStruct((2, rows, d_model), BF16)) + tuple(jax.ShapeDtypeStruct((n_blk // RING * rb, 2 * e_dim), F32) for _, rb in by_rows(rows, 8)) + tuple(jax.ShapeDtypeStruct((slab, n), F32) for _, n in o_lanes) + (jax.ShapeDtypeStruct(h_ring, BF16),) * 3,
        in_specs=[vmem] * 8,
        out_specs=(anyspace,) * 5 + (vmem,) * 3 + (anyspace,) * 3,
        scratch_shapes=[pltpu.VMEM((n_blk * rb, 2 * e_dim), BF16) for _, rb in by_rows(rows, 16)]
        + [
            pltpu.VMEM((seq, 2 * e_dim), BF16),
            pltpu.VMEM((2, 2, n_cols, e_dim), BF16),
            pltpu.VMEM(heads, BF16),
            pltpu.VMEM((2, e_dim, n_cols), BF16),
            pltpu.VMEM((2, e_dim, n_cols), BF16),
            pltpu.VMEM((2, e_dim, n_cols), F32),
            pltpu.VMEM((2, 1, n_cols), F32),
            pltpu.VMEM((2, 1, n_cols), F32),
            pltpu.VMEM((2, 1, n_cols), F32),
            pltpu.VMEM((TILE, n_cols), BF16),
            pltpu.VMEM((TILE, n_cols), BF16),
            pltpu.VMEM((seq, 2 * e_dim), F32),
            pltpu.VMEM((n_tok, n_cols), BF16),
            pltpu.VMEM((2, rows, d_model), F32),
            pltpu.VMEM((rows, d_model), F32),
            pltpu.VMEM((2, rows, d_model), BF16),
        ]
        + [pltpu.VMEM(heads, BF16)] * 4
        + [pltpu.VMEM(h_ring, BF16)] * 3
        + [pltpu.VMEM((RING * n_tok, lanes), BF16) for _, lanes in o_lanes]
        + [pltpu.VMEM((RING * n_tok, slab), BF16)] * 3
        + [pltpu.VMEM((n_blk * rb, 2 * e_dim), F32) for _, rb in by_rows(rows, 8)]
        + pair(30) * 6
        + pair(3) * 9
        + pair(4)
        + pair(2) * 3
        + [pltpu.VMEM((slab_rows(rb)[0], 2 * e_dim), F32) for _, rb in by_rows(rows, 8)]
        + [pltpu.SemaphoreType.DMA((8,))],
        compiler_params=pltpu.CompilerParams(collective_id=2, has_side_effects=True, vmem_limit_bytes=VMEM_LIMIT),
        cost_estimate=pl.CostEstimate(flops=14 * work * e_dim, bytes_accessed=seq * e_dim * 12, transcendentals=2 * work),
        name="attention",
    )(key_loc, val_loc, q_home, hid, grad, w_out, cos_t, sin_t)


GRAD_PLAN = (
    "r.rs_start1", "d.rs_start1", "weights.q", "s.rs_start1", "d.rs_mid1", "r.rs_mid1", "s.rs_mid1", "d.rs_end1",
    "d.rs_start2", "r.rs_end1", "r.rs_start2", "s.rs_end1", "s.rs_start2", "d.rs_end2", "weights.prep", "weights.kv",
    "r.rs_end2", "s.rs_end2", "o.ag_start2", "q.ag_start2", "weights.slab", "t.rs_start1", "o.ag_end2",
    "o.ag_start1", "t.rs_mid1", "q.ag_end2", "q.ag_start1", "t.rs_end1", "t.rs_start2", "o.ag_mid1", "q.ag_mid1",
    "t.rs_end2", "k.ag_start2", "o.ag_end1", "o.ag_start0", "k.ag_end2", "k.ag_start1", "q.ag_end1", "q.ag_start0",
    "k.ag_mid1", "o.ag_mid0", "k.ag_end1", "k.ag_start0", "q.ag_mid0", "k.ag_mid0", "k.ag_end0", "o.ag_end0",
    "q.ag_end0",
)


def grad_kernel(sl0, sl1, sl2, dqh_ref, red0, red1, red2, hi0, hi1, hi2, cos_ref, sin_ref, gq_ref, go_ref, gk_ref, gv_ref, dkd_ref, yq, yo, yk, yp, turn_scr, tok_scr, kvt_scr, kvr_scr, mine_scr, give_scr, got_scr, xk, *rest):
    rest = list(rest)

    def grab(n):
        return [rest.pop(0) for _ in range(n)]

    n_blk = RING ** 3
    n_batch, _, head_dim = dqh_ref.shape
    n_tok, n_cols = tok_scr.shape
    d_model = yq.shape[0]
    rows, lanes = n_tok // n_batch, 2 * head_dim
    n_local = n_cols // head_dim
    q_lanes, o_lanes = thirds(n_local, head_dim), wide_lanes(d_model)
    split = by_rows(rows, 8)
    tp, cp = lax.axis_index("tp"), lax.axis_index("cp")
    partner = (1 - tp, cp)
    rings = [ring_of(axis) for axis in COLOURS]

    def shifted(c, n_rows):
        return 0 - rings[ORDERS[c][0]][0] * (n_rows // RING)

    xs, xos, xqs, hr, dqr = (grab(3) for _ in range(5))
    sem_d, sem_q, sem_o, sem_g = ([grab(2) for _ in COLOURS] for _ in range(4))
    sem_k, sem_kr = grab(2), grab(2)
    p_d = [Part(rings, ORDERS[c], split[c][1], sem_d[c], x=xs[c], recv=[None] + grab(2), row0=shifted(c, n_blk * split[c][1]), lanes=(0, lanes)) for c in COLOURS]
    p_s = [Part(rings, ORDERS[c], d_model // n_blk, sem_q[c], x=xqs[c], recv=[None] + grab(2), row0=shifted(c, d_model), lanes=(0, q_lanes[c][1])) for c in COLOURS]
    p_q = [Part(rings, ORDERS[c], d_model // n_blk, sem_q[c], y=yq, lanes=q_lanes[c]) for c in COLOURS]
    p_r = [Part(rings, ORDERS[c], n_cols // n_blk, sem_o[c], x=xos[c], recv=[None] + grab(2), row0=shifted(c, n_cols), lanes=(0, o_lanes[c][1])) for c in COLOURS]
    p_o = [Part(rings, ORDERS[c], n_cols // n_blk, sem_o[c], y=yo, lanes=o_lanes[c]) for c in COLOURS]
    p_t = [Part(rings, ORDERS[2], d_model // n_blk, sem_k, x=xk, recv=[None] + grab(2), row0=shifted(2, d_model), lanes=(0, head_dim))]
    p_k = [Part(rings, ORDERS[2], d_model // n_blk, sem_k, y=yk, lanes=(0, head_dim))]
    in_sem, out_sem, swap_s, swap_r = rest

    loads = [pltpu.make_async_copy(src, dst, in_sem.at[i]) for i, (src, dst) in enumerate(zip((sl0, sl1, sl2, red0, red1, red2, hi0, hi1, hi2), xs + xos + hr))]
    for copy in loads:
        copy.start()
    place_heads(tok_scr, dqh_ref)

    def tok_cols(c):
        return pl.ds(*q_lanes[c])

    dq_sent = []
    for c in COLOURS:
        ring = rings[ORDERS[c][0]]
        dqr[c][pl.ds(pl.multiple_of(ring[0] * n_tok, n_tok), n_tok), :] = tok_scr[:, tok_cols(c)]
        dq_sent += spread(ring, lambda pos, c=c: tok_scr.at[:, tok_cols(c)], dqr[c], n_tok, sem_g[c])
    ring_k = rings[ORDERS[2][0]]
    kv_sent = spread(ring_k, lambda pos: kvt_scr, kvr_scr, n_tok, sem_kr)
    enter(rings, with_partner=True)
    for copy in dq_sent:
        copy.start()
    for copy in loads:
        copy.wait()
    half_dim = head_dim // 2
    first = tp == 0
    swap_small = pltpu.make_async_remote_copy(src_ref=give_scr, dst_ref=got_scr, send_sem=swap_s.at[0], recv_sem=swap_r.at[0], device_id=partner, device_id_type=MESH)
    swap = pltpu.make_async_remote_copy(src_ref=yk, dst_ref=yp, send_sem=swap_s.at[1], recv_sem=swap_r.at[1], device_id=partner, device_id_type=MESH)

    def put_o(which):
        for c, part in enumerate(p_o):
            slab, _, _, starts, *_ = part.place(0)
            for i in which:
                pltpu.make_async_copy(part.view(yo, starts[i], slab), part.view(go_ref, starts[i], slab), out_sem.at[c]).start()

    def turn_q(which):
        for c, part in enumerate(p_q):
            slab, _, _, starts, *_ = part.place(0)
            for i in which:
                at = pl.multiple_of(starts[i], slab)
                for h in range(q_lanes[c][0] // head_dim, sum(q_lanes[c]) // head_dim):
                    turn_scr[pl.ds(at * n_local + h, slab, stride=n_local), :] = yq[pl.ds(at, slab), pl.ds(h * head_dim, head_dim)]

    def own_block(parts, sums):
        for part, total in zip(parts, sums):
            at, lanes_y, lanes_x = part.own_rows(), pl.ds(*part.lanes), pl.ds(*total.lanes)
            part.y[pl.ds(pl.multiple_of(at, 8), part.rb), lanes_y] = total.x[pl.ds(pl.multiple_of(total.own_rows(), 8), part.rb), lanes_x]

    def slab_term(dst, hid, other):
        for at in range(0, dst.shape[0], D_TILE):
            dst[pl.ds(at, D_TILE), :] = dot_ta(hid[:, at:at + D_TILE], other[...])

    def weights_q():
        for copy in dq_sent:
            copy.wait_recv()
        for c in COLOURS:
            slab_term(xqs[c], hr[c], dqr[c])

    def new_dkv():
        dkd_ref[...] = mine_scr[...].astype(BF16)
        return dkd_ref[:, :head_dim], dkd_ref[:, head_dim:]

    def weights_prep():
        for c in COLOURS:
            at, rb = split[c]
            own = xs[c][pl.ds(pl.multiple_of(p_d[c].own_rows(), 8), rb), :]
            cos_tab, sin_tab = cos_ref[pl.ds(at, rb), :], sin_ref[pl.ds(at, rb), :]
            low, high = own[:, :half_dim], own[:, half_dim:head_dim]
            mine_scr[pl.ds(at, rb), :head_dim] = jnp.concatenate([low * cos_tab + high * sin_tab, high * cos_tab - low * sin_tab], axis=1)
            mine_scr[pl.ds(at, rb), head_dim:] = own[:, head_dim:]
        dk_new, dv_new = new_dkv()
        give_scr[...] = jnp.where(first, dv_new, dk_new)
        swap_small.start()

    def weights_kv():
        swap_small.wait()
        got = got_scr[...]
        keep = jnp.where(first, dkd_ref[:, :head_dim], dkd_ref[:, head_dim:])
        kvt_scr[...] = jnp.concatenate([jnp.where(first, keep, got), jnp.where(first, got, keep)], axis=0)
        kvr_scr[pl.ds(pl.multiple_of(ring_k[0] * n_tok, n_tok), n_tok), :] = kvt_scr[...]
        for copy in kv_sent:
            copy.start()

    def weights_slab():
        for copy in kv_sent:
            copy.wait_recv()
        slab_term(xk, hr[2], kvr_scr)

    groups = {"d": p_d, "s": p_s, "q": p_q, "r": p_r, "o": p_o, "t": p_t, "k": p_k}
    after = {
        "weights.q": weights_q,
        "weights.prep": weights_prep,
        "weights.kv": weights_kv,
        "weights.slab": weights_slab,
        "r.rs_end2": lambda: own_block(p_o, p_r),
        "s.rs_end2": lambda: own_block(p_q, p_s),
        "t.rs_end2": lambda: own_block(p_k, p_t),
        "o.ag_mid0": lambda: put_o((0, 1, 3)),
        "o.ag_end0": lambda: put_o((2,)),
        "q.ag_start0": lambda: turn_q((0,)),
        "q.ag_mid0": lambda: turn_q((1, 3)),
        "q.ag_end0": lambda: turn_q((2,)),
        "k.ag_end0": swap.start,
    }
    for step in GRAD_PLAN:
        who, what = step.split(".")
        if who in groups:
            stage(groups[who], what)
        if step in after:
            after[step]()
    out_q = pltpu.make_async_copy(turn_scr, gq_ref, out_sem.at[3])
    out_q.start()
    swap.wait()

    def put_kv(k_src, v_src):
        outs = [pltpu.make_async_copy(k_src, gk_ref, out_sem.at[4]), pltpu.make_async_copy(v_src, gv_ref, out_sem.at[5])]
        for copy in outs:
            copy.start()
        for copy in outs:
            copy.wait()

    @pl.when(first)
    def _():
        put_kv(yk, yp)

    @pl.when(jnp.logical_not(first))
    def _():
        put_kv(yp, yk)

    out_q.wait()
    for c, part in enumerate(p_o):
        pltpu.make_async_copy(part.view(yo, 0, n_cols), part.view(go_ref, 0, n_cols), out_sem.at[c]).wait()
    for part in p_d + p_s + p_r + p_t:
        part.drain(rs=(1, 2))
    for part in p_q + p_o + p_k:
        part.drain(ag=COLOURS)
    for copy in dq_sent + kv_sent:
        copy.wait_send()


def grad_sums(slabs, dq_home, reds, h_rings, cos_tab, sin_tab, d_model):
    n_batch, n_rows, head_dim = dq_home.shape
    rows = cos_tab.shape[0]
    n_tok, n_cols = n_batch * rows, n_rows // rows * head_dim
    n_blk = RING ** 3
    lanes = 2 * head_dim
    q_lanes, o_lanes = thirds(n_cols // head_dim, head_dim), wide_lanes(d_model)
    split = by_rows(rows, 8)
    vmem, anyspace = pl.BlockSpec(memory_space=pltpu.VMEM), pl.BlockSpec(memory_space=pl.ANY)

    def full(*shape):
        return pltpu.VMEM(shape, F32)

    def half(*shape):
        return pltpu.VMEM(shape, BF16)

    def later(rb, width):
        return [full(n, width) for n in slab_rows(rb)[1:]]

    slab, ring_tok = d_model // RING, RING * n_tok
    scratch = [full(d_model, n_cols), full(n_cols, d_model), full(d_model, head_dim), full(d_model, head_dim), full(d_model * n_cols // head_dim, head_dim)]
    scratch += [half(n_tok, n_cols), half(n_tok, head_dim), half(ring_tok, head_dim), full(rows, lanes), half(rows, head_dim), half(rows, head_dim), full(slab, head_dim)]
    scratch += [full(n_blk // RING * rb, lanes) for _, rb in split]
    scratch += [full(n_cols // RING, w) for _, w in o_lanes] + [full(slab, w) for _, w in q_lanes]
    scratch += [half(ring_tok, slab)] * 3 + [half(ring_tok, w) for _, w in q_lanes]
    scratch += pair(30) * 9 + pair(3) * 3 + pair(30) + pair(3)
    for _, rb in split:
        scratch += later(rb, lanes)
    for _, w in q_lanes:
        scratch += later(d_model // n_blk, w)
    for _, w in o_lanes:
        scratch += later(n_cols // n_blk, w)
    scratch += later(d_model // n_blk, head_dim)
    scratch += [pltpu.SemaphoreType.DMA((9,)), pltpu.SemaphoreType.DMA((6,))] + pair(2)
    return pl.pallas_call(
        grad_kernel,
        out_shape=(
            jax.ShapeDtypeStruct((d_model * n_cols // head_dim, head_dim), F32),
            jax.ShapeDtypeStruct((n_cols, d_model), F32),
            jax.ShapeDtypeStruct((d_model, head_dim), F32),
            jax.ShapeDtypeStruct((d_model, head_dim), F32),
            jax.ShapeDtypeStruct((rows, lanes), BF16),
        ),
        in_specs=[anyspace] * 3 + [vmem] + [anyspace] * 6 + [vmem] * 2,
        out_specs=(anyspace,) * 4 + (vmem,),
        scratch_shapes=scratch,
        compiler_params=pltpu.CompilerParams(collective_id=3, has_side_effects=True, vmem_limit_bytes=VMEM_LIMIT),
        cost_estimate=pl.CostEstimate(flops=n_tok * d_model * n_cols * 160, bytes_accessed=40 << 20, transcendentals=0),
        name="grad_sums",
    )(*slabs, dq_home, *reds, *h_rings, cos_tab, sin_tab)


def solution(mesh):
    cp_size = mesh.shape["cp"]
    partner = [(0, 1), (1, 0)]

    def local_program(hidden, grad_out, w_query, w_key, w_value, w_out):
        block_len = hidden.shape[1]
        n_local = w_query.shape[1]
        head_dim = w_key.shape[1]
        q_scale = head_dim ** -0.5
        cp_idx = lax.axis_index("cp")
        tp_idx = lax.axis_index("tp")
        mirror_idx = cp_size - 1 - cp_idx
        cos_tab, sin_tab = rope_tables(cp_idx * block_len + jnp.arange(block_len), head_dim)
        cos_mir, sin_mir = rope_tables(mirror_idx * block_len + jnp.arange(block_len), head_dim)

        def pick(pair, idx):
            return lax.dynamic_index_in_dim(pair, idx, 0, keepdims=False)

        def sum_over_tp(part, extra=None):
            total = pick(part, tp_idx) + lax.ppermute(pick(part, 1 - tp_idx), "tp", partner)
            if extra is not None:
                total = total + extra
            mine = total.astype(BF16)
            other = lax.ppermute(mine, "tp", partner)
            first = tp_idx == 0
            return jnp.stack([jnp.where(first, mine, other), jnp.where(first, other, mine)])

        hid_b = pick(hidden, tp_idx)
        key_loc = rotate(dot(hid_b, w_key), cos_tab, sin_tab).astype(BF16)
        val_loc = dot(hid_b, w_value).astype(BF16)
        q_pre = jnp.einsum("bsd,dhe->bhse", hidden, w_query, preferred_element_type=F32)
        queries = (rotate(q_pre, cos_tab, sin_tab) * q_scale).astype(BF16)
        q_home = queries.reshape(2, n_local * block_len, head_dim)
        d_model = hidden.shape[-1]
        hid, grad = hidden.reshape(-1, d_model), grad_out.reshape(-1, d_model)
        tabs_t = [jnp.stack(pair_t) for pair_t in ((cos_tab.T, cos_mir.T), (sin_tab.T, sin_mir.T))]
        dq_home, attn_out, *more = attention(key_loc, val_loc, q_home, hid, grad, w_out.reshape(-1, d_model), *tabs_t)
        dq_pre = dq_home.reshape(2, n_local, block_len, head_dim)
        grad_q, grad_o, d_w_key, d_w_value, dkv_new = grad_sums(more[:3], dq_home, more[3:6], more[6:], cos_tab, sin_tab, d_model)
        d_w_query = grad_q.reshape(w_query.shape)
        d_w_out = grad_o.reshape(w_out.shape)
        dk_pre, dv_pre = dkv_new[:, :head_dim], dkv_new[:, head_dim:]
        dh_kv = dot(dk_pre, w_key.T) + dot(dv_pre, w_value.T)
        d_hidden = sum_over_tp(jnp.einsum("cirf,eif->cre", dq_pre, w_query, preferred_element_type=F32), dh_kv)
        return attn_out, d_hidden, d_w_query, d_w_key, d_w_value, d_w_out

    row_spec = P(None, "cp", None)
    return jax.shard_map(local_program, mesh=mesh, in_specs=(row_spec, row_spec, P(None, "tp", None), P(), P(), P("tp", None, None)), out_specs=(row_spec, row_spec, P(None, "tp", None), P(), P(), P("tp", None, None)), check_vma=False)
```

```python
import jax
import jax.numpy as jnp
from jax import lax
from jax.experimental import pallas as pl
from jax.experimental.pallas import tpu as pltpu
from jax.sharding import PartitionSpec as P

ROPE_BASE = 10000.0
BLK = 128
TILE = 512
COLOURS = range(3)
VMEM_LIMIT = 67000000
COLS = 256
F32 = jnp.float32
BF16 = jnp.bfloat16


def rope_tables(positions, head_dim):
    half_dim = head_dim // 2
    inv_freq = 1.0 / jnp.power(ROPE_BASE, jnp.arange(half_dim, dtype=F32) * (2.0 / head_dim))
    angles = positions.astype(F32)[:, None] * inv_freq[None, :]
    return jnp.cos(angles), jnp.sin(angles)


def rotate(rot_in, cos_tab, sin_tab):
    half_dim = rot_in.shape[-1] // 2
    low_half = rot_in[..., :half_dim]
    high_half = rot_in[..., half_dim:]
    return jnp.concatenate([low_half * cos_tab - high_half * sin_tab, high_half * cos_tab + low_half * sin_tab], axis=-1)


def unrotate(rot_in, cos_tab, sin_tab):
    return rotate(rot_in, cos_tab, -sin_tab)


def dot(a, b):
    return jnp.dot(a, b, preferred_element_type=F32)


def dot_ta(a, b):
    return lax.dot_general(a, b, (((0,), (0,)), ((), ())), preferred_element_type=F32)


def causal_mask(k_start, q_start, cols):
    k_pos = k_start + lax.broadcasted_iota(jnp.int32, (TILE, cols), 0)
    q_pos = q_start + lax.broadcasted_iota(jnp.int32, (TILE, cols), 1) % BLK
    return k_pos <= q_pos


RING = 4
AXIS_STRIDE = (RING * RING, RING, 1)
ORDERS = ((0, 1, 2), (1, 2, 0), (2, 0, 1))
MESH = pl.DeviceIdType.MESH
HOPS = 12


def ring_of(axis):
    cp, tp = lax.axis_index("cp"), lax.axis_index("tp")
    stride = AXIS_STRIDE[axis]
    pos = (cp // stride) % RING
    right = cp + ((pos + 1) % RING - pos) * stride
    left = cp + ((pos + RING - 1) % RING - pos) * stride
    across = cp + ((pos + 2) % RING - pos) * stride
    return pos, (tp, right), (tp, left), (tp, across)


def enter(rings, with_partner=False, with_mirror=False):
    barrier = pltpu.get_barrier_semaphore()
    peers = []
    for _, *others in rings:
        peers += others
    if with_partner:
        peers.append((1 - lax.axis_index("tp"), lax.axis_index("cp")))
    if with_mirror:
        mirror = RING ** 3 - 1 - lax.axis_index("cp")
        peers += [(0, mirror), (1, mirror)]
    for peer in peers:
        pl.semaphore_signal(barrier, inc=1, device_id=peer, device_id_type=MESH)
    pl.semaphore_wait(barrier, len(peers))


def remote(src, dst, sems, idx, device):
    return pltpu.make_async_remote_copy(src_ref=src, dst_ref=dst, send_sem=sems[0].at[idx], recv_sem=sems[1].at[idx], device_id=device, device_id_type=MESH)


def add_rows(dst, dst0, srcs, n_rows, lanes):
    strip = next(s for s in (64, 48, 40, 32, 24, 16, 8) if n_rows % s == 0)
    if lanes[1] > 256:
        strip = next(s for s in (16, 8) if n_rows % s == 0)

    def body(i, carry):
        off = pl.multiple_of(dst0 + i * strip, 8)
        total = dst[pl.ds(off, strip), pl.ds(*lanes)]
        for ref, start in srcs:
            total = total + ref[pl.ds(pl.multiple_of(start + i * strip, 8), strip), :]
        dst[pl.ds(off, strip), pl.ds(*lanes)] = total
        return carry

    lax.fori_loop(0, n_rows // strip, body, 0)


class Part:
    def __init__(self, rings, order, rb, sems, x=None, y=None, recv=None, row0=0, lanes=None, align=8, direct=2):
        self.direct = direct
        self.rb, self.sems, self.x, self.y, self.recv = rb, sems, x, y, recv
        self.row0, self.lanes, self.align = row0, lanes, align
        self.places = []
        base = row0
        for phase in COLOURS:
            slab = rb * RING ** (2 - phase)
            h0 = -(-slab // (2 * align)) * align
            pos, right, left, across = rings[order[phase]]
            starts = [base + ((pos + d) % RING) * slab for d in range(RING)]
            self.places.append((slab, h0, slab - h0, starts, right, left, across))
            base = starts[0]

    def view(self, ref, start, n_rows):
        return ref.at[pl.ds(pl.multiple_of(start, self.align), n_rows), pl.ds(*self.lanes)]

    def place(self, phase):
        return self.places[phase]

    def hop(self, phase, i):
        slab, h0, h1, (own, rgt, opp, lft), right, left, across = self.place(phase)
        if phase >= self.direct:
            start, n_rows, at, device = {
                0: (opp, slab, 0, across),
                2: (rgt, slab, slab, right),
                3: (lft, slab, 2 * slab, left),
                6: (own, slab, 0, right),
                7: (own, slab, 0, left),
                8: (own, slab, 0, across),
            }[i]
        else:
            start, n_rows, at, device = (
                (opp, h0, 0, right),
                (opp + h0, h1, h0, left),
                (rgt + h0, h1, slab + h0, right),
                (lft, h0, 2 * slab, left),
                (rgt, h0, slab, right),
                (lft + h0, h1, 2 * slab + h0, left),
                (own, h0, 0, right),
                (own + h0, h1, 0, left),
                (lft, h0, 0, right),
                (rgt + h0, h1, 0, left),
                (own + h0, h1, 0, right),
                (own, h0, 0, left),
            )[i]
        if i < 6:
            src, dst = self.view(self.x, start, n_rows), self.recv[phase].at[pl.ds(at, n_rows)]
        else:
            src = dst = self.view(self.y, start, n_rows)
        return remote(src, dst, self.sems, HOPS * phase + i, device)

    def rs_start(self, phase):
        for i in (0, 2, 3) if phase >= self.direct else range(4):
            self.hop(phase, i).start()

    def rs_mid(self, phase):
        if phase >= self.direct:
            return
        slab, h0, h1, (own, rgt, opp, lft), *_ = self.place(phase)
        buf = self.recv[phase]
        self.hop(phase, 0).wait_recv()
        add_rows(self.x, rgt, [(buf, 0)], h0, self.lanes)
        self.hop(phase, 4).start()
        self.hop(phase, 1).wait_recv()
        add_rows(self.x, lft + h0, [(buf, h0)], h1, self.lanes)
        self.hop(phase, 5).start()

    def rs_end(self, phase):
        slab, _, _, (own, _, _, _), *_ = self.place(phase)
        buf = self.recv[phase]
        terms = [(buf, slab), (buf, 2 * slab)]
        if phase >= self.direct:
            terms.append((buf, 0))
        for i in (0, 2, 3) if phase >= self.direct else range(2, 6):
            self.hop(phase, i).wait_recv()
        add_rows(self.x, own, terms, slab, self.lanes)

    def ag_start(self, phase):
        for i in (6, 7, 8) if phase >= self.direct else (6, 7, 10, 11):
            self.hop(phase, i).start()

    def ag_mid(self, phase):
        if phase >= self.direct:
            return
        self.hop(phase, 6).wait_recv()
        self.hop(phase, 8).start()
        self.hop(phase, 7).wait_recv()
        self.hop(phase, 9).start()
        self.hop(phase, 10).wait_recv()
        self.hop(phase, 11).wait_recv()

    def ag_end(self, phase):
        for i in (6, 7, 8) if phase >= self.direct else (8, 9):
            self.hop(phase, i).wait_recv()

    def own_rows(self):
        return self.place(2)[3][0]

    def drain(self, rs=(), ag=()):
        for phase in rs:
            for i in (0, 2, 3) if phase >= self.direct else range(6):
                self.hop(phase, i).wait_send()
        for phase in ag:
            for i in (6, 7, 8) if phase >= self.direct else range(6, HOPS):
                self.hop(phase, i).wait_send()


def stage(parts, step):
    for part in parts:
        getattr(part, step[:-1])(int(step[-1]))


def slab_rows(rb):
    return [3 * rb * RING ** (2 - phase) for phase in COLOURS]


def place_in_order(block, order):
    digit = [(block // s) % RING for s in AXIS_STRIDE]
    return (digit[order[0]] * RING + digit[order[1]]) * RING + digit[order[2]]


def by_rows(n_rows, align):
    unit = n_rows // align
    counts = [(unit + 2 - c) // 3 for c in COLOURS]
    starts = [sum(counts[:c]) * align for c in COLOURS]
    return [(starts[c], counts[c] * align) for c in COLOURS]


def pair(n):
    return [pltpu.SemaphoreType.DMA((n,)), pltpu.SemaphoreType.DMA((n,))]


def thirds(n, unit):
    most = n * 3 // 8
    sizes = (most, most, n - 2 * most)
    return [(unit * most * c, unit * size) for c, size in enumerate(sizes)]


def wide_lanes(d_model):
    few = d_model // 128 * 5 // 16 * 128
    sizes = (few, d_model - 2 * few, few)
    return [(sum(sizes[:c]), size) for c, size in enumerate(sizes)]


def spread(ring, src_of, dst, n_rows, sems):
    pos, right, left, across = ring
    rows = dst.at[pl.ds(pl.multiple_of(pos * n_rows, n_rows), n_rows)]
    hops = enumerate((right, across, left))
    return [remote(src_of((pos + i + 1) % RING), rows, sems, i, device) for i, device in hops]


def place_heads(dst, src):
    n_batch, n_rows, head_dim = src.shape
    for b in range(n_batch):
        for h in range(n_rows // BLK):
            dst[pl.ds(b * BLK, BLK), pl.ds(h * head_dim, head_dim)] = src[b, h * BLK:(h + 1) * BLK, :]


D_TILE = 256


class Return:
    def __init__(self, src, dst, sems):
        self.src, self.dst, self.sems = src, dst, sems
        self.cp, self.tp = lax.axis_index("cp"), lax.axis_index("tp")
        self.mirror = RING ** 3 - 1 - self.cp
        self.group = self.cp // (RING ** 3 // 2)
        self.is_mine = self.tp == self.group

    def give(self, piece_idx):
        device = (self.group, self.mirror) if piece_idx else (1 - self.tp, self.cp)
        return pltpu.make_async_remote_copy(src_ref=self.src.at[piece_idx], dst_ref=self.dst.at[self.tp], send_sem=self.sems[0].at[piece_idx], recv_sem=self.sems[1].at[self.tp], device_id=device, device_id_type=MESH)

    def take(self, batch):
        return pltpu.make_async_remote_copy(src_ref=self.src.at[1], dst_ref=self.dst.at[batch], send_sem=self.sems[0].at[1], recv_sem=self.sems[1].at[batch], device_id=(self.group, self.mirror), device_id_type=MESH)

    def start(self):
        self.give(1).start()

        @pl.when(jnp.logical_not(self.is_mine))
        def _():
            self.give(0).start()

        @pl.when(self.is_mine)
        def _():
            self.dst[self.tp] = self.src[0]

    def wait(self):
        self.take(1 - self.tp).wait_recv()

        @pl.when(jnp.logical_not(self.is_mine))
        def _():
            self.take(self.tp).wait_recv()

    def drain(self):
        self.give(1).wait_send()

        @pl.when(jnp.logical_not(self.is_mine))
        def _():
            self.give(0).wait_send()


class Handout:
    def __init__(self, src, dst, sems):
        self.src, self.dst, self.sems = src, dst, sems
        self.cp, self.tp = lax.axis_index("cp"), lax.axis_index("tp")
        self.mirror = RING ** 3 - 1 - self.cp
        self.is_mine = self.tp == self.cp // (RING ** 3 // 2)

    def copy(self, kind, batch, slot, device, sem):
        return pltpu.make_async_remote_copy(src_ref=self.src[kind].at[batch], dst_ref=self.dst.at[slot, kind], send_sem=self.sems[0].at[2 * kind + sem], recv_sem=self.sems[1].at[2 * kind + slot], device_id=device, device_id_type=MESH)

    def near(self, kind):
        return self.copy(kind, 1 - self.tp, 0, (1 - self.tp, self.cp), 0)

    def far(self, kind, batch):
        return self.copy(kind, batch, 1, (batch, self.mirror), batch)

    def start(self, kind):
        @pl.when(self.is_mine)
        def _():
            self.near(kind).start()
            self.dst[0, kind] = self.src[kind][self.tp]

        @pl.when(jnp.logical_not(self.is_mine))
        def _():
            self.far(kind, 0).start()
            self.far(kind, 1).start()

    def wait(self, kind):
        self.far(kind, 0).wait_recv()

        @pl.when(jnp.logical_not(self.is_mine))
        def _():
            self.near(kind).wait_recv()

    def drain(self, kind):
        @pl.when(self.is_mine)
        def _():
            self.near(kind).wait_send()

        @pl.when(jnp.logical_not(self.is_mine))
        def _():
            self.far(kind, 0).wait_send()
            self.far(kind, 1).wait_send()


D_TILE = 256


def attn_kernel(k_ref, v_ref, q_ref, hid_ref, grad_ref, wo_ref, cos_ref, sin_ref, dqh_ref, out_ref, sl0, sl1, sl2, red0, red1, red2, ho0, ho1, ho2, y0, y1, y2, kv_scr, qd_scr, o_scr, qt_scr, dot_scr, dqt_scr, m_scr, l_scr, delta_scr, p_scr, ds_scr, dkv_scr, tok_scr, part_scr, got_scr, out_scr, rot_scr, oh_scr, dqh_scr, do_home, *rest):
    rest = list(rest)

    def grab(n):
        return [rest.pop(0) for _ in range(n)]

    hr, gr, orr, xs = (grab(3) for _ in range(4))
    k_sems, d_sems, r_sems, h_sems, g_sems, or_sems = ([grab(2) for _ in COLOURS] for _ in range(6))
    red_scr = grab(3)
    hand_sems, oh_sems, dqh_sems, swap_sems = (grab(2) for _ in range(4))
    n_groups, _, n_cols, e_dim = qd_scr.shape
    rows = k_ref.shape[0]
    per_tile = TILE // BLK
    n_blk = RING ** 3
    d_model = grad_ref.shape[1]
    cp = lax.axis_index("cp")
    mirror = n_blk - 1 - cp
    rings = [ring_of(axis) for axis in COLOURS]
    o_lanes = wide_lanes(d_model)
    ys = (y0, y1, y2)
    split = by_rows(rows, 16)
    p_kv = [Part(rings, ORDERS[c], split[c][1], k_sems[c], y=ys[c], lanes=(0, 2 * e_dim), align=16, direct=1) for c in COLOURS]
    rows_d = by_rows(rows, 8)
    p_d = [Part(rings, ORDERS[c], rows_d[c][1], d_sems[c], x=xs[c], recv=grab(1), lanes=(0, 2 * e_dim)) for c in COLOURS]
    first_rows = [0 - rings[order[0]][0] * (n_cols // RING) for order in ORDERS]
    p_r = [Part(rings, ORDERS[c], n_cols // n_blk, r_sems[c], x=red_scr[c], recv=[None] + grab(2), row0=first_rows[c], lanes=(0, o_lanes[c][1])) for c in COLOURS]
    h_out, = rest
    hand = Handout((q_ref, do_home), qd_scr, hand_sems)
    o_back = Return(o_scr, oh_scr, oh_sems)
    dq_back = Return(rot_scr, dqh_scr, dqh_sems)

    for c in COLOURS:
        own = pl.ds(pl.multiple_of(p_kv[c].own_rows(), 16), split[c][1])
        ys[c][own, :e_dim] = k_ref[pl.ds(*split[c]), :]
        ys[c][own, e_dim:] = v_ref[pl.ds(*split[c]), :]
    enter(rings, with_partner=True, with_mirror=True)
    stage(p_kv, "ag_start2")
    stage(p_kv, "ag_end2")
    stage(p_kv, "ag_start1")
    hand.start(0)
    stage(p_kv, "ag_end1")
    stage(p_kv, "ag_start0")
    for cols in range(0, n_cols, COLS):
        res = lax.dot_general(grad_ref[...], wo_ref[pl.ds(cols, COLS), :], (((1,), (1,)), ((), ())), preferred_element_type=F32).astype(BF16)
        for b in range(n_groups):
            for h in range(COLS // e_dim):
                do_home[b, pl.ds(cols + h * rows, rows), :] = res[b * rows:(b + 1) * rows, h * e_dim:(h + 1) * e_dim]
    dqt_scr[...] = jnp.zeros_like(dqt_scr)
    dkv_scr[...] = jnp.zeros_like(dkv_scr)
    m_scr[...] = jnp.full_like(m_scr, -jnp.inf)
    l_scr[...] = jnp.zeros_like(l_scr)
    hand.wait(0)
    for grp in range(n_groups):
        qt_scr[grp] = qd_scr[grp, 0].T
    stage(p_kv, "ag_mid0")
    hand.start(1)
    stage(p_kv, "ag_end0")

    def place_kv(blk, carry):
        for c in COLOURS:
            at, rb = split[c]
            src = pl.ds(pl.multiple_of(place_in_order(blk, ORDERS[c]) * rb, 16), rb)
            kv_scr[pl.ds(pl.multiple_of(blk * rows + at, 16), rb), :] = ys[c][src, :]
        return carry

    h_slab = d_model // RING
    n_tok = hid_ref.shape[0]

    def hid_cols(pos):
        return hid_ref.at[:, pl.ds(pl.multiple_of(pos * h_slab, h_slab), h_slab)]

    def grad_cols(c):
        return grad_ref.at[:, pl.ds(*o_lanes[c])]

    h_sent, g_sent = [], []
    for c in COLOURS:
        ring = rings[ORDERS[c][0]]
        here = pl.ds(pl.multiple_of(ring[0] * n_tok, n_tok), n_tok)
        h_sent += spread(ring, hid_cols, hr[c], n_tok, h_sems[c])
        g_sent += spread(ring, lambda pos, c=c: grad_cols(c), gr[c], n_tok, g_sems[c])
        hr[c][here, :] = hid_cols(ring[0])[...]
        gr[c][here, :] = grad_cols(c)[...]
    for copy in g_sent:
        copy.start()
    for copy in h_sent:
        copy.start()
    lax.fori_loop(0, n_blk, place_kv, 0)

    n_first = cp // per_tile + 1
    n_steps = n_blk // per_tile + 1

    def over_tiles(tile_step, extra):
        def body(t, carry):
            grp = (t - n_first + n_steps) // n_steps
            piece = cp + grp * (mirror - cp)
            tile_idx = t - grp * n_first
            last = tile_idx == piece // per_tile

            @pl.when(jnp.logical_not(last))
            def _():
                tile_step(grp, tile_idx, piece, False)

            @pl.when(last)
            def _():
                tile_step(grp, tile_idx, piece, True)

            for when, action in extra:
                pl.when(t == when)(action)
            return carry

        lax.fori_loop(0, n_steps, body, 0)

    def fwd_step(grp, tile_idx, piece, masked):
        row0 = pl.multiple_of(tile_idx * TILE, TILE)
        k_t = kv_scr[pl.ds(row0, TILE), :e_dim]
        v_t = kv_scr[pl.ds(row0, TILE), e_dim:]
        for c0 in range(0, n_cols, COLS):
            cs = slice(c0, c0 + COLS)
            s = dot(k_t, qt_scr[grp, :, cs])
            if masked:
                s = jnp.where(causal_mask(row0, piece * BLK, COLS), s, -jnp.inf)
            m_old = m_scr[grp, :, cs]
            m_new = jnp.maximum(m_old, jnp.max(s, axis=0, keepdims=True))
            p = jnp.exp(s - m_new)
            alpha = jnp.exp(m_old - m_new)
            m_scr[grp, :, cs] = m_new
            l_scr[grp, :, cs] = l_scr[grp, :, cs] * alpha + jnp.sum(p, axis=0, keepdims=True)
            dqt_scr[grp, :, cs] = dqt_scr[grp, :, cs] * alpha + dot_ta(v_t, p.astype(BF16))

    over_tiles(fwd_step, ())
    hand.wait(1)
    for grp in range(n_groups):
        o_t = (dqt_scr[grp] / l_scr[grp]).astype(BF16)
        o_scr[grp] = o_t.T
        dot_scr[grp] = qd_scr[grp, 1].T
        delta_scr[grp] = jnp.sum(dot_scr[grp].astype(F32) * o_t.astype(F32), axis=0, keepdims=True)
    o_back.start()
    m_scr[...] = m_scr[...] + jnp.log(l_scr[...])
    dqt_scr[...] = jnp.zeros_like(dqt_scr)

    def bwd_step(grp, tile_idx, piece, masked):
        row0 = pl.multiple_of(tile_idx * TILE, TILE)
        k_t = kv_scr[pl.ds(row0, TILE), :e_dim]
        v_t = kv_scr[pl.ds(row0, TILE), e_dim:]
        for c0 in range(0, n_cols, COLS):
            cs = slice(c0, c0 + COLS)
            s = dot(k_t, qt_scr[grp, :, cs])
            p = jnp.exp(s - m_scr[grp, :, cs])
            if masked:
                p = jnp.where(causal_mask(row0, piece * BLK, COLS), p, 0.0)
            d_p = dot(v_t, dot_scr[grp, :, cs])
            p_scr[:, cs] = p.astype(BF16)
            ds_scr[:, cs] = (p * (d_p - delta_scr[grp, :, cs])).astype(BF16)
        at = pl.ds(row0, TILE)
        dkv_scr[at, :e_dim] += dot(ds_scr[...], qd_scr[grp, 0])
        dkv_scr[at, e_dim:] += dot(p_scr[...], qd_scr[grp, 1])
        dqt_scr[grp] += dot_ta(k_t, ds_scr[...])

    o_slab = n_cols // RING

    def o_cols(pos):
        return tok_scr.at[:, pl.ds(pl.multiple_of(pos * o_slab, o_slab), o_slab)]

    def o_spread():
        return [copy for c in COLOURS for copy in spread(rings[ORDERS[c][0]], o_cols, orr[c], n_tok, or_sems[c])]

    def send_o():
        o_back.wait()
        place_heads(tok_scr, oh_scr)
        for c in COLOURS:
            pos = rings[ORDERS[c][0]][0]
            orr[c][pl.ds(pl.multiple_of(pos * n_tok, n_tok), n_tok), :] = o_cols(pos)[...]
        for copy in o_spread():
            copy.start()

    def slab_wo():
        for copy in o_spread() + g_sent:
            copy.wait_recv()
        for c, red in enumerate(red_scr):
            for at in range(0, red.shape[1], 128):
                red[:, at:at + 128] = dot_ta(orr[c][...], gr[c][:, at:at + 128])
        stage(p_r, "rs_start1")

    def step_wo():
        stage(p_r, "rs_end1")
        stage(p_r, "rs_start2")

    over_tiles(bwd_step, ((3, send_o), (7, slab_wo), (10, lambda: stage(p_r, "rs_mid1")), (13, step_wo)))

    def place_dkv(blk, carry):
        for c in COLOURS:
            at, rb = rows_d[c]
            dst = pl.ds(pl.multiple_of(place_in_order(blk, ORDERS[c]) * rb, 8), rb)
            xs[c][dst, :] = dkv_scr[pl.ds(pl.multiple_of(blk * rows + at, 8), rb), :]
        return carry

    lax.fori_loop(0, n_blk, place_dkv, 0)
    stage(p_d, "rs_start0")
    stage(p_r, "rs_end2")
    for part, out in zip(p_r, (red0, red1, red2)):
        out[...] = part.x[pl.ds(pl.multiple_of(part.own_rows(), 8), part.rb), :]

    scale = e_dim ** -0.5
    half_dim = e_dim // 2
    for grp in range(n_groups):
        cos_t, sin_t = cos_ref[grp], sin_ref[grp]
        for h in range(n_cols // rows):
            cols = slice(h * rows, (h + 1) * rows)
            low, high = dqt_scr[grp, :half_dim, cols], dqt_scr[grp, half_dim:, cols]
            turned = jnp.concatenate([low * cos_t + high * sin_t, high * cos_t - low * sin_t], axis=0) * scale
            rot_scr[grp, cols, :] = turned.T.astype(BF16)
    dq_back.start()
    for copy in h_sent:
        copy.wait_recv()
    h_outs = [pltpu.make_async_copy(hr[c], out, h_out.at[c]) for c, out in enumerate((ho0, ho1, ho2))]
    for copy in h_outs:
        copy.start()

    tp = lax.axis_index("tp")
    partner = (1 - tp, cp)
    for at in range(0, d_model, D_TILE):
        cols = slice(at, at + D_TILE)
        res = dot(tok_scr[...], wo_ref[:, cols])
        for b in range(n_groups):
            part_scr[b, :, cols] = res[b * rows:(b + 1) * rows]

    def swap(src, dst, i):
        return pltpu.make_async_remote_copy(src_ref=src, dst_ref=dst, send_sem=swap_sems[0].at[i], recv_sem=swap_sems[1].at[i], device_id=partner, device_id_type=MESH)

    swap_part = swap(part_scr.at[1 - tp], got_scr, 0)
    swap_part.start()
    stage(p_d, "rs_mid0")
    swap_part.wait()
    out_scr[tp] = (part_scr[tp] + got_scr[...]).astype(BF16)
    swap_out = swap(out_scr.at[tp], out_scr.at[tp], 1)
    swap_out.start()
    dq_back.wait()

    def put(src, dst):
        copy = pltpu.make_async_copy(src, dst, h_out.at[len(h_outs)])
        copy.start()
        h_outs.append(copy)

    put(dqh_scr, dqh_ref)
    swap_out.wait()
    put(out_scr, out_ref)
    stage(p_d, "rs_end0")
    for part, out in zip(p_d, (sl0, sl1, sl2)):
        slab, _, _, starts, *_ = part.place(0)
        put(part.view(part.x, starts[0], slab), out)
    for part in p_kv:
        part.drain(ag=COLOURS)
    for part in p_d:
        part.drain(rs=(0,))
    for part in p_r:
        part.drain(rs=(1, 2))
    for kind in range(2):
        hand.drain(kind)
    for copy in h_sent + g_sent + o_spread():
        copy.wait_send()
    for copy in h_outs:
        copy.wait()
    o_back.drain()
    dq_back.drain()


def attention(key_loc, val_loc, q_home, hid, grad, w_out, cos_t, sin_t):
    n_batch, n_cols, e_dim = q_home.shape
    rows = key_loc.shape[0]
    n_tok, d_model = grad.shape
    n_blk = RING ** 3
    seq = n_blk * rows
    o_lanes = wide_lanes(d_model)
    slab = n_cols // RING
    vmem, anyspace = pl.BlockSpec(memory_space=pltpu.VMEM), pl.BlockSpec(memory_space=pl.ANY)
    heads = (2, n_cols, e_dim)
    h_ring = (RING * n_tok, d_model // RING)
    work = n_cols * seq
    return pl.pallas_call(
        attn_kernel,
        out_shape=(jax.ShapeDtypeStruct(heads, BF16), jax.ShapeDtypeStruct((2, rows, d_model), BF16)) + tuple(jax.ShapeDtypeStruct((n_blk // RING * rb, 2 * e_dim), F32) for _, rb in by_rows(rows, 8)) + tuple(jax.ShapeDtypeStruct((n_cols // n_blk, n), F32) for _, n in o_lanes) + (jax.ShapeDtypeStruct(h_ring, BF16),) * 3,
        in_specs=[vmem] * 8,
        out_specs=(anyspace,) * 5 + (vmem,) * 3 + (anyspace,) * 3,
        scratch_shapes=[pltpu.VMEM((n_blk * rb, 2 * e_dim), BF16) for _, rb in by_rows(rows, 16)]
        + [
            pltpu.VMEM((seq, 2 * e_dim), BF16),
            pltpu.VMEM((2, 2, n_cols, e_dim), BF16),
            pltpu.VMEM(heads, BF16),
            pltpu.VMEM((2, e_dim, n_cols), BF16),
            pltpu.VMEM((2, e_dim, n_cols), BF16),
            pltpu.VMEM((2, e_dim, n_cols), F32),
            pltpu.VMEM((2, 1, n_cols), F32),
            pltpu.VMEM((2, 1, n_cols), F32),
            pltpu.VMEM((2, 1, n_cols), F32),
            pltpu.VMEM((TILE, n_cols), BF16),
            pltpu.VMEM((TILE, n_cols), BF16),
            pltpu.VMEM((seq, 2 * e_dim), F32),
            pltpu.VMEM((n_tok, n_cols), BF16),
            pltpu.VMEM((2, rows, d_model), F32),
            pltpu.VMEM((rows, d_model), F32),
            pltpu.VMEM((2, rows, d_model), BF16),
        ]
        + [pltpu.VMEM(heads, BF16)] * 4
        + [pltpu.VMEM(h_ring, BF16)] * 3
        + [pltpu.VMEM((RING * n_tok, lanes), BF16) for _, lanes in o_lanes]
        + [pltpu.VMEM((RING * n_tok, slab), BF16)] * 3
        + [pltpu.VMEM((n_blk * rb, 2 * e_dim), F32) for _, rb in by_rows(rows, 8)]
        + pair(3 * HOPS) * 9
        + pair(3) * 9
        + [pltpu.VMEM((slab, lanes), F32) for _, lanes in o_lanes]
        + pair(4)
        + pair(2) * 3
        + [pltpu.VMEM((slab_rows(rb)[0], 2 * e_dim), F32) for _, rb in by_rows(rows, 8)]
        + [pltpu.VMEM((n, lanes), F32) for _, lanes in o_lanes for n in slab_rows(n_cols // n_blk)[1:]]
        + [pltpu.SemaphoreType.DMA((8,))],
        compiler_params=pltpu.CompilerParams(collective_id=2, has_side_effects=True, vmem_limit_bytes=VMEM_LIMIT),
        cost_estimate=pl.CostEstimate(flops=14 * work * e_dim, bytes_accessed=seq * e_dim * 12, transcendentals=2 * work),
        name="attention",
    )(key_loc, val_loc, q_home, hid, grad, w_out, cos_t, sin_t)


GRAD_PLAN = (
    "o.ag_start2", "d.rs_start1", "o.ag_end2", "o.ag_start1", "weights.q", "d.rs_mid1", "o.ag_mid1", "d.rs_end1",
    "d.rs_start2", "s.rs_start1", "d.rs_end2", "o.ag_end1", "weights.prep", "s.rs_mid1", "weights.kv", "o.ag_start0",
    "weights.slab", "t.rs_start1", "s.rs_end1", "t.rs_mid1", "s.rs_start2", "o.ag_mid0", "s.rs_end2", "t.rs_end1",
    "q.ag_start2", "t.rs_start2", "t.rs_end2", "k.ag_start2", "q.ag_end2", "q.ag_start1", "k.ag_end2", "k.ag_start1",
    "q.ag_mid1", "k.ag_mid1", "q.ag_end1", "q.ag_start0", "k.ag_end1", "k.ag_start0", "o.ag_end0", "k.ag_mid0",
    "q.ag_mid0", "k.ag_end0", "q.ag_end0",
)


def grad_kernel(sl0, sl1, sl2, dqh_ref, red0, red1, red2, hi0, hi1, hi2, cos_ref, sin_ref, gq_ref, go_ref, gk_ref, gv_ref, dkd_ref, yq, yo, yk, yp, turn_scr, tok_scr, kvt_scr, kvr_scr, mine_scr, give_scr, got_scr, xk, *rest):
    rest = list(rest)

    def grab(n):
        return [rest.pop(0) for _ in range(n)]

    n_blk = RING ** 3
    n_batch, _, head_dim = dqh_ref.shape
    n_tok, n_cols = tok_scr.shape
    d_model = yq.shape[0]
    rows, lanes = n_tok // n_batch, 2 * head_dim
    n_local = n_cols // head_dim
    q_lanes, o_lanes = thirds(n_local, head_dim), wide_lanes(d_model)
    split = by_rows(rows, 8)
    tp, cp = lax.axis_index("tp"), lax.axis_index("cp")
    partner = (1 - tp, cp)
    rings = [ring_of(axis) for axis in COLOURS]

    def shifted(c, n_rows):
        return 0 - rings[ORDERS[c][0]][0] * (n_rows // RING)

    xs, xqs, hr, dqr = (grab(3) for _ in range(4))
    sem_d, sem_q, sem_o, sem_g = ([grab(2) for _ in COLOURS] for _ in range(4))
    sem_k, sem_kr = grab(2), grab(2)
    p_d = [Part(rings, ORDERS[c], split[c][1], sem_d[c], x=xs[c], recv=[None] + grab(2), row0=shifted(c, n_blk * split[c][1]), lanes=(0, lanes)) for c in COLOURS]
    p_s = [Part(rings, ORDERS[c], d_model // n_blk, sem_q[c], x=xqs[c], recv=[None] + grab(2), row0=shifted(c, d_model), lanes=(0, q_lanes[c][1])) for c in COLOURS]
    p_q = [Part(rings, ORDERS[c], d_model // n_blk, sem_q[c], y=yq, lanes=q_lanes[c]) for c in COLOURS]
    p_o = [Part(rings, ORDERS[c], n_cols // n_blk, sem_o[c], y=yo, lanes=o_lanes[c]) for c in COLOURS]
    p_t = [Part(rings, ORDERS[2], d_model // n_blk, sem_k, x=xk, recv=[None] + grab(2), row0=shifted(2, d_model), lanes=(0, head_dim))]
    p_k = [Part(rings, ORDERS[2], d_model // n_blk, sem_k, y=yk, lanes=(0, head_dim))]
    in_sem, out_sem, swap_s, swap_r = rest

    loads = [pltpu.make_async_copy(src, dst, in_sem.at[i]) for i, (src, dst) in enumerate(zip((sl0, sl1, sl2, hi0, hi1, hi2), xs + hr))]
    for copy in loads:
        copy.start()
    place_heads(tok_scr, dqh_ref)

    def tok_cols(c):
        return pl.ds(*q_lanes[c])

    for part, red in zip(p_o, (red0, red1, red2)):
        part.y[pl.ds(pl.multiple_of(part.own_rows(), 8), part.rb), pl.ds(*part.lanes)] = red[...]
    dq_sent = []
    for c in COLOURS:
        ring = rings[ORDERS[c][0]]
        dqr[c][pl.ds(pl.multiple_of(ring[0] * n_tok, n_tok), n_tok), :] = tok_scr[:, tok_cols(c)]
        dq_sent += spread(ring, lambda pos, c=c: tok_scr.at[:, tok_cols(c)], dqr[c], n_tok, sem_g[c])
    ring_k = rings[ORDERS[2][0]]
    kv_sent = spread(ring_k, lambda pos: kvt_scr, kvr_scr, n_tok, sem_kr)
    enter(rings, with_partner=True)
    for copy in dq_sent:
        copy.start()
    for copy in loads:
        copy.wait()
    half_dim = head_dim // 2
    first = tp == 0
    swap_small = pltpu.make_async_remote_copy(src_ref=give_scr, dst_ref=got_scr, send_sem=swap_s.at[0], recv_sem=swap_r.at[0], device_id=partner, device_id_type=MESH)
    swap = pltpu.make_async_remote_copy(src_ref=yk, dst_ref=yp, send_sem=swap_s.at[1], recv_sem=swap_r.at[1], device_id=partner, device_id_type=MESH)

    def put_o(which):
        for c, part in enumerate(p_o):
            slab, _, _, starts, *_ = part.place(0)
            for i in which:
                pltpu.make_async_copy(part.view(yo, starts[i], slab), part.view(go_ref, starts[i], slab), out_sem.at[c]).start()

    def turn_q(which):
        for c, part in enumerate(p_q):
            slab, _, _, starts, *_ = part.place(0)
            for i in which:
                at = pl.multiple_of(starts[i], slab)
                for h in range(q_lanes[c][0] // head_dim, sum(q_lanes[c]) // head_dim):
                    turn_scr[pl.ds(at * n_local + h, slab, stride=n_local), :] = yq[pl.ds(at, slab), pl.ds(h * head_dim, head_dim)]

    def own_block(parts, sums):
        for part, total in zip(parts, sums):
            at, lanes_y, lanes_x = part.own_rows(), pl.ds(*part.lanes), pl.ds(*total.lanes)
            part.y[pl.ds(pl.multiple_of(at, 8), part.rb), lanes_y] = total.x[pl.ds(pl.multiple_of(total.own_rows(), 8), part.rb), lanes_x]

    def slab_term(dst, hid, other):
        for at in range(0, dst.shape[0], D_TILE):
            dst[pl.ds(at, D_TILE), :] = dot_ta(hid[:, at:at + D_TILE], other[...])

    def weights_q():
        for copy in dq_sent:
            copy.wait_recv()
        for c in COLOURS:
            slab_term(xqs[c], hr[c], dqr[c])

    def new_dkv():
        dkd_ref[...] = mine_scr[...].astype(BF16)
        return dkd_ref[:, :head_dim], dkd_ref[:, head_dim:]

    def weights_prep():
        for c in COLOURS:
            at, rb = split[c]
            own = xs[c][pl.ds(pl.multiple_of(p_d[c].own_rows(), 8), rb), :]
            cos_tab, sin_tab = cos_ref[pl.ds(at, rb), :], sin_ref[pl.ds(at, rb), :]
            low, high = own[:, :half_dim], own[:, half_dim:head_dim]
            mine_scr[pl.ds(at, rb), :head_dim] = jnp.concatenate([low * cos_tab + high * sin_tab, high * cos_tab - low * sin_tab], axis=1)
            mine_scr[pl.ds(at, rb), head_dim:] = own[:, head_dim:]
        dk_new, dv_new = new_dkv()
        give_scr[...] = jnp.where(first, dv_new, dk_new)
        swap_small.start()

    def weights_kv():
        swap_small.wait()
        got = got_scr[...]
        keep = jnp.where(first, dkd_ref[:, :head_dim], dkd_ref[:, head_dim:])
        kvt_scr[...] = jnp.concatenate([jnp.where(first, keep, got), jnp.where(first, got, keep)], axis=0)
        kvr_scr[pl.ds(pl.multiple_of(ring_k[0] * n_tok, n_tok), n_tok), :] = kvt_scr[...]
        for copy in kv_sent:
            copy.start()

    def weights_slab():
        for copy in kv_sent:
            copy.wait_recv()
        slab_term(xk, hr[2], kvr_scr)

    groups = {"d": p_d, "s": p_s, "q": p_q, "o": p_o, "t": p_t, "k": p_k}
    after = {
        "weights.q": weights_q,
        "weights.prep": weights_prep,
        "weights.kv": weights_kv,
        "weights.slab": weights_slab,
        "s.rs_end2": lambda: own_block(p_q, p_s),
        "t.rs_end2": lambda: own_block(p_k, p_t),
        "o.ag_mid0": lambda: put_o((0, 1, 3)),
        "o.ag_end0": lambda: put_o((2,)),
        "q.ag_start0": lambda: turn_q((0,)),
        "q.ag_mid0": lambda: turn_q((1, 3)),
        "q.ag_end0": lambda: turn_q((2,)),
        "k.ag_end0": swap.start,
    }
    for step in GRAD_PLAN:
        who, what = step.split(".")
        if who in groups:
            stage(groups[who], what)
        if step in after:
            after[step]()
    out_q = pltpu.make_async_copy(turn_scr, gq_ref, out_sem.at[3])
    out_q.start()
    swap.wait()

    def put_kv(k_src, v_src):
        outs = [pltpu.make_async_copy(k_src, gk_ref, out_sem.at[4]), pltpu.make_async_copy(v_src, gv_ref, out_sem.at[5])]
        for copy in outs:
            copy.start()
        for copy in outs:
            copy.wait()

    @pl.when(first)
    def _():
        put_kv(yk, yp)

    @pl.when(jnp.logical_not(first))
    def _():
        put_kv(yp, yk)

    out_q.wait()
    for c, part in enumerate(p_o):
        pltpu.make_async_copy(part.view(yo, 0, n_cols), part.view(go_ref, 0, n_cols), out_sem.at[c]).wait()
    for part in p_d + p_s + p_t:
        part.drain(rs=(1, 2))
    for part in p_q + p_o + p_k:
        part.drain(ag=COLOURS)
    for copy in dq_sent + kv_sent:
        copy.wait_send()


def grad_sums(slabs, dq_home, reds, h_rings, cos_tab, sin_tab, d_model):
    n_batch, n_rows, head_dim = dq_home.shape
    rows = cos_tab.shape[0]
    n_tok, n_cols = n_batch * rows, n_rows // rows * head_dim
    n_blk = RING ** 3
    lanes = 2 * head_dim
    q_lanes = thirds(n_cols // head_dim, head_dim)
    split = by_rows(rows, 8)
    vmem, anyspace = pl.BlockSpec(memory_space=pltpu.VMEM), pl.BlockSpec(memory_space=pl.ANY)

    def full(*shape):
        return pltpu.VMEM(shape, F32)

    def half(*shape):
        return pltpu.VMEM(shape, BF16)

    def later(rb, width):
        return [full(n, width) for n in slab_rows(rb)[1:]]

    slab, ring_tok = d_model // RING, RING * n_tok
    scratch = [full(d_model, n_cols), full(n_cols, d_model), full(d_model, head_dim), full(d_model, head_dim), full(d_model * n_cols // head_dim, head_dim)]
    scratch += [half(n_tok, n_cols), half(n_tok, head_dim), half(ring_tok, head_dim), full(rows, lanes), half(rows, head_dim), half(rows, head_dim), full(slab, head_dim)]
    scratch += [full(n_blk // RING * rb, lanes) for _, rb in split]
    scratch += [full(slab, w) for _, w in q_lanes]
    scratch += [half(ring_tok, slab)] * 3 + [half(ring_tok, w) for _, w in q_lanes]
    scratch += pair(3 * HOPS) * 9 + pair(3) * 3 + pair(3 * HOPS) + pair(3)
    for _, rb in split:
        scratch += later(rb, lanes)
    for _, w in q_lanes:
        scratch += later(d_model // n_blk, w)
    scratch += later(d_model // n_blk, head_dim)
    scratch += [pltpu.SemaphoreType.DMA((6,)), pltpu.SemaphoreType.DMA((6,))] + pair(2)
    return pl.pallas_call(
        grad_kernel,
        out_shape=(
            jax.ShapeDtypeStruct((d_model * n_cols // head_dim, head_dim), F32),
            jax.ShapeDtypeStruct((n_cols, d_model), F32),
            jax.ShapeDtypeStruct((d_model, head_dim), F32),
            jax.ShapeDtypeStruct((d_model, head_dim), F32),
            jax.ShapeDtypeStruct((rows, lanes), BF16),
        ),
        in_specs=[anyspace] * 3 + [vmem] * 4 + [anyspace] * 3 + [vmem] * 2,
        out_specs=(anyspace,) * 4 + (vmem,),
        scratch_shapes=scratch,
        compiler_params=pltpu.CompilerParams(collective_id=3, has_side_effects=True, vmem_limit_bytes=VMEM_LIMIT),
        cost_estimate=pl.CostEstimate(flops=n_tok * d_model * n_cols * 160, bytes_accessed=40 << 20, transcendentals=0),
        name="grad_sums",
    )(*slabs, dq_home, *reds, *h_rings, cos_tab, sin_tab)


def solution(mesh):
    cp_size = mesh.shape["cp"]
    partner = [(0, 1), (1, 0)]

    def local_program(hidden, grad_out, w_query, w_key, w_value, w_out):
        block_len = hidden.shape[1]
        n_local = w_query.shape[1]
        head_dim = w_key.shape[1]
        q_scale = head_dim ** -0.5
        cp_idx = lax.axis_index("cp")
        tp_idx = lax.axis_index("tp")
        mirror_idx = cp_size - 1 - cp_idx
        cos_tab, sin_tab = rope_tables(cp_idx * block_len + jnp.arange(block_len), head_dim)
        cos_mir, sin_mir = rope_tables(mirror_idx * block_len + jnp.arange(block_len), head_dim)

        def pick(pair, idx):
            return lax.dynamic_index_in_dim(pair, idx, 0, keepdims=False)

        def sum_over_tp(part, extra=None):
            total = pick(part, tp_idx) + lax.ppermute(pick(part, 1 - tp_idx), "tp", partner)
            if extra is not None:
                total = total + extra
            mine = total.astype(BF16)
            other = lax.ppermute(mine, "tp", partner)
            first = tp_idx == 0
            return jnp.stack([jnp.where(first, mine, other), jnp.where(first, other, mine)])

        hid_b = pick(hidden, tp_idx)
        key_loc = rotate(dot(hid_b, w_key), cos_tab, sin_tab).astype(BF16)
        val_loc = dot(hid_b, w_value).astype(BF16)
        q_pre = jnp.einsum("bsd,dhe->bhse", hidden, w_query, preferred_element_type=F32)
        queries = (rotate(q_pre, cos_tab, sin_tab) * q_scale).astype(BF16)
        q_home = queries.reshape(2, n_local * block_len, head_dim)
        d_model = hidden.shape[-1]
        hid, grad = hidden.reshape(-1, d_model), grad_out.reshape(-1, d_model)
        tabs_t = [jnp.stack(pair_t) for pair_t in ((cos_tab.T, cos_mir.T), (sin_tab.T, sin_mir.T))]
        dq_home, attn_out, *more = attention(key_loc, val_loc, q_home, hid, grad, w_out.reshape(-1, d_model), *tabs_t)
        dq_pre = dq_home.reshape(2, n_local, block_len, head_dim)
        grad_q, grad_o, d_w_key, d_w_value, dkv_new = grad_sums(more[:3], dq_home, more[3:6], more[6:], cos_tab, sin_tab, d_model)
        d_w_query = grad_q.reshape(w_query.shape)
        d_w_out = grad_o.reshape(w_out.shape)
        dk_pre, dv_pre = dkv_new[:, :head_dim], dkv_new[:, head_dim:]
        dh_kv = dot(dk_pre, w_key.T) + dot(dv_pre, w_value.T)
        d_hidden = sum_over_tp(jnp.einsum("cirf,eif->cre", dq_pre, w_query, preferred_element_type=F32), dh_kv)
        return attn_out, d_hidden, d_w_query, d_w_key, d_w_value, d_w_out

    row_spec = P(None, "cp", None)
    return jax.shard_map(local_program, mesh=mesh, in_specs=(row_spec, row_spec, P(None, "tp", None), P(), P(), P("tp", None, None)), out_specs=(row_spec, row_spec, P(None, "tp", None), P(), P(), P("tp", None, None)), check_vma=False)
```

```python
import jax
import jax.numpy as jnp
from jax import lax
from jax.experimental import pallas as pl
from jax.experimental.pallas import tpu as pltpu
from jax.sharding import PartitionSpec as P

ROPE_BASE = 10000.0
BLK = 128
TILE = 512
COLOURS = range(3)
VMEM_LIMIT = 67000000
COLS = 256
F32 = jnp.float32
BF16 = jnp.bfloat16


def rope_tables(positions, head_dim):
    half_dim = head_dim // 2
    inv_freq = 1.0 / jnp.power(ROPE_BASE, jnp.arange(half_dim, dtype=F32) * (2.0 / head_dim))
    angles = positions.astype(F32)[:, None] * inv_freq[None, :]
    return jnp.cos(angles), jnp.sin(angles)


def rotate(rot_in, cos_tab, sin_tab):
    half_dim = rot_in.shape[-1] // 2
    low_half = rot_in[..., :half_dim]
    high_half = rot_in[..., half_dim:]
    return jnp.concatenate([low_half * cos_tab - high_half * sin_tab, high_half * cos_tab + low_half * sin_tab], axis=-1)


def unrotate(rot_in, cos_tab, sin_tab):
    return rotate(rot_in, cos_tab, -sin_tab)


def dot(a, b):
    return jnp.dot(a, b, preferred_element_type=F32)


def dot_ta(a, b):
    return lax.dot_general(a, b, (((0,), (0,)), ((), ())), preferred_element_type=F32)


def causal_mask(k_start, q_start, cols):
    k_pos = k_start + lax.broadcasted_iota(jnp.int32, (TILE, cols), 0)
    q_pos = q_start + lax.broadcasted_iota(jnp.int32, (TILE, cols), 1) % BLK
    return k_pos <= q_pos


RING = 4
AXIS_STRIDE = (RING * RING, RING, 1)
ORDERS = ((0, 1, 2), (1, 2, 0), (2, 0, 1))
MESH = pl.DeviceIdType.MESH
HOPS = 12


def ring_of(axis):
    cp, tp = lax.axis_index("cp"), lax.axis_index("tp")
    stride = AXIS_STRIDE[axis]
    pos = (cp // stride) % RING
    right = cp + ((pos + 1) % RING - pos) * stride
    left = cp + ((pos + RING - 1) % RING - pos) * stride
    across = cp + ((pos + 2) % RING - pos) * stride
    return pos, (tp, right), (tp, left), (tp, across)


def enter(rings, with_partner=False, with_mirror=False):
    barrier = pltpu.get_barrier_semaphore()
    peers = []
    for _, *others in rings:
        peers += others
    if with_partner:
        peers.append((1 - lax.axis_index("tp"), lax.axis_index("cp")))
    if with_mirror:
        mirror = RING ** 3 - 1 - lax.axis_index("cp")
        peers += [(0, mirror), (1, mirror)]
    for peer in peers:
        pl.semaphore_signal(barrier, inc=1, device_id=peer, device_id_type=MESH)
    pl.semaphore_wait(barrier, len(peers))


def remote(src, dst, sems, idx, device):
    return pltpu.make_async_remote_copy(src_ref=src, dst_ref=dst, send_sem=sems[0].at[idx], recv_sem=sems[1].at[idx], device_id=device, device_id_type=MESH)


def add_rows(dst, dst0, srcs, n_rows, lanes):
    strip = next(s for s in (64, 48, 40, 32, 24, 16, 8) if n_rows % s == 0)
    if lanes[1] > 256:
        strip = next(s for s in (16, 8) if n_rows % s == 0)

    def body(i, carry):
        off = pl.multiple_of(dst0 + i * strip, 8)
        total = dst[pl.ds(off, strip), pl.ds(*lanes)]
        for ref, start in srcs:
            total = total + ref[pl.ds(pl.multiple_of(start + i * strip, 8), strip), :]
        dst[pl.ds(off, strip), pl.ds(*lanes)] = total
        return carry

    lax.fori_loop(0, n_rows // strip, body, 0)


class Part:
    def __init__(self, rings, order, rb, sems, x=None, y=None, recv=None, row0=0, lanes=None, align=8, direct=2):
        self.direct = direct
        self.rb, self.sems, self.x, self.y, self.recv = rb, sems, x, y, recv
        self.row0, self.lanes, self.align = row0, lanes, align
        self.places = []
        base = row0
        for phase in COLOURS:
            slab = rb * RING ** (2 - phase)
            h0 = -(-slab // (2 * align)) * align
            pos, right, left, across = rings[order[phase]]
            starts = [base + ((pos + d) % RING) * slab for d in range(RING)]
            self.places.append((slab, h0, slab - h0, starts, right, left, across))
            base = starts[0]

    def view(self, ref, start, n_rows):
        return ref.at[pl.ds(pl.multiple_of(start, self.align), n_rows), pl.ds(*self.lanes)]

    def place(self, phase):
        return self.places[phase]

    def hop(self, phase, i):
        slab, h0, h1, (own, rgt, opp, lft), right, left, across = self.place(phase)
        if phase >= self.direct:
            start, n_rows, at, device = {
                0: (opp, slab, 0, across),
                2: (rgt, slab, slab, right),
                3: (lft, slab, 2 * slab, left),
                6: (own, slab, 0, right),
                7: (own, slab, 0, left),
                8: (own, slab, 0, across),
            }[i]
        else:
            start, n_rows, at, device = (
                (opp, h0, 0, right),
                (opp + h0, h1, h0, left),
                (rgt + h0, h1, slab + h0, right),
                (lft, h0, 2 * slab, left),
                (rgt, h0, slab, right),
                (lft + h0, h1, 2 * slab + h0, left),
                (own, h0, 0, right),
                (own + h0, h1, 0, left),
                (lft, h0, 0, right),
                (rgt + h0, h1, 0, left),
                (own + h0, h1, 0, right),
                (own, h0, 0, left),
            )[i]
        if i < 6:
            src, dst = self.view(self.x, start, n_rows), self.recv[phase].at[pl.ds(at, n_rows)]
        else:
            src = dst = self.view(self.y, start, n_rows)
        return remote(src, dst, self.sems, HOPS * phase + i, device)

    def rs_start(self, phase):
        for i in (0, 2, 3) if phase >= self.direct else range(4):
            self.hop(phase, i).start()

    def rs_mid(self, phase):
        if phase >= self.direct:
            return
        slab, h0, h1, (own, rgt, opp, lft), *_ = self.place(phase)
        buf = self.recv[phase]
        self.hop(phase, 0).wait_recv()
        add_rows(self.x, rgt, [(buf, 0)], h0, self.lanes)
        self.hop(phase, 4).start()
        self.hop(phase, 1).wait_recv()
        add_rows(self.x, lft + h0, [(buf, h0)], h1, self.lanes)
        self.hop(phase, 5).start()

    def rs_end(self, phase):
        slab, _, _, (own, _, _, _), *_ = self.place(phase)
        buf = self.recv[phase]
        terms = [(buf, slab), (buf, 2 * slab)]
        if phase >= self.direct:
            terms.append((buf, 0))
        for i in (0, 2, 3) if phase >= self.direct else range(2, 6):
            self.hop(phase, i).wait_recv()
        add_rows(self.x, own, terms, slab, self.lanes)

    def ag_start(self, phase):
        for i in (6, 7, 8) if phase >= self.direct else (6, 7, 10, 11):
            self.hop(phase, i).start()

    def ag_mid(self, phase):
        if phase >= self.direct:
            return
        self.hop(phase, 6).wait_recv()
        self.hop(phase, 8).start()
        self.hop(phase, 7).wait_recv()
        self.hop(phase, 9).start()
        self.hop(phase, 10).wait_recv()
        self.hop(phase, 11).wait_recv()

    def ag_end(self, phase):
        for i in (6, 7, 8) if phase >= self.direct else (8, 9):
            self.hop(phase, i).wait_recv()

    def own_rows(self):
        return self.place(2)[3][0]

    def drain(self, rs=(), ag=()):
        for phase in rs:
            for i in (0, 2, 3) if phase >= self.direct else range(6):
                self.hop(phase, i).wait_send()
        for phase in ag:
            for i in (6, 7, 8) if phase >= self.direct else range(6, HOPS):
                self.hop(phase, i).wait_send()


def stage(parts, step):
    for part in parts:
        getattr(part, step[:-1])(int(step[-1]))


def slab_rows(rb):
    return [3 * rb * RING ** (2 - phase) for phase in COLOURS]


def place_in_order(block, order):
    digit = [(block // s) % RING for s in AXIS_STRIDE]
    return (digit[order[0]] * RING + digit[order[1]]) * RING + digit[order[2]]


def by_rows(n_rows, align):
    unit = n_rows // align
    counts = [(unit + 2 - c) // 3 for c in COLOURS]
    starts = [sum(counts[:c]) * align for c in COLOURS]
    return [(starts[c], counts[c] * align) for c in COLOURS]


def pair(n):
    return [pltpu.SemaphoreType.DMA((n,)), pltpu.SemaphoreType.DMA((n,))]


def thirds(n, unit):
    most = n * 3 // 8
    sizes = (most, most, n - 2 * most)
    return [(unit * most * c, unit * size) for c, size in enumerate(sizes)]


def wide_lanes(d_model):
    few = d_model // 128 * 5 // 16 * 128
    sizes = (few, d_model - 2 * few, few)
    return [(sum(sizes[:c]), size) for c, size in enumerate(sizes)]


def spread(ring, src_of, dst, n_rows, sems):
    pos, right, left, across = ring
    rows = dst.at[pl.ds(pl.multiple_of(pos * n_rows, n_rows), n_rows)]
    hops = enumerate((right, across, left))
    return [remote(src_of((pos + i + 1) % RING), rows, sems, i, device) for i, device in hops]


def place_heads(dst, src):
    n_batch, n_rows, head_dim = src.shape
    for b in range(n_batch):
        for h in range(n_rows // BLK):
            dst[pl.ds(b * BLK, BLK), pl.ds(h * head_dim, head_dim)] = src[b, h * BLK:(h + 1) * BLK, :]


D_TILE = 256


class Return:
    def __init__(self, src, dst, sems):
        self.src, self.dst, self.sems = src, dst, sems
        self.cp, self.tp = lax.axis_index("cp"), lax.axis_index("tp")
        self.mirror = RING ** 3 - 1 - self.cp
        self.group = self.cp // (RING ** 3 // 2)
        self.is_mine = self.tp == self.group

    def give(self, piece_idx):
        device = (self.group, self.mirror) if piece_idx else (1 - self.tp, self.cp)
        return pltpu.make_async_remote_copy(src_ref=self.src.at[piece_idx], dst_ref=self.dst.at[self.tp], send_sem=self.sems[0].at[piece_idx], recv_sem=self.sems[1].at[self.tp], device_id=device, device_id_type=MESH)

    def take(self, batch):
        return pltpu.make_async_remote_copy(src_ref=self.src.at[1], dst_ref=self.dst.at[batch], send_sem=self.sems[0].at[1], recv_sem=self.sems[1].at[batch], device_id=(self.group, self.mirror), device_id_type=MESH)

    def start(self):
        self.give(1).start()

        @pl.when(jnp.logical_not(self.is_mine))
        def _():
            self.give(0).start()

        @pl.when(self.is_mine)
        def _():
            self.dst[self.tp] = self.src[0]

    def wait(self):
        self.take(1 - self.tp).wait_recv()

        @pl.when(jnp.logical_not(self.is_mine))
        def _():
            self.take(self.tp).wait_recv()

    def drain(self):
        self.give(1).wait_send()

        @pl.when(jnp.logical_not(self.is_mine))
        def _():
            self.give(0).wait_send()


class Handout:
    def __init__(self, src, dst, sems):
        self.src, self.dst, self.sems = src, dst, sems
        self.cp, self.tp = lax.axis_index("cp"), lax.axis_index("tp")
        self.mirror = RING ** 3 - 1 - self.cp
        self.is_mine = self.tp == self.cp // (RING ** 3 // 2)

    def copy(self, kind, batch, slot, device, sem):
        return pltpu.make_async_remote_copy(src_ref=self.src[kind].at[batch], dst_ref=self.dst.at[slot, kind], send_sem=self.sems[0].at[2 * kind + sem], recv_sem=self.sems[1].at[2 * kind + slot], device_id=device, device_id_type=MESH)

    def near(self, kind):
        return self.copy(kind, 1 - self.tp, 0, (1 - self.tp, self.cp), 0)

    def far(self, kind, batch):
        return self.copy(kind, batch, 1, (batch, self.mirror), batch)

    def start(self, kind):
        @pl.when(self.is_mine)
        def _():
            self.near(kind).start()
            self.dst[0, kind] = self.src[kind][self.tp]

        @pl.when(jnp.logical_not(self.is_mine))
        def _():
            self.far(kind, 0).start()
            self.far(kind, 1).start()

    def wait(self, kind):
        self.far(kind, 0).wait_recv()

        @pl.when(jnp.logical_not(self.is_mine))
        def _():
            self.near(kind).wait_recv()

    def drain(self, kind):
        @pl.when(self.is_mine)
        def _():
            self.near(kind).wait_send()

        @pl.when(jnp.logical_not(self.is_mine))
        def _():
            self.far(kind, 0).wait_send()
            self.far(kind, 1).wait_send()


D_TILE = 256


def attn_kernel(k_ref, v_ref, q_ref, hid_ref, grad_ref, wo_ref, cos_ref, sin_ref, dqh_ref, out_ref, sl0, sl1, sl2, red0, red1, red2, ho0, ho1, ho2, y0, y1, y2, kv_scr, qd_scr, o_scr, qt_scr, dot_scr, dqt_scr, m_scr, l_scr, delta_scr, p_scr, ds_scr, dkv_scr, tok_scr, part_scr, got_scr, out_scr, rot_scr, oh_scr, dqh_scr, do_home, *rest):
    rest = list(rest)

    def grab(n):
        return [rest.pop(0) for _ in range(n)]

    hr, gr, orr, xs = (grab(3) for _ in range(4))
    k_sems, d_sems, r_sems, h_sems, g_sems, or_sems = ([grab(2) for _ in COLOURS] for _ in range(6))
    red_scr = grab(3)
    hand_sems, oh_sems, dqh_sems, swap_sems = (grab(2) for _ in range(4))
    n_groups, _, n_cols, e_dim = qd_scr.shape
    rows = k_ref.shape[0]
    per_tile = TILE // BLK
    n_blk = RING ** 3
    d_model = grad_ref.shape[1]
    cp = lax.axis_index("cp")
    mirror = n_blk - 1 - cp
    rings = [ring_of(axis) for axis in COLOURS]
    o_lanes = wide_lanes(d_model)
    ys = (y0, y1, y2)
    split = by_rows(rows, 16)
    p_kv = [Part(rings, ORDERS[c], split[c][1], k_sems[c], y=ys[c], lanes=(0, 2 * e_dim), align=16, direct=1) for c in COLOURS]
    rows_d = by_rows(rows, 8)
    p_d = [Part(rings, ORDERS[c], rows_d[c][1], d_sems[c], x=xs[c], recv=grab(1), lanes=(0, 2 * e_dim)) for c in COLOURS]
    first_rows = [0 - rings[order[0]][0] * (n_cols // RING) for order in ORDERS]
    p_r = [Part(rings, ORDERS[c], n_cols // n_blk, r_sems[c], x=red_scr[c], recv=[None] + grab(2), row0=first_rows[c], lanes=(0, o_lanes[c][1])) for c in COLOURS]
    h_out, = rest
    hand = Handout((q_ref, do_home), qd_scr, hand_sems)
    o_back = Return(o_scr, oh_scr, oh_sems)
    dq_back = Return(rot_scr, dqh_scr, dqh_sems)

    for c in COLOURS:
        own = pl.ds(pl.multiple_of(p_kv[c].own_rows(), 16), split[c][1])
        ys[c][own, :e_dim] = k_ref[pl.ds(*split[c]), :]
        ys[c][own, e_dim:] = v_ref[pl.ds(*split[c]), :]
    enter(rings, with_partner=True, with_mirror=True)
    stage(p_kv, "ag_start2")
    stage(p_kv, "ag_end2")
    stage(p_kv, "ag_start1")
    hand.start(0)
    stage(p_kv, "ag_end1")
    stage(p_kv, "ag_start0")
    for cols in range(0, n_cols, COLS):
        res = lax.dot_general(grad_ref[...], wo_ref[pl.ds(cols, COLS), :], (((1,), (1,)), ((), ())), preferred_element_type=F32).astype(BF16)
        for b in range(n_groups):
            for h in range(COLS // e_dim):
                do_home[b, pl.ds(cols + h * rows, rows), :] = res[b * rows:(b + 1) * rows, h * e_dim:(h + 1) * e_dim]
    dqt_scr[...] = jnp.zeros_like(dqt_scr)
    dkv_scr[...] = jnp.zeros_like(dkv_scr)
    m_scr[...] = jnp.full_like(m_scr, -jnp.inf)
    l_scr[...] = jnp.zeros_like(l_scr)
    hand.wait(0)
    for grp in range(n_groups):
        qt_scr[grp] = qd_scr[grp, 0].T
    stage(p_kv, "ag_mid0")
    hand.start(1)
    stage(p_kv, "ag_end0")

    def place_kv(blk, carry):
        for c in COLOURS:
            at, rb = split[c]
            src = pl.ds(pl.multiple_of(place_in_order(blk, ORDERS[c]) * rb, 16), rb)
            kv_scr[pl.ds(pl.multiple_of(blk * rows + at, 16), rb), :] = ys[c][src, :]
        return carry

    h_slab = d_model // RING
    n_tok = hid_ref.shape[0]

    def hid_cols(pos):
        return hid_ref.at[:, pl.ds(pl.multiple_of(pos * h_slab, h_slab), h_slab)]

    def grad_cols(c):
        return grad_ref.at[:, pl.ds(*o_lanes[c])]

    h_sent, g_sent = [], []
    for c in COLOURS:
        ring = rings[ORDERS[c][0]]
        here = pl.ds(pl.multiple_of(ring[0] * n_tok, n_tok), n_tok)
        h_sent += spread(ring, hid_cols, hr[c], n_tok, h_sems[c])
        g_sent += spread(ring, lambda pos, c=c: grad_cols(c), gr[c], n_tok, g_sems[c])
        hr[c][here, :] = hid_cols(ring[0])[...]
        gr[c][here, :] = grad_cols(c)[...]
    for copy in g_sent:
        copy.start()
    lax.fori_loop(0, n_blk, place_kv, 0)

    n_first = cp // per_tile + 1
    n_steps = n_blk // per_tile + 1

    def over_tiles(tile_step, extra):
        def body(t, carry):
            grp = (t - n_first + n_steps) // n_steps
            piece = cp + grp * (mirror - cp)
            tile_idx = t - grp * n_first
            last = tile_idx == piece // per_tile

            @pl.when(jnp.logical_not(last))
            def _():
                tile_step(grp, tile_idx, piece, False)

            @pl.when(last)
            def _():
                tile_step(grp, tile_idx, piece, True)

            for when, action in extra:
                pl.when(t == when)(action)
            return carry

        lax.fori_loop(0, n_steps, body, 0)

    def fwd_step(grp, tile_idx, piece, masked):
        row0 = pl.multiple_of(tile_idx * TILE, TILE)
        k_t = kv_scr[pl.ds(row0, TILE), :e_dim]
        v_t = kv_scr[pl.ds(row0, TILE), e_dim:]
        for c0 in range(0, n_cols, COLS):
            cs = slice(c0, c0 + COLS)
            s = dot(k_t, qt_scr[grp, :, cs])
            if masked:
                s = jnp.where(causal_mask(row0, piece * BLK, COLS), s, -jnp.inf)
            m_old = m_scr[grp, :, cs]
            m_new = jnp.maximum(m_old, jnp.max(s, axis=0, keepdims=True))
            p = jnp.exp(s - m_new)
            alpha = jnp.exp(m_old - m_new)
            m_scr[grp, :, cs] = m_new
            l_scr[grp, :, cs] = l_scr[grp, :, cs] * alpha + jnp.sum(p, axis=0, keepdims=True)
            dqt_scr[grp, :, cs] = dqt_scr[grp, :, cs] * alpha + dot_ta(v_t, p.astype(BF16))

    over_tiles(fwd_step, ())
    hand.wait(1)
    for grp in range(n_groups):
        o_t = (dqt_scr[grp] / l_scr[grp]).astype(BF16)
        o_scr[grp] = o_t.T
        dot_scr[grp] = qd_scr[grp, 1].T
        delta_scr[grp] = jnp.sum(dot_scr[grp].astype(F32) * o_t.astype(F32), axis=0, keepdims=True)
    o_back.start()
    m_scr[...] = m_scr[...] + jnp.log(l_scr[...])
    dqt_scr[...] = jnp.zeros_like(dqt_scr)

    def bwd_step(grp, tile_idx, piece, masked):
        row0 = pl.multiple_of(tile_idx * TILE, TILE)
        k_t = kv_scr[pl.ds(row0, TILE), :e_dim]
        v_t = kv_scr[pl.ds(row0, TILE), e_dim:]
        for c0 in range(0, n_cols, COLS):
            cs = slice(c0, c0 + COLS)
            s = dot(k_t, qt_scr[grp, :, cs])
            p = jnp.exp(s - m_scr[grp, :, cs])
            if masked:
                p = jnp.where(causal_mask(row0, piece * BLK, COLS), p, 0.0)
            d_p = dot(v_t, dot_scr[grp, :, cs])
            p_scr[:, cs] = p.astype(BF16)
            ds_scr[:, cs] = (p * (d_p - delta_scr[grp, :, cs])).astype(BF16)
        at = pl.ds(row0, TILE)
        dkv_scr[at, :e_dim] += dot(ds_scr[...], qd_scr[grp, 0])
        dkv_scr[at, e_dim:] += dot(p_scr[...], qd_scr[grp, 1])
        dqt_scr[grp] += dot_ta(k_t, ds_scr[...])

    o_slab = n_cols // RING

    def o_cols(pos):
        return tok_scr.at[:, pl.ds(pl.multiple_of(pos * o_slab, o_slab), o_slab)]

    def o_spread():
        return [copy for c in COLOURS for copy in spread(rings[ORDERS[c][0]], o_cols, orr[c], n_tok, or_sems[c])]

    def send_o():
        o_back.wait()
        place_heads(tok_scr, oh_scr)
        for c in COLOURS:
            pos = rings[ORDERS[c][0]][0]
            orr[c][pl.ds(pl.multiple_of(pos * n_tok, n_tok), n_tok), :] = o_cols(pos)[...]
        for copy in o_spread():
            copy.start()

    def slab_wo():
        for copy in o_spread() + g_sent:
            copy.wait_recv()
        for c, red in enumerate(red_scr):
            for at in range(0, red.shape[1], 128):
                red[:, at:at + 128] = dot_ta(orr[c][...], gr[c][:, at:at + 128])
        stage(p_r, "rs_start1")
        for copy in h_sent:
            copy.start()

    over_tiles(bwd_step, ((3, send_o), (8, slab_wo), (11, lambda: stage(p_r, "rs_mid1"))))

    def place_dkv(blk, carry):
        for c in COLOURS:
            at, rb = rows_d[c]
            dst = pl.ds(pl.multiple_of(place_in_order(blk, ORDERS[c]) * rb, 8), rb)
            xs[c][dst, :] = dkv_scr[pl.ds(pl.multiple_of(blk * rows + at, 8), rb), :]
        return carry

    lax.fori_loop(0, n_blk, place_dkv, 0)
    stage(p_d, "rs_start0")

    scale = e_dim ** -0.5
    half_dim = e_dim // 2
    for grp in range(n_groups):
        cos_t, sin_t = cos_ref[grp], sin_ref[grp]
        for h in range(n_cols // rows):
            cols = slice(h * rows, (h + 1) * rows)
            low, high = dqt_scr[grp, :half_dim, cols], dqt_scr[grp, half_dim:, cols]
            turned = jnp.concatenate([low * cos_t + high * sin_t, high * cos_t - low * sin_t], axis=0) * scale
            rot_scr[grp, cols, :] = turned.T.astype(BF16)
    dq_back.start()
    tp = lax.axis_index("tp")
    partner = (1 - tp, cp)
    for at in range(0, d_model, D_TILE):
        cols = slice(at, at + D_TILE)
        res = dot(tok_scr[...], wo_ref[:, cols])
        for b in range(n_groups):
            part_scr[b, :, cols] = res[b * rows:(b + 1) * rows]

    def swap(src, dst, i):
        return pltpu.make_async_remote_copy(src_ref=src, dst_ref=dst, send_sem=swap_sems[0].at[i], recv_sem=swap_sems[1].at[i], device_id=partner, device_id_type=MESH)

    swap_part = swap(part_scr.at[1 - tp], got_scr, 0)
    swap_part.start()
    stage(p_r, "rs_end1")
    stage(p_r, "rs_start2")
    stage(p_d, "rs_mid0")
    for copy in h_sent:
        copy.wait_recv()
    h_outs = [pltpu.make_async_copy(hr[c], out, h_out.at[c]) for c, out in enumerate((ho0, ho1, ho2))]
    for copy in h_outs:
        copy.start()
    swap_part.wait()
    out_scr[tp] = (part_scr[tp] + got_scr[...]).astype(BF16)
    swap_out = swap(out_scr.at[tp], out_scr.at[tp], 1)
    swap_out.start()
    dq_back.wait()

    def put(src, dst):
        copy = pltpu.make_async_copy(src, dst, h_out.at[len(h_outs)])
        copy.start()
        h_outs.append(copy)

    put(dqh_scr, dqh_ref)
    swap_out.wait()
    put(out_scr, out_ref)
    stage(p_r, "rs_end2")
    for part, out in zip(p_r, (red0, red1, red2)):
        out[...] = part.x[pl.ds(pl.multiple_of(part.own_rows(), 8), part.rb), :]
    stage(p_d, "rs_end0")
    for part, out in zip(p_d, (sl0, sl1, sl2)):
        slab, _, _, starts, *_ = part.place(0)
        put(part.view(part.x, starts[0], slab), out)
    for part in p_kv:
        part.drain(ag=COLOURS)
    for part in p_d:
        part.drain(rs=(0,))
    for part in p_r:
        part.drain(rs=(1, 2))
    for kind in range(2):
        hand.drain(kind)
    for copy in h_sent + g_sent + o_spread():
        copy.wait_send()
    for copy in h_outs:
        copy.wait()
    o_back.drain()
    dq_back.drain()


def attention(key_loc, val_loc, q_home, hid, grad, w_out, cos_t, sin_t):
    n_batch, n_cols, e_dim = q_home.shape
    rows = key_loc.shape[0]
    n_tok, d_model = grad.shape
    n_blk = RING ** 3
    seq = n_blk * rows
    o_lanes = wide_lanes(d_model)
    slab = n_cols // RING
    vmem, anyspace = pl.BlockSpec(memory_space=pltpu.VMEM), pl.BlockSpec(memory_space=pl.ANY)
    heads = (2, n_cols, e_dim)
    h_ring = (RING * n_tok, d_model // RING)
    work = n_cols * seq
    return pl.pallas_call(
        attn_kernel,
        out_shape=(jax.ShapeDtypeStruct(heads, BF16), jax.ShapeDtypeStruct((2, rows, d_model), BF16)) + tuple(jax.ShapeDtypeStruct((n_blk // RING * rb, 2 * e_dim), F32) for _, rb in by_rows(rows, 8)) + tuple(jax.ShapeDtypeStruct((n_cols // n_blk, n), F32) for _, n in o_lanes) + (jax.ShapeDtypeStruct(h_ring, BF16),) * 3,
        in_specs=[vmem] * 8,
        out_specs=(anyspace,) * 5 + (vmem,) * 3 + (anyspace,) * 3,
        scratch_shapes=[pltpu.VMEM((n_blk * rb, 2 * e_dim), BF16) for _, rb in by_rows(rows, 16)]
        + [
            pltpu.VMEM((seq, 2 * e_dim), BF16),
            pltpu.VMEM((2, 2, n_cols, e_dim), BF16),
            pltpu.VMEM(heads, BF16),
            pltpu.VMEM((2, e_dim, n_cols), BF16),
            pltpu.VMEM((2, e_dim, n_cols), BF16),
            pltpu.VMEM((2, e_dim, n_cols), F32),
            pltpu.VMEM((2, 1, n_cols), F32),
            pltpu.VMEM((2, 1, n_cols), F32),
            pltpu.VMEM((2, 1, n_cols), F32),
            pltpu.VMEM((TILE, n_cols), BF16),
            pltpu.VMEM((TILE, n_cols), BF16),
            pltpu.VMEM((seq, 2 * e_dim), F32),
            pltpu.VMEM((n_tok, n_cols), BF16),
            pltpu.VMEM((2, rows, d_model), F32),
            pltpu.VMEM((rows, d_model), F32),
            pltpu.VMEM((2, rows, d_model), BF16),
        ]
        + [pltpu.VMEM(heads, BF16)] * 4
        + [pltpu.VMEM(h_ring, BF16)] * 3
        + [pltpu.VMEM((RING * n_tok, lanes), BF16) for _, lanes in o_lanes]
        + [pltpu.VMEM((RING * n_tok, slab), BF16)] * 3
        + [pltpu.VMEM((n_blk * rb, 2 * e_dim), F32) for _, rb in by_rows(rows, 8)]
        + pair(3 * HOPS) * 9
        + pair(3) * 9
        + [pltpu.VMEM((slab, lanes), F32) for _, lanes in o_lanes]
        + pair(4)
        + pair(2) * 3
        + [pltpu.VMEM((slab_rows(rb)[0], 2 * e_dim), F32) for _, rb in by_rows(rows, 8)]
        + [pltpu.VMEM((n, lanes), F32) for _, lanes in o_lanes for n in slab_rows(n_cols // n_blk)[1:]]
        + [pltpu.SemaphoreType.DMA((8,))],
        compiler_params=pltpu.CompilerParams(collective_id=2, has_side_effects=True, vmem_limit_bytes=VMEM_LIMIT),
        cost_estimate=pl.CostEstimate(flops=14 * work * e_dim, bytes_accessed=seq * e_dim * 12, transcendentals=2 * work),
        name="attention",
    )(key_loc, val_loc, q_home, hid, grad, w_out, cos_t, sin_t)


GRAD_PLAN = (
    "o.ag_start2", "d.rs_start1", "o.ag_end2", "o.ag_start1", "weights.q", "d.rs_mid1", "o.ag_mid1", "d.rs_end1",
    "d.rs_start2", "s.rs_start1", "d.rs_end2", "o.ag_end1", "weights.prep", "s.rs_mid1", "weights.kv", "o.ag_start0",
    "weights.slab", "t.rs_start1", "s.rs_end1", "t.rs_mid1", "s.rs_start2", "o.ag_mid0", "s.rs_end2", "t.rs_end1",
    "q.ag_start2", "t.rs_start2", "t.rs_end2", "k.ag_start2", "q.ag_end2", "q.ag_start1", "k.ag_end2", "k.ag_start1",
    "q.ag_mid1", "k.ag_mid1", "q.ag_end1", "q.ag_start0", "k.ag_end1", "k.ag_start0", "o.ag_end0", "k.ag_mid0",
    "q.ag_mid0", "k.ag_end0", "q.ag_end0",
)


def grad_kernel(sl0, sl1, sl2, dqh_ref, red0, red1, red2, hi0, hi1, hi2, cos_ref, sin_ref, gq_ref, go_ref, gk_ref, gv_ref, dkd_ref, yq, yo, yk, yp, turn_scr, tok_scr, kvt_scr, kvr_scr, mine_scr, give_scr, got_scr, xk, *rest):
    rest = list(rest)

    def grab(n):
        return [rest.pop(0) for _ in range(n)]

    n_blk = RING ** 3
    n_batch, _, head_dim = dqh_ref.shape
    n_tok, n_cols = tok_scr.shape
    d_model = yq.shape[0]
    rows, lanes = n_tok // n_batch, 2 * head_dim
    n_local = n_cols // head_dim
    q_lanes, o_lanes = thirds(n_local, head_dim), wide_lanes(d_model)
    split = by_rows(rows, 8)
    tp, cp = lax.axis_index("tp"), lax.axis_index("cp")
    partner = (1 - tp, cp)
    rings = [ring_of(axis) for axis in COLOURS]

    def shifted(c, n_rows):
        return 0 - rings[ORDERS[c][0]][0] * (n_rows // RING)

    xs, xqs, hr, dqr = (grab(3) for _ in range(4))
    sem_d, sem_q, sem_o, sem_g = ([grab(2) for _ in COLOURS] for _ in range(4))
    sem_k, sem_kr = grab(2), grab(2)
    p_d = [Part(rings, ORDERS[c], split[c][1], sem_d[c], x=xs[c], recv=[None] + grab(2), row0=shifted(c, n_blk * split[c][1]), lanes=(0, lanes)) for c in COLOURS]
    p_s = [Part(rings, ORDERS[c], d_model // n_blk, sem_q[c], x=xqs[c], recv=[None] + grab(2), row0=shifted(c, d_model), lanes=(0, q_lanes[c][1])) for c in COLOURS]
    p_q = [Part(rings, ORDERS[c], d_model // n_blk, sem_q[c], y=yq, lanes=q_lanes[c]) for c in COLOURS]
    p_o = [Part(rings, ORDERS[c], n_cols // n_blk, sem_o[c], y=yo, lanes=o_lanes[c]) for c in COLOURS]
    p_t = [Part(rings, ORDERS[2], d_model // n_blk, sem_k, x=xk, recv=[None] + grab(2), row0=shifted(2, d_model), lanes=(0, head_dim))]
    p_k = [Part(rings, ORDERS[2], d_model // n_blk, sem_k, y=yk, lanes=(0, head_dim))]
    in_sem, out_sem, swap_s, swap_r = rest

    loads = [pltpu.make_async_copy(src, dst, in_sem.at[i]) for i, (src, dst) in enumerate(zip((sl0, sl1, sl2, hi0, hi1, hi2), xs + hr))]
    for copy in loads:
        copy.start()
    place_heads(tok_scr, dqh_ref)

    def tok_cols(c):
        return pl.ds(*q_lanes[c])

    for part, red in zip(p_o, (red0, red1, red2)):
        part.y[pl.ds(pl.multiple_of(part.own_rows(), 8), part.rb), pl.ds(*part.lanes)] = red[...]
    dq_sent = []
    for c in COLOURS:
        ring = rings[ORDERS[c][0]]
        dqr[c][pl.ds(pl.multiple_of(ring[0] * n_tok, n_tok), n_tok), :] = tok_scr[:, tok_cols(c)]
        dq_sent += spread(ring, lambda pos, c=c: tok_scr.at[:, tok_cols(c)], dqr[c], n_tok, sem_g[c])
    ring_k = rings[ORDERS[2][0]]
    kv_sent = spread(ring_k, lambda pos: kvt_scr, kvr_scr, n_tok, sem_kr)
    enter(rings, with_partner=True)
    for copy in dq_sent:
        copy.start()
    for copy in loads:
        copy.wait()
    half_dim = head_dim // 2
    first = tp == 0
    swap_small = pltpu.make_async_remote_copy(src_ref=give_scr, dst_ref=got_scr, send_sem=swap_s.at[0], recv_sem=swap_r.at[0], device_id=partner, device_id_type=MESH)
    swap = pltpu.make_async_remote_copy(src_ref=yk, dst_ref=yp, send_sem=swap_s.at[1], recv_sem=swap_r.at[1], device_id=partner, device_id_type=MESH)

    def put_o(which):
        for c, part in enumerate(p_o):
            slab, _, _, starts, *_ = part.place(0)
            for i in which:
                pltpu.make_async_copy(part.view(yo, starts[i], slab), part.view(go_ref, starts[i], slab), out_sem.at[c]).start()

    def turn_q(which):
        for c, part in enumerate(p_q):
            slab, _, _, starts, *_ = part.place(0)
            for i in which:
                at = pl.multiple_of(starts[i], slab)
                for h in range(q_lanes[c][0] // head_dim, sum(q_lanes[c]) // head_dim):
                    turn_scr[pl.ds(at * n_local + h, slab, stride=n_local), :] = yq[pl.ds(at, slab), pl.ds(h * head_dim, head_dim)]

    def own_block(parts, sums):
        for part, total in zip(parts, sums):
            at, lanes_y, lanes_x = part.own_rows(), pl.ds(*part.lanes), pl.ds(*total.lanes)
            part.y[pl.ds(pl.multiple_of(at, 8), part.rb), lanes_y] = total.x[pl.ds(pl.multiple_of(total.own_rows(), 8), part.rb), lanes_x]

    def slab_term(dst, hid, other):
        for at in range(0, dst.shape[0], D_TILE):
            dst[pl.ds(at, D_TILE), :] = dot_ta(hid[:, at:at + D_TILE], other[...])

    def weights_q():
        for copy in dq_sent:
            copy.wait_recv()
        for c in COLOURS:
            slab_term(xqs[c], hr[c], dqr[c])

    def new_dkv():
        dkd_ref[...] = mine_scr[...].astype(BF16)
        return dkd_ref[:, :head_dim], dkd_ref[:, head_dim:]

    def weights_prep():
        for c in COLOURS:
            at, rb = split[c]
            own = xs[c][pl.ds(pl.multiple_of(p_d[c].own_rows(), 8), rb), :]
            cos_tab, sin_tab = cos_ref[pl.ds(at, rb), :], sin_ref[pl.ds(at, rb), :]
            low, high = own[:, :half_dim], own[:, half_dim:head_dim]
            mine_scr[pl.ds(at, rb), :head_dim] = jnp.concatenate([low * cos_tab + high * sin_tab, high * cos_tab - low * sin_tab], axis=1)
            mine_scr[pl.ds(at, rb), head_dim:] = own[:, head_dim:]
        dk_new, dv_new = new_dkv()
        give_scr[...] = jnp.where(first, dv_new, dk_new)
        swap_small.start()

    def weights_kv():
        swap_small.wait()
        got = got_scr[...]
        keep = jnp.where(first, dkd_ref[:, :head_dim], dkd_ref[:, head_dim:])
        kvt_scr[...] = jnp.concatenate([jnp.where(first, keep, got), jnp.where(first, got, keep)], axis=0)
        kvr_scr[pl.ds(pl.multiple_of(ring_k[0] * n_tok, n_tok), n_tok), :] = kvt_scr[...]
        for copy in kv_sent:
            copy.start()

    def weights_slab():
        for copy in kv_sent:
            copy.wait_recv()
        slab_term(xk, hr[2], kvr_scr)

    groups = {"d": p_d, "s": p_s, "q": p_q, "o": p_o, "t": p_t, "k": p_k}
    after = {
        "weights.q": weights_q,
        "weights.prep": weights_prep,
        "weights.kv": weights_kv,
        "weights.slab": weights_slab,
        "s.rs_end2": lambda: own_block(p_q, p_s),
        "t.rs_end2": lambda: own_block(p_k, p_t),
        "o.ag_mid0": lambda: put_o((0, 1, 3)),
        "o.ag_end0": lambda: put_o((2,)),
        "q.ag_start0": lambda: turn_q((0,)),
        "q.ag_mid0": lambda: turn_q((1, 3)),
        "q.ag_end0": lambda: turn_q((2,)),
        "k.ag_end0": swap.start,
    }
    for step in GRAD_PLAN:
        who, what = step.split(".")
        if who in groups:
            stage(groups[who], what)
        if step in after:
            after[step]()
    out_q = pltpu.make_async_copy(turn_scr, gq_ref, out_sem.at[3])
    out_q.start()
    swap.wait()

    def put_kv(k_src, v_src):
        outs = [pltpu.make_async_copy(k_src, gk_ref, out_sem.at[4]), pltpu.make_async_copy(v_src, gv_ref, out_sem.at[5])]
        for copy in outs:
            copy.start()
        for copy in outs:
            copy.wait()

    @pl.when(first)
    def _():
        put_kv(yk, yp)

    @pl.when(jnp.logical_not(first))
    def _():
        put_kv(yp, yk)

    out_q.wait()
    for c, part in enumerate(p_o):
        pltpu.make_async_copy(part.view(yo, 0, n_cols), part.view(go_ref, 0, n_cols), out_sem.at[c]).wait()
    for part in p_d + p_s + p_t:
        part.drain(rs=(1, 2))
    for part in p_q + p_o + p_k:
        part.drain(ag=COLOURS)
    for copy in dq_sent + kv_sent:
        copy.wait_send()


def grad_sums(slabs, dq_home, reds, h_rings, cos_tab, sin_tab, d_model):
    n_batch, n_rows, head_dim = dq_home.shape
    rows = cos_tab.shape[0]
    n_tok, n_cols = n_batch * rows, n_rows // rows * head_dim
    n_blk = RING ** 3
    lanes = 2 * head_dim
    q_lanes = thirds(n_cols // head_dim, head_dim)
    split = by_rows(rows, 8)
    vmem, anyspace = pl.BlockSpec(memory_space=pltpu.VMEM), pl.BlockSpec(memory_space=pl.ANY)

    def full(*shape):
        return pltpu.VMEM(shape, F32)

    def half(*shape):
        return pltpu.VMEM(shape, BF16)

    def later(rb, width):
        return [full(n, width) for n in slab_rows(rb)[1:]]

    slab, ring_tok = d_model // RING, RING * n_tok
    scratch = [full(d_model, n_cols), full(n_cols, d_model), full(d_model, head_dim), full(d_model, head_dim), full(d_model * n_cols // head_dim, head_dim)]
    scratch += [half(n_tok, n_cols), half(n_tok, head_dim), half(ring_tok, head_dim), full(rows, lanes), half(rows, head_dim), half(rows, head_dim), full(slab, head_dim)]
    scratch += [full(n_blk // RING * rb, lanes) for _, rb in split]
    scratch += [full(slab, w) for _, w in q_lanes]
    scratch += [half(ring_tok, slab)] * 3 + [half(ring_tok, w) for _, w in q_lanes]
    scratch += pair(3 * HOPS) * 9 + pair(3) * 3 + pair(3 * HOPS) + pair(3)
    for _, rb in split:
        scratch += later(rb, lanes)
    for _, w in q_lanes:
        scratch += later(d_model // n_blk, w)
    scratch += later(d_model // n_blk, head_dim)
    scratch += [pltpu.SemaphoreType.DMA((6,)), pltpu.SemaphoreType.DMA((6,))] + pair(2)
    return pl.pallas_call(
        grad_kernel,
        out_shape=(
            jax.ShapeDtypeStruct((d_model * n_cols // head_dim, head_dim), F32),
            jax.ShapeDtypeStruct((n_cols, d_model), F32),
            jax.ShapeDtypeStruct((d_model, head_dim), F32),
            jax.ShapeDtypeStruct((d_model, head_dim), F32),
            jax.ShapeDtypeStruct((rows, lanes), BF16),
        ),
        in_specs=[anyspace] * 3 + [vmem] * 4 + [anyspace] * 3 + [vmem] * 2,
        out_specs=(anyspace,) * 4 + (vmem,),
        scratch_shapes=scratch,
        compiler_params=pltpu.CompilerParams(collective_id=3, has_side_effects=True, vmem_limit_bytes=VMEM_LIMIT),
        cost_estimate=pl.CostEstimate(flops=n_tok * d_model * n_cols * 160, bytes_accessed=40 << 20, transcendentals=0),
        name="grad_sums",
    )(*slabs, dq_home, *reds, *h_rings, cos_tab, sin_tab)


def solution(mesh):
    cp_size = mesh.shape["cp"]
    partner = [(0, 1), (1, 0)]

    def local_program(hidden, grad_out, w_query, w_key, w_value, w_out):
        block_len = hidden.shape[1]
        n_local = w_query.shape[1]
        head_dim = w_key.shape[1]
        q_scale = head_dim ** -0.5
        cp_idx = lax.axis_index("cp")
        tp_idx = lax.axis_index("tp")
        mirror_idx = cp_size - 1 - cp_idx
        cos_tab, sin_tab = rope_tables(cp_idx * block_len + jnp.arange(block_len), head_dim)
        cos_mir, sin_mir = rope_tables(mirror_idx * block_len + jnp.arange(block_len), head_dim)

        def pick(pair, idx):
            return lax.dynamic_index_in_dim(pair, idx, 0, keepdims=False)

        def sum_over_tp(part, extra=None):
            total = pick(part, tp_idx) + lax.ppermute(pick(part, 1 - tp_idx), "tp", partner)
            if extra is not None:
                total = total + extra
            mine = total.astype(BF16)
            other = lax.ppermute(mine, "tp", partner)
            first = tp_idx == 0
            return jnp.stack([jnp.where(first, mine, other), jnp.where(first, other, mine)])

        hid_b = pick(hidden, tp_idx)
        key_loc = rotate(dot(hid_b, w_key), cos_tab, sin_tab).astype(BF16)
        val_loc = dot(hid_b, w_value).astype(BF16)
        q_pre = jnp.einsum("bsd,dhe->bhse", hidden, w_query, preferred_element_type=F32)
        queries = (rotate(q_pre, cos_tab, sin_tab) * q_scale).astype(BF16)
        q_home = queries.reshape(2, n_local * block_len, head_dim)
        d_model = hidden.shape[-1]
        hid, grad = hidden.reshape(-1, d_model), grad_out.reshape(-1, d_model)
        tabs_t = [jnp.stack(pair_t) for pair_t in ((cos_tab.T, cos_mir.T), (sin_tab.T, sin_mir.T))]
        dq_home, attn_out, *more = attention(key_loc, val_loc, q_home, hid, grad, w_out.reshape(-1, d_model), *tabs_t)
        dq_pre = dq_home.reshape(2, n_local, block_len, head_dim)
        grad_q, grad_o, d_w_key, d_w_value, dkv_new = grad_sums(more[:3], dq_home, more[3:6], more[6:], cos_tab, sin_tab, d_model)
        d_w_query = grad_q.reshape(w_query.shape)
        d_w_out = grad_o.reshape(w_out.shape)
        dk_pre, dv_pre = dkv_new[:, :head_dim], dkv_new[:, head_dim:]
        dh_kv = dot(dk_pre, w_key.T) + dot(dv_pre, w_value.T)
        d_hidden = sum_over_tp(jnp.einsum("cirf,eif->cre", dq_pre, w_query, preferred_element_type=F32), dh_kv)
        return attn_out, d_hidden, d_w_query, d_w_key, d_w_value, d_w_out

    row_spec = P(None, "cp", None)
    return jax.shard_map(local_program, mesh=mesh, in_specs=(row_spec, row_spec, P(None, "tp", None), P(), P(), P("tp", None, None)), out_specs=(row_spec, row_spec, P(None, "tp", None), P(), P(), P("tp", None, None)), check_vma=False)
```
